32 devices in a mesh: gx: 4 (over z), gy: 4 (over x, core), gz: 2 (over y).
Axes of the slice: x: 2, y: 2, z: 4, core: 2. Of those that a mesh axis runs over, the one named last changes fastest.
Arguments:
- x_a: bfloat16 [32, 8, 64, 256], P(None, 'gx', 'gy', 'gz'), may hold values from -12 to 12
- x_b: bfloat16 [32, 8, 64, 256], P(None, 'gx', 'gy', 'gz'), may hold values from -12 to 12
- w_first: bfloat16 [3, 3, 3, 32, 32], replicated, may hold values from -0.21875 to 0.21875
- w_second: bfloat16 [3, 3, 3, 32, 32], replicated, may hold values from -0.21875 to 0.21875
- gain_first: float32 [32], replicated, may hold values from 0.1 to 1.9
- bias_first: float32 [32], replicated, may hold values from -2 to 2
- gain_second: float32 [32], replicated, may hold values from 0.1 to 1.9
- bias_second: float32 [32], replicated, may hold values from -2 to 2
- grad_out: bfloat16 [32, 8, 64, 256], P(None, 'gx', 'gy', 'gz'), may hold values from -6 to 6
Outputs:
- y_a: bfloat16 [32, 8, 64, 256], P(None, 'gx', 'gy', 'gz')
- dx_b: bfloat16 [32, 8, 64, 256], P(None, 'gx', 'gy', 'gz')
- grad_w_first: float32 [3, 3, 3, 32, 32], replicated
- grad_w_second: float32 [3, 3, 3, 32, 32], replicated
- grad_norm: float32 [4, 32], replicated
The draws below stay inside these ranges and needn't reach their ends.
All inputs are finite; a program needn't handle non-finite values.
Results may differ from the reference program's by a relative error of at most 0.0063.
Values may be sent and summed in bfloat16 or wider, within the bound.
A program may use at most 128 MiB of HBM per device.

```python
import math
import jax
import jax.numpy as jnp
from jax import lax

C = 32
NX = 8
NY = 64
NZ = 256
VOXELS = 131072


def draw_volume(key, salt):
    folded = jax.random.fold_in(key, salt)
    depth = jnp.arange(NX, dtype=jnp.float32) / max(NX - 1, 1)
    base = jnp.clip(jax.random.normal(folded, (C, NX, NY, NZ), jnp.float32), -4.0, 4.0)
    ramp = 1.0 + 2.0 * depth
    value = base * ramp[None, :, None, None]
    return value.astype(jnp.bfloat16)


def draw_x_a(key, part):
    return draw_volume(key, 11)


def draw_x_b(key, part):
    return draw_volume(key, 23)


def block_levels(key, extent, cuts, smallest, high):
    level = 1.0
    for axis_at, blocks in cuts:
        draws = jax.random.uniform(jax.random.fold_in(jax.random.fold_in(key, 6), axis_at), (blocks,), jnp.float32, smallest / len(cuts), high / len(cuts))
        level = level * jnp.repeat(jnp.exp(draws), extent[axis_at] // blocks).reshape((-1,) + (1,) * (len(extent) - 1 - axis_at))
    return level


def bell_draw(own_key, extent, scale, bound, cuts=(), kind=jnp.bfloat16):
    result = jax.random.normal(own_key, extent, jnp.float32) * scale
    if len(cuts) > 0:
        result = block_levels(own_key, extent, cuts, -0.22, 0.18) * result
    return jnp.clip(result, min=-bound, max=bound).astype(kind)


def setup_inputs(seed: int = 0) -> dict:
    arg_keys = jax.random.split(jax.random.key(seed), 10)
    return {
        "x_a": draw_x_a(jax.random.fold_in(arg_keys[9], 71), 0),
        "x_b": draw_x_b(jax.random.fold_in(arg_keys[9], 71), 0),
        "w_first": bell_draw(arg_keys[2], (3, 3, 3, C, C), (27 * C) ** -0.5, 0.21875),
        "w_second": bell_draw(arg_keys[3], (3, 3, 3, C, C), (27 * C) ** -0.5, 0.21875),
        "gain_first": jnp.clip(1.0 + 0.18 * jax.random.normal(arg_keys[4], (C,), jnp.float32), 0.1, 1.9),
        "bias_first": bell_draw(arg_keys[5], (C,), 0.5, 2.0, (), jnp.float32),
        "gain_second": jnp.clip(1.0 + 0.18 * jax.random.normal(arg_keys[6], (C,), jnp.float32), 0.1, 1.9),
        "bias_second": bell_draw(arg_keys[7], (C,), 0.5, 2.0, (), jnp.float32),
        "grad_out": bell_draw(arg_keys[8], (C, NX, NY, NZ), 1.0, 6.0, ((1, 4), (2, 4), (3, 2))),
    }


EPSILON = 1e-05

def spread(values):
    return values[:, None, None, None]

def silu_slope(value):
    sigma = jax.nn.sigmoid(value)
    return sigma * (1.0 + value * (1.0 - sigma))

def pad_volume(volume):
    return jnp.pad(volume, ((0, 0), (1, 1), (1, 1), (1, 1)))

def convolve(padded, weight):
    in_chan = padded.shape[0]
    out_chan = weight.shape[3]
    span_x = padded.shape[1] - 2
    span_y = padded.shape[2] - 2
    span_z = padded.shape[3] - 2
    total = jnp.zeros((out_chan, span_x * span_y * span_z), jnp.float32)
    for shift_x in range(3):
        for shift_y in range(3):
            pieces = [padded[:, shift_x:shift_x + span_x, shift_y:shift_y + span_y, shift_z:shift_z + span_z] for shift_z in range(3)]
            stacked = jnp.concatenate(pieces, axis=0).reshape(3 * in_chan, -1)
            matrix = weight[shift_x, shift_y].transpose(1, 0, 2).reshape(out_chan, 3 * in_chan)
            total = total + jnp.dot(matrix, stacked, preferred_element_type=jnp.float32)
    return total.reshape(out_chan, span_x, span_y, span_z)

def kernel_grad(padded, upstream):
    in_chan = padded.shape[0]
    out_chan = upstream.shape[0]
    span_x, span_y, span_z = (upstream.shape[1], upstream.shape[2], upstream.shape[3])
    flat = upstream.reshape(out_chan, -1)
    rows = []
    for shift_x in range(3):
        for shift_y in range(3):
            pieces = [padded[:, shift_x:shift_x + span_x, shift_y:shift_y + span_y, shift_z:shift_z + span_z] for shift_z in range(3)]
            stacked = jnp.concatenate(pieces, axis=0).reshape(3 * in_chan, -1)
            product = lax.dot_general(flat, stacked, (((1,), (1,)), ((), ())), preferred_element_type=jnp.float32)
            rows.append(product.reshape(out_chan, 3, in_chan).transpose(1, 0, 2))
    return jnp.stack(rows).reshape(3, 3, 3, out_chan, in_chan)

def flipped(weight):
    return jnp.flip(weight, (0, 1, 2)).transpose(0, 1, 2, 4, 3)

def forward_layer(features, weight, gain, bias):
    conv_out = convolve(pad_volume(features), weight)
    means = lax.optimization_barrier(jnp.sum(conv_out, axis=(1, 2, 3))) / VOXELS
    variance = lax.optimization_barrier(jnp.sum(jnp.square(conv_out - spread(means)), axis=(1, 2, 3))) / VOXELS
    scales = lax.rsqrt(variance + EPSILON)
    normed = (conv_out - spread(means)) * spread(scales)
    preact = spread(gain) * normed + spread(bias)
    output = (preact * jax.nn.sigmoid(preact)).astype(jnp.bfloat16)
    return (output, preact, normed, scales)

def backward_layer(upstream, preact, normed, scales, gain):
    slope = upstream * silu_slope(preact)
    sum_d = lax.optimization_barrier(jnp.sum(slope, axis=(1, 2, 3)))
    sum_dx = lax.optimization_barrier(jnp.sum(slope * normed, axis=(1, 2, 3)))
    delta = spread(gain * scales) * (slope - spread(sum_d / VOXELS) - normed * spread(sum_dx / VOXELS))
    return (delta.astype(jnp.bfloat16), sum_d, sum_dx)

def reference(x_a, x_b, w_first, w_second, gain_first, bias_first, gain_second, bias_second, grad_out):
    hidden_a = forward_layer(x_a, w_first, gain_first, bias_first)[0]
    y_a = forward_layer(hidden_a, w_second, gain_second, bias_second)[0]
    hidden_b, pre_one, norm_one, scale_one = forward_layer(x_b, w_first, gain_first, bias_first)
    unused, pre_two, norm_two, scale_two = forward_layer(hidden_b, w_second, gain_second, bias_second)
    factor = 1.0 / math.sqrt(VOXELS)
    delta_two, sum_d2, sum_x2 = backward_layer(grad_out.astype(jnp.float32), pre_two, norm_two, scale_two, gain_second)
    grad_w_second = kernel_grad(pad_volume(hidden_b), delta_two) * factor
    upstream_one = convolve(pad_volume(delta_two), flipped(w_second))
    delta_one, sum_d1, sum_x1 = backward_layer(upstream_one, pre_one, norm_one, scale_one, gain_first)
    grad_w_first = kernel_grad(pad_volume(x_b), delta_one) * factor
    dx_b = convolve(pad_volume(delta_one), flipped(w_first)).astype(jnp.bfloat16)
    grad_norm = jnp.stack([sum_x1, sum_d1, sum_x2, sum_d2]) * factor
    return (y_a, dx_b, grad_w_first, grad_w_second, grad_norm)
```

```python
import functools
import math

import jax
import jax.numpy as jnp
from jax import lax
from jax.experimental import pallas as pl
from jax.experimental.pallas import tpu as pltpu
from jax.sharding import PartitionSpec as P

EPSILON = 1e-05
AXES = ("gx", "gy", "gz")
MESH = pl.DeviceIdType.MESH
XB, XA, GO, C1B, C1A, C2B, E1 = range(7)
D2, D1 = 7, 8
OFFSETS = [(a, b, c) for a in (-1, 0, 1) for b in (-1, 0, 1) for c in (-1, 0, 1)
           if (a, b, c) != (0, 0, 0)]
GROUP = 4
DEEP = 8


def slope_of(z):
    s = jax.nn.sigmoid(z)
    return s * (1.0 + z * (1.0 - s))


def code(offset):
    a, b, c = offset
    return (a + 1) * 9 + (b + 1) * 3 + c + 1


def minus(offset):
    return tuple(-o for o in offset)


def kernel(
    sizes, voxels, units,
    xa, xb, go, w1, w2, g1, b1, g2, b2,
    ya, dxb, gw1, gw2, gnorm,
    raw, wraw, gains, tall, mats, pads, edge_out, edge_in, cols,
    shift_xb, shift_a, shift_hb, shift_d,
    f1b, f1a, f2b, fd2, fd1, c2a, e1, slots, wsum, wunit, wslot, wfull,
    load_sem, halo_send, halo_recv, sum_send, sum_recv, w_send, w_recv,
):
    chan, nx, ny, nz = raw.shape[1:]
    wide = ny + 2
    own = nx * ny
    pitch = tall.shape[0] // chan
    count = math.prod(sizes)
    local = float(own * nz)
    factor = 1.0 / math.sqrt(voxels)
    me = [lax.axis_index(a) for a in AXES]
    rank = (me[0] * sizes[1] + me[1]) * sizes[2] + me[2]
    lane = lax.broadcasted_iota(jnp.int32, (chan, nz), 1)
    chan_of = lax.broadcasted_iota(jnp.int32, (chan, nz), 0)
    zero = jnp.zeros((chan, nz), jnp.float32)
    bf16, f32 = jnp.bfloat16, jnp.float32

    others = [(a, b, c) for a in range(sizes[0]) for b in range(sizes[1])
              for c in range(sizes[2])][1:]

    def at_offset(offset):
        return [lax.rem(m + o, s) for m, o, s in zip(me, offset, sizes)]

    def ids(place):
        return dict(zip(AXES, place))

    barrier = pltpu.get_barrier_semaphore()
    for offset in others:
        pl.semaphore_signal(
            barrier, inc=1, device_id=ids(at_offset(offset)), device_id_type=MESH)

    loads = []
    for at, (src, dst) in enumerate((
            (xb, raw.at[0]), (w1, wraw.at[0]), (xa, raw.at[1]), (go, raw.at[2]),
            (w2, wraw.at[1]), (g1, gains.at[0]), (b1, gains.at[1]), (g2, gains.at[2]),
            (b2, gains.at[3]))):
        copy = pltpu.make_async_copy(src, dst, load_sem.at[at])
        copy.start()
        loads.append(copy)

    inside = []
    for k in range(3):
        inside.append({-1: me[k] > 0, 0: None, 1: me[k] < sizes[k] - 1})

    def reaches(offset):
        known = [inside[k][o] for k, o in enumerate(offset) if o]
        flag = known[0]
        for more in known[1:]:
            flag = jnp.logical_and(flag, more)
        return flag

    def halo_copies(v, offset, centred):
        to = ids([me[k] + o for k, o in enumerate(offset)])

        def remote(src, dst, m):
            return pltpu.make_async_remote_copy(
                src_ref=src, dst_ref=dst, send_sem=halo_send.at[v, m],
                recv_sem=halo_recv.at[v, m], device_id=to, device_id_type=MESH)

        found = []
        if centred or offset[2]:
            found.append(remote(edge_out.at[v], edge_in.at[v, code(offset)], code(offset)))
        if not offset[2]:
            def cut(o, n):
                if o == 0:
                    return pl.ds(1, n), pl.ds(1, n)
                return (n, 0) if o > 0 else (1, n + 1)
            (sx, dx), (sy, dy) = cut(offset[0], nx), cut(offset[1], ny)
            m = 27 + (offset[0] + 1) * 3 + offset[1] + 1
            found.append(remote(pads.at[v, sx, sy], pads.at[v, dx, dy], m))
        return found

    order = sorted(OFFSETS, key=lambda o: (o[2] == 0, o[1] == 0 and o[2] == 0))

    def halo_start(v, centred=False):
        for offset in order:
            @pl.when(reaches(offset))
            def _(offset=offset):
                for copy in halo_copies(v, offset, centred):
                    copy.start()

    def halo_wait(v, centred=False):
        for offset in order:
            @pl.when(reaches(offset))
            def _(offset=offset):
                for copy in halo_copies(v, offset, centred):
                    copy.wait_send()
                for copy in halo_copies(v, minus(offset), centred):
                    copy.wait_recv()

    def total(value):
        return jnp.sum(value, axis=1, keepdims=True)

    def turned(tile, by):
        return pltpu.roll(tile, by, 1)

    def emit(v, tile_of, centre=None):
        def step(x, edge):
            for y in range(ny):
                tile = tile_of(x, y)
                if centre is not None:
                    tile = tile - centre
                pads[v, x + 1, y + 1] = tile.astype(bf16)
                r = x * ny + y
                edge = jnp.where(lane == r, tile[:, 0:1], edge)
                edge = jnp.where(lane == own + r, tile[:, nz - 1:nz], edge)
            return edge
        edge = lax.fori_loop(0, nx, step, zero if centre is None else centre)
        edge_out[v] = edge.astype(bf16)

    def edge_tile(v, near, centred):
        tile = edge_in[v, code(minus(near))].astype(f32)
        return tile + tile[:, nz - 1:nz] if centred else tile

    def collect_columns(v, centred=False):
        for side in range(2):
            dz = 2 * side - 1
            first = 0 if side else own
            for dx in (-1, 0, 1):
                left, mid, right = [edge_tile(v, (dx, dy, dz), centred) for dy in (-1, 0, 1)]
                for x in ((0,), range(1, nx + 1), (nx + 1,))[dx + 1]:
                    base = first + (nx - 1, x - 1, 0)[dx + 1] * ny
                    tile = turned(mid, (1 - base) % nz)
                    tile = jnp.where(lane == 0, turned(left, (1 - base - ny) % nz), tile)
                    tile = jnp.where(lane == ny + 1, turned(right, (ny + 1 - base) % nz), tile)
                    cols[v, x, side] = tile

    def halo_rows(fn):
        def step(y, carry):
            fn(0, y, (-1, 0, 0))
            fn(nx + 1, y, (1, 0, 0))
            return carry
        lax.fori_loop(1, ny + 1, step, 0)
        for y, dy in ((0, -1), (ny + 1, 1)):
            for x in range(nx + 2):
                fn(x, y, (-1 if x == 0 else 1 if x == nx + 1 else 0, dy, 0))

    def collect_centred(v, full):
        collect_columns(v, True)
        centres = {}
        for dx in (-1, 0, 1):
            for dy in (-1, 0, 1):
                if dx or dy:
                    tile = edge_in[v, code((-dx, -dy, 0))].astype(f32)
                    centres[dx, dy, 0] = jnp.broadcast_to(tile[:, nz - 1:nz], zero.shape)

        def fn(x, y, near):
            full[x, y] = pads[v, x, y].astype(f32) + centres[near]
        halo_rows(fn)

    def build(tile_of, shifted, turn):
        low_y = jnp.where(me[1] > 0, 0, 1)
        high_y = jnp.where(me[1] < sizes[1] - 1, wide, wide - 1)

        def step(x, carry):
            x_ok = jnp.logical_and(
                jnp.logical_or(x > 0, me[0] > 0),
                jnp.logical_or(x < nx + 1, me[0] < sizes[0] - 1))
            ok = {1: x_ok, 0: jnp.logical_and(x_ok, me[1] > 0),
                  2: jnp.logical_and(x_ok, me[1] < sizes[1] - 1)}
            some = {k: jnp.where(f, nz, 0) for k, f in ok.items()}
            sides = []
            for side, flag in ((0, me[2] > 0), (1, me[2] < sizes[2] - 1)):
                last = jnp.where(jnp.logical_and(x_ok, flag), high_y, 0)
                keep = jnp.logical_and(lane >= low_y, lane < last)
                sides.append(jnp.where(keep, tile_of(x, wide + side), 0.0))
            for y in range(wide):
                limit = some[0 if y == 0 else 2 if y == wide - 1 else 1]
                tile = jnp.where(lane < limit, tile_of(x, y), 0.0)
                low = jnp.where(lane == 0, turned(sides[0], (nz - y) % nz), turned(tile, 1))
                high = jnp.where(
                    lane == nz - 1, turned(sides[1], nz - 1 - y), turned(tile, nz - 1))
                row = x * wide + y
                shifted[row, 0:chan] = (high if turn else low).astype(bf16)
                shifted[row, chan:2 * chan] = tile.astype(bf16)
                shifted[row, 2 * chan:] = (low if turn else high).astype(bf16)
            return carry
        lax.fori_loop(0, nx + 2, step, 0)

    def at(full, v):
        def tile_of(x, y):
            return cols[v, x, y - wide] if isinstance(y, int) and y >= wide else full[x, y]
        return tile_of

    def at_pads(v):
        def tile_of(x, y):
            if isinstance(y, int) and y >= wide:
                return cols[v, x, y - wide]
            return pads[v, x, y].astype(f32)
        return tile_of

    def stacked(shifted, x, y, n, turn=False):
        parts = []
        for tx in range(3):
            for ty in range(3):
                row = (x + (2 - tx if turn else tx)) * wide + y + (2 - ty if turn else ty)
                parts.append(jnp.concatenate([shifted[row + u] for u in range(n)], axis=1))
        return jnp.concatenate(parts, axis=0)

    def conv_rows(shifted, w, turn, finish, init):
        def step(i, carry):
            x, y0 = i // (ny // DEEP), (i % (ny // DEEP)) * DEEP
            for p in range(0, DEEP, GROUP):
                o = jnp.dot(w, stacked(shifted, x, y0 + p, GROUP, turn),
                            preferred_element_type=f32)
                for u in range(GROUP):
                    carry = finish(x, y0 + p + u, o[:, u * nz:(u + 1) * nz], carry)
            return carry
        return lax.fori_loop(0, nx * (ny // DEEP), step, init)

    def conv_stats(shifted, w, full, shift):
        def finish(x, y, o, carry):
            full[x + shift, y + shift] = o
            return carry[0] + o, carry[1] + o * o
        return conv_rows(shifted, w, False, finish, (zero, zero))

    def row_of(values):
        tile = zero
        for k, value in enumerate(values):
            tile = jnp.where(lane == k * chan + chan_of, value, tile)
        return jnp.sum(tile, axis=0, keepdims=True)

    def column(row, k):
        return total(jnp.where(lane == k * chan + chan_of, row, 0.0))

    def spread(value):
        return jnp.broadcast_to(value, zero.shape)

    def all_start(buf, value, j, send, recv):
        buf[rank] = value
        for offset in others:
            to = at_offset(offset)
            pltpu.make_async_remote_copy(
                src_ref=buf.at[rank], dst_ref=buf.at[rank], send_sem=send.at[j],
                recv_sem=recv.at[j], device_id=ids(to), device_id_type=MESH).start()

    def wait_bytes(buf, sem):
        some = buf.at[pl.ds(0, count - 1)]
        pltpu.make_async_copy(some, some, sem).wait()

    def tree(values):
        while len(values) > 1:
            values = [values[i] + values[i + 1] if i + 1 < len(values) else values[i]
                      for i in range(0, len(values), 2)]
        return values[0]

    def sums_start(j, values):
        all_start(slots.at[j], row_of([total(v) for v in values]), j, sum_send, sum_recv)

    def sums_finish(j):
        wait_bytes(slots.at[j], sum_recv.at[j])
        wait_bytes(slots.at[j], sum_send.at[j])
        return tree([slots[j, r] for r in range(count)])

    def norm(row):
        mean = column(row, 0) / voxels
        var = column(row, 1) / voxels - mean * mean
        return spread(mean), spread(lax.rsqrt(var + EPSILON))

    def centre_of(sums):
        return spread(total(sums[0]) / local).astype(bf16).astype(f32)

    def weights_start(j, value):
        tiles = value.shape[1] // nz
        for u in range(tiles * (chan // 8)):
            r, t = u // tiles, u % tiles
            wunit[j, u // units, pl.ds((u % units) * 8, 8)] = value[
                r * 8:r * 8 + 8, t * nz:(t + 1) * nz]
        wslot[j, rank] = wunit[j, rank]
        for offset in others:
            to = at_offset(offset)
            r = (to[0] * sizes[1] + to[1]) * sizes[2] + to[2]
            pltpu.make_async_remote_copy(
                src_ref=wunit.at[j, r], dst_ref=wslot.at[j, rank], send_sem=w_send.at[j],
                recv_sem=w_recv.at[j], device_id=ids(to), device_id_type=MESH).start()

    def weights_share(j):
        wait_bytes(wslot.at[j], w_recv.at[j])
        wait_bytes(wslot.at[j], w_send.at[j])
        value = tree([wslot[j, r] for r in range(count)]) * factor
        all_start(wfull.at[j], value, 2 + j, w_send, w_recv)

    def weights_finish(j, out):
        wait_bytes(wfull.at[j], w_recv.at[2 + j])
        wait_bytes(wfull.at[j], w_send.at[2 + j])
        tiles = wsum.shape[1] // nz
        for u in range(tiles * (chan // 8)):
            r, t = u // tiles, u % tiles
            piece = wfull[j, u // units, pl.ds((u % units) * 8, 8)]
            for k in range(nz // chan):
                tap = t * (nz // chan) + k
                if tap < 27:
                    out[tap, pl.ds(r * 8, 8)] = piece[:, k * chan:(k + 1) * chan]

    def wgrad(shifted_d, shifted):
        wsum[...] = jnp.zeros(wsum.shape, f32)

        def step(i, carry):
            x, y = i // (ny // DEEP), (i % (ny // DEEP)) * DEEP
            row = (x + 1) * wide + y + 1
            delta = jnp.concatenate(
                [shifted_d[row + u, chan:2 * chan] for u in range(DEEP)], axis=1)
            wsum[:, 0:27 * chan] += lax.dot_general(
                delta, stacked(shifted, x, y, DEEP), (((1,), (1,)), ((), ())),
                preferred_element_type=f32)
            return carry
        lax.fori_loop(0, nx * (ny // DEEP), step, 0)
        return wsum[...]

    def take(k):
        def step(c, carry):
            at_row = pl.multiple_of(c * pitch, 8)
            for x in range(nx):
                tall[pl.ds(at_row + x * ny, ny)] = raw[k, c, x].astype(f32)
            return carry
        lax.fori_loop(0, chan, step, 0, unroll=4)

        def tile_of(x, y):
            return tall[pl.ds(x * ny + y, chan, stride=pitch)]
        return tile_of

    def give(out):
        def step(c, carry):
            at_row = pl.multiple_of(c * pitch, 8)
            for x in range(nx):
                out[c, x] = tall[pl.ds(at_row + x * ny, ny)].astype(bf16)
            return carry
        lax.fori_loop(0, chan, step, 0, unroll=4)

    def put_row(x, y, tile):
        tall[pl.ds(x * ny + y, chan, stride=pitch)] = tile

    def prepare(k):
        taps = [wraw[k, t].astype(f32) for t in range(27)]
        mats[2 * k] = jnp.concatenate(taps, axis=1).astype(bf16)
        mats[2 * k + 1] = jnp.concatenate(taps, axis=0).T.astype(bf16)

    loads[0].wait()
    emit(XB, take(0))
    pl.semaphore_wait(barrier, count - 1)
    halo_start(XB)
    loads[2].wait()
    emit(XA, take(1))
    halo_start(XA)
    loads[3].wait()
    emit(GO, take(2))
    halo_start(GO)
    loads[1].wait()
    prepare(0)
    loads[4].wait()
    prepare(1)
    for k in range(5, 9):
        loads[k].wait()

    def gain(k):
        value = spread(jnp.concatenate([gains[k]] * (nz // chan), axis=1))
        return spread(column(value, 0))
    gain_one, bias_one, gain_two, bias_two = [gain(k) for k in range(4)]

    halo_wait(XB)
    collect_columns(XB)
    build(at_pads(XB), shift_xb, False)
    sums = conv_stats(shift_xb, mats[0], f1b, 1)
    sums_start(0, sums)
    emit(C1B, lambda x, y: f1b[x + 1, y + 1], centre_of(sums))
    halo_start(C1B, True)

    halo_wait(XA)
    collect_columns(XA)
    build(at_pads(XA), shift_a, False)
    sums = conv_stats(shift_a, mats[0], f1a, 1)
    sums_start(1, sums)
    emit(C1A, lambda x, y: f1a[x + 1, y + 1], centre_of(sums))
    halo_start(C1A, True)

    def silu(z):
        return z * jax.nn.sigmoid(z)

    halo_wait(C1B, True)
    collect_centred(C1B, f1b)
    mean_one, scale_one = norm(sums_finish(0))
    steep_one = gain_one * scale_one
    tile_1b = at(f1b, C1B)

    def z_one(x, y):
        return (tile_1b(x, y) - mean_one) * steep_one + bias_one
    build(lambda x, y: silu(z_one(x, y)), shift_hb, False)
    sums = conv_stats(shift_hb, mats[2], f2b, 1)
    sums_start(2, sums)
    emit(C2B, lambda x, y: f2b[x + 1, y + 1], centre_of(sums))
    halo_start(C2B, True)

    halo_wait(C1A, True)
    collect_centred(C1A, f1a)
    mean_a, scale_a = norm(sums_finish(1))
    steep_a = gain_one * scale_a
    tile_1a = at(f1a, C1A)
    build(lambda x, y: silu((tile_1a(x, y) - mean_a) * steep_a + bias_one), shift_a, False)
    sums_start(3, conv_stats(shift_a, mats[2], c2a, 0))

    halo_wait(GO)
    collect_columns(GO)
    halo_wait(C2B, True)
    collect_centred(C2B, f2b)
    mean_two, scale_two = norm(sums_finish(2))
    steep_two = gain_two * scale_two
    tile_2b = at(f2b, C2B)
    tile_go = at_pads(GO)

    def d_two(x, y):
        return tile_go(x, y) * slope_of((tile_2b(x, y) - mean_two) * steep_two + bias_two)

    def own_two(x, carry):
        sd, sx = carry
        for y in range(1, ny + 1):
            d = d_two(x, y)
            fd2[x, y] = d
            sd, sx = sd + d, sx + d * (tile_2b(x, y) - mean_two)
        return sd, sx
    sd, sx = lax.fori_loop(1, nx + 1, own_two, (zero, zero))
    sums_start(4, (sx * scale_two, sd))

    def halo_two(x, y, near):
        fd2[x, y] = d_two(x, y)
    halo_rows(halo_two)
    for x in range(nx + 2):
        for side in range(2):
            cols[D2, x, side] = d_two(x, wide + side)

    mean_a2, scale_a2 = norm(sums_finish(3))
    steep_a2 = gain_two * scale_a2

    def finish_a(x, carry):
        for y in range(ny):
            put_row(x, y, silu((c2a[x, y] - mean_a2) * steep_a2 + bias_two))
        return carry
    lax.fori_loop(0, nx, finish_a, 0)
    give(ya)

    row_two = sums_finish(4)
    sx2 = spread(column(row_two, 0) / voxels) * scale_two
    sd2 = spread(column(row_two, 1) / voxels)
    tile_d2 = at(fd2, D2)
    build(lambda x, y: steep_two * (tile_d2(x, y) - sd2 - (tile_2b(x, y) - mean_two) * sx2),
          shift_d, True)

    def back(x, y, o, carry):
        sd, sx = carry
        e1[x, y] = o
        d = o * slope_of(z_one(x + 1, y + 1))
        fd1[x + 1, y + 1] = d
        return sd + d, sx + d * (tile_1b(x + 1, y + 1) - mean_one)
    sd, sx = conv_rows(shift_d, mats[3], True, back, (zero, zero))
    sums_start(5, (sx * scale_one, sd))
    emit(E1, lambda x, y: e1[x, y])
    halo_start(E1)
    weights_start(0, wgrad(shift_d, shift_hb))

    halo_wait(E1)
    collect_columns(E1)

    def halo_one(x, y, near):
        fd1[x, y] = pads[E1, x, y].astype(f32) * slope_of(z_one(x, y))
    halo_rows(halo_one)
    for x in range(nx + 2):
        for side in range(2):
            cols[D1, x, side] = cols[E1, x, side] * slope_of(z_one(x, wide + side))

    row_one = sums_finish(5)
    sx1 = spread(column(row_one, 0) / voxels) * scale_one
    sd1 = spread(column(row_one, 1) / voxels)
    tile_d1 = at(fd1, D1)
    build(lambda x, y: steep_one * (tile_d1(x, y) - sd1 - (tile_1b(x, y) - mean_one) * sx1),
          shift_d, True)
    weights_start(1, wgrad(shift_d, shift_xb))
    weights_share(0)

    def last(x, y, o, carry):
        put_row(x, y, o)
        return carry
    conv_rows(shift_d, mats[1], True, last, 0)
    give(dxb)
    for k, row in enumerate((row_one, row_two)):
        for j in range(2):
            gnorm[2 * k + j:2 * k + j + 1, :] = row[:, j * chan:(j + 1) * chan] * factor
    weights_finish(0, gw2)
    weights_share(1)
    weights_finish(1, gw1)


def deliver(*refs):
    sem = refs[-1]
    half = (len(refs) - 1) // 2
    copies = [pltpu.make_async_copy(src, dst, sem.at[k])
              for k, (src, dst) in enumerate(zip(refs[:half], refs[half:-1]))]
    for copy in copies:
        copy.start()
    for copy in copies:
        copy.wait()


def body(sizes, x_a, x_b, w_first, w_second, gain_first, bias_first, gain_second, bias_second,
         grad_out):
    chan, nx, ny, nz = x_a.shape
    count = math.prod(sizes)
    voxels = float(nx * ny * nz * count)
    taps = 27 * chan
    bf16, f32 = jnp.bfloat16, jnp.float32
    tiles = -(-taps // nz)
    units = -(-tiles * (chan // 8) // count)
    full = (nx + 2, ny + 2, chan, nz)
    span = (nx + 2) * (ny + 2)
    grid = (nx, ny, chan, nz)
    vmem = pl.BlockSpec(memory_space=pltpu.VMEM)
    hbm = pl.BlockSpec(memory_space=pl.ANY)
    dma = pltpu.SemaphoreType.DMA
    shapes = (
        jax.ShapeDtypeStruct(x_a.shape, bf16),
        jax.ShapeDtypeStruct(x_a.shape, bf16),
        jax.ShapeDtypeStruct((27, chan, chan), f32),
        jax.ShapeDtypeStruct((27, chan, chan), f32),
        jax.ShapeDtypeStruct((4, chan), f32),
    )
    results = pl.pallas_call(
        functools.partial(kernel, sizes, voxels, units),
        out_shape=shapes,
        in_specs=[hbm] * 9,
        out_specs=[vmem] * 5,
        scratch_shapes=[
            pltpu.VMEM((3, chan, nx, ny, nz), bf16),
            pltpu.VMEM((2, 27, chan, chan), bf16),
            pltpu.VMEM((4, 1, chan), f32),
            pltpu.VMEM((chan * (nx * ny + 8), nz), f32),
            pltpu.VMEM((4, chan, taps), bf16),
            pltpu.VMEM((7,) + full, bf16),
            pltpu.VMEM((7, chan, nz), bf16),
            pltpu.VMEM((7, 27, chan, nz), bf16),
            pltpu.VMEM((9, nx + 2, 2, chan, nz), f32),
        ] + [pltpu.VMEM((span, 3 * chan, nz), bf16)] * 4
        + [pltpu.VMEM(full, f32)] * 5
        + [pltpu.VMEM(grid, f32)] * 2
        + [
            pltpu.VMEM((6, count, 1, nz), f32),
            pltpu.VMEM((chan, tiles * nz), f32),
            pltpu.VMEM((2, count, 8 * units, nz), f32),
            pltpu.VMEM((2, count, 8 * units, nz), f32),
            pltpu.VMEM((2, count, 8 * units, nz), f32),
            dma((9,)),
            dma((7, 36)), dma((7, 36)),
            dma((6,)), dma((6,)),
            dma((4,)), dma((4,)),
        ],
        compiler_params=pltpu.CompilerParams(
            collective_id=0, has_side_effects=True, vmem_limit_bytes=56 * 1024 * 1024),
    )(
        x_a, x_b, grad_out,
        w_first.reshape(27, chan, chan), w_second.reshape(27, chan, chan),
        gain_first.reshape(1, chan), bias_first.reshape(1, chan),
        gain_second.reshape(1, chan), bias_second.reshape(1, chan),
    )
    y_a, dx_b, gw1, gw2, gnorm = pl.pallas_call(
        deliver,
        out_shape=shapes,
        in_specs=[vmem] * 5,
        out_specs=[hbm] * 5,
        scratch_shapes=[dma((5,))],
    )(*results)
    cube = (3, 3, 3, chan, chan)
    return y_a, dx_b, gw1.reshape(cube), gw2.reshape(cube), gnorm


def solution(mesh):
    sizes = tuple(mesh.shape[a] for a in AXES)
    split = P(None, *AXES)
    return jax.shard_map(
        functools.partial(body, sizes),
        mesh=mesh,
        in_specs=(split, split, P(), P(), P(), P(), P(), P(), split),
        out_specs=(split, split, P(), P(), P()),
        check_vma=False,
    )
```

```python
import functools
import math

import jax
import jax.numpy as jnp
from jax import lax
from jax.experimental import pallas as pl
from jax.experimental.pallas import tpu as pltpu
from jax.sharding import PartitionSpec as P

EPSILON = 1e-05
AXES = ("gx", "gy", "gz")
MESH = pl.DeviceIdType.MESH
XB, XA, GO, C1B, C1A, C2B, E1 = range(7)
D2, D1 = range(2)
OFFSETS = [(a, b, c) for a in (-1, 0, 1) for b in (-1, 0, 1) for c in (-1, 0, 1)
           if (a, b, c) != (0, 0, 0)]
DEEP = 4


def slope_of(z):
    s = jax.nn.sigmoid(z)
    return s * (1.0 + z * (1.0 - s))


def code(offset):
    a, b, c = offset
    return (a + 1) * 9 + (b + 1) * 3 + c + 1


def minus(offset):
    return tuple(-o for o in offset)


def kernel(
    sizes, voxels, units,
    xa, xb, go, w1, w2, g1, b1, g2, b2,
    ya, dxb, gw1, gw2, gnorm,
    raw, wraw, gains, tall, mats, pads, edge_out, edge_in, cols, dcols, offs,
    shift_xb, shift_a, shift_hb, shift_d,
    fd2, fd1, c1b, c1a, c2b, c2a, e1, d1h, slots, xsum, xfull, kcol, wsum,
    unit_h, slot_h, unit_f, slot_f, wfull,
    load_sem, halo_send, halo_recv, sum_send, sum_recv, w_send, w_recv,
):
    chan, nx, ny, nz = raw.shape[1:]
    wide = ny + 2
    own = nx * ny
    pitch = tall.shape[0] // chan
    count = math.prod(sizes)
    local = float(own * nz)
    factor = 1.0 / math.sqrt(voxels)
    tiles = wsum.shape[1] // nz
    me = [lax.axis_index(a) for a in AXES]

    def rank_of(place):
        return (place[0] * sizes[1] + place[1]) * sizes[2] + place[2]
    rank = rank_of(me)
    lane = lax.broadcasted_iota(jnp.int32, (chan, nz), 1)
    chan_of = lax.broadcasted_iota(jnp.int32, (chan, nz), 0)
    odd = lax.rem(lane, 2) == 1
    zero = jnp.zeros((chan, nz), jnp.float32)
    bf16, f32 = jnp.bfloat16, jnp.float32

    others = [(a, b, c) for a in range(sizes[0]) for b in range(sizes[1])
              for c in range(sizes[2])][1:]

    def at_offset(offset):
        return [lax.rem(m + o + s, s) for m, o, s in zip(me, offset, sizes)]

    def ids(place):
        return dict(zip(AXES, place))

    barrier = pltpu.get_barrier_semaphore()
    for offset in others:
        pl.semaphore_signal(
            barrier, inc=1, device_id=ids(at_offset(offset)), device_id_type=MESH)

    loads = []
    for at, (src, dst) in enumerate((
            (xb, raw.at[0]), (w1, wraw.at[0]), (xa, raw.at[1]), (go, raw.at[2]),
            (w2, wraw.at[1]), (g1, gains.at[0]), (b1, gains.at[1]), (g2, gains.at[2]),
            (b2, gains.at[3]))):
        copy = pltpu.make_async_copy(src, dst, load_sem.at[at])
        copy.start()
        loads.append(copy)

    inside = []
    for k in range(3):
        inside.append({-1: me[k] > 0, 0: None, 1: me[k] < sizes[k] - 1})

    def reaches(offset):
        known = [inside[k][o] for k, o in enumerate(offset) if o]
        flag = known[0]
        for more in known[1:]:
            flag = jnp.logical_and(flag, more)
        return flag

    def halo_copy(v, offset):
        to = ids([me[k] + o for k, o in enumerate(offset)])
        if offset[2]:
            src, dst = edge_out.at[v], edge_in.at[v, code(offset)]
        else:
            def cut(o, n):
                if o == 0:
                    return pl.ds(1, n), pl.ds(1, n)
                return (n, 0) if o > 0 else (1, n + 1)
            (sx, dx), (sy, dy) = cut(offset[0], nx), cut(offset[1], ny)
            src, dst = pads.at[v, sx, sy], pads.at[v, dx, dy]
        m = code(offset)
        return pltpu.make_async_remote_copy(
            src_ref=src, dst_ref=dst, send_sem=halo_send.at[v, m],
            recv_sem=halo_recv.at[v, m], device_id=to, device_id_type=MESH)

    order = sorted(OFFSETS, key=lambda o: (o[1] == 0 and o[2] == 0, o[0] != 0))
    sides = [o for o in order if o[0] == 0]
    faces = [o for o in order if o[0] != 0]

    def halo_start(v):
        for offset in order:
            @pl.when(reaches(offset))
            def _(offset=offset):
                halo_copy(v, offset).start()

    def halo_wait(v, part):
        for offset in part:
            @pl.when(reaches(offset))
            def _(offset=offset):
                halo_copy(v, offset).wait_send()
                halo_copy(v, minus(offset)).wait_recv()

    def total(value):
        return jnp.sum(value, axis=1, keepdims=True)

    def spread(value):
        return jnp.broadcast_to(value, zero.shape)

    def turned(tile, by):
        by = by % nz
        return pltpu.roll(tile, by, 1) if by else tile

    def emit(v, tile_of, centre=None):
        def step(x, edge):
            for y in range(ny):
                tile = tile_of(x, y)
                if centre is not None:
                    tile = tile - centre
                pads[v, x + 1, y + 1] = tile.astype(bf16)
                r = 2 * (x * ny + y)
                edge = jnp.where(lane == r, tile[:, nz - 1:nz], edge)
                edge = jnp.where(lane == r + 1, tile[:, 0:1], edge)
            return edge
        edge_out[v] = lax.fori_loop(0, nx, step, zero).astype(bf16)

    first_lanes = jnp.logical_or(lane == 0, lane == nz - 1)
    last_lanes = jnp.logical_or(lane == 2 * ny + 1, lane == 2 * ny + 2)

    def by_row(first, middle, last):
        return jnp.where(first_lanes, first, jnp.where(last_lanes, last, middle))

    def collect(v, part):
        for dx in (0,) if part is sides else (-1, 1):
            low, high = [[edge_in[v, code((-dx, -dy, -dz))] for dy in (-1, 0, 1)]
                         for dz in (-1, 1)]
            for x in range(1, nx + 1) if dx == 0 else (0,) if dx < 0 else (nx + 1,):
                base = (nx - 1, x - 1, 0)[dx + 1] * ny
                moves = (-2 * (base + ny), -2 * base, 2 * ny - 2 * base)
                got = [jnp.where(odd, turned(h, by), turned(l, by + 2))
                       for l, h, by in zip(low, high, moves)]
                cols[v, x] = by_row(*got)

    row_of_lane = jnp.where(lane == nz - 1, 0, lax.div(lane + 1, 2))
    low_y = jnp.where(me[1] > 0, 0, 1)
    high_y = jnp.where(me[1] < sizes[1] - 1, wide, wide - 1)
    low_z = jnp.where(me[2] > 0, 1, 0)
    high_z = jnp.where(me[2] < sizes[2] - 1, 1, 0)
    keep_edge = jnp.where(jnp.logical_and(row_of_lane >= low_y, row_of_lane < high_y),
                          jnp.where(odd, high_z, low_z), 0)

    def build(tile_of, shifted, turn, part):
        inner = part is sides

        def step(i, carry):
            if inner:
                x, x_ok = i + 1, None
            else:
                x = i * (nx + 1)
                x_ok = jnp.where(i == 0, me[0], sizes[0] - 1 - me[0]) > 0

            def both(flag):
                return flag if x_ok is None else jnp.logical_and(x_ok, flag)
            limits = {0: jnp.where(both(me[1] > 0), nz, 0),
                      wide - 1: jnp.where(both(me[1] < sizes[1] - 1), nz, 0)}
            middle = None if inner else jnp.where(x_ok, nz, 0)
            least = 1 if inner else jnp.where(x_ok, 1, 2)
            edge = tile_of(x, wide, inner)
            edge = jnp.where(keep_edge >= least, edge, jnp.zeros_like(edge)).astype(bf16)
            for y in range(wide):
                tile = tile_of(x, y, inner)
                limit = limits.get(y, middle)
                if limit is not None:
                    tile = jnp.where(lane < limit, tile, jnp.zeros_like(tile))
                tile = tile.astype(bf16)
                ends = turned(edge, -2 * y)
                low = jnp.where(lane == 0, ends, turned(tile, 1))
                high = jnp.where(lane == nz - 1, ends, turned(tile, -1))
                row = x * wide + y
                shifted[row, 0:chan] = high if turn else low
                shifted[row, chan:2 * chan] = tile
                shifted[row, 2 * chan:] = low if turn else high
            return carry
        lax.fori_loop(0, nx if inner else 2, step, 0)

    def raw_tiles(v):
        def tile_of(x, y, inner):
            return cols[v, x] if isinstance(y, int) and y == wide else pads[v, x, y]
        return tile_of

    def centred(v, k, full):
        def tile_of(x, y, inner):
            if not isinstance(y, int):
                return pads[v, x, y].astype(f32) + offs[k, x, 1]
            if y == wide:
                return cols[v, x].astype(f32) + offs[k, x, 3]
            if inner and 0 < y < wide - 1:
                return full[x - 1, y - 1] + offs[k, x, 1]
            kind = 0 if y == 0 else 2 if y == wide - 1 else 1
            return pads[v, x, y].astype(f32) + offs[k, x, kind]
        return tile_of

    def halo_rows(fn, part):
        if part is faces:
            def step(i, carry):
                for y in range(wide):
                    fn(i * (nx + 1), y, False)
                return carry
            lax.fori_loop(0, 2, step, 0)
        else:
            for x in range(1, nx + 1):
                for y in (0, wide - 1):
                    fn(x, y, True)

    def xs_of(part):
        return range(1, nx + 1) if part is sides else (0, nx + 1)

    def stack_rows(shifted, a, y, deep):
        parts = []
        for yi in range(deep + 2):
            parts.append(jnp.concatenate(
                [shifted[(x + a) * wide + y + yi] for x in range(nx)], axis=1))
        return parts

    def conv_rows(shifted, w, finish, init):
        def step(i, carry):
            y0 = i * DEEP
            data = jnp.concatenate(
                [p for a in range(3) for p in stack_rows(shifted, a, y0, DEEP)], axis=0)
            o = jnp.dot(mats[w], data, preferred_element_type=f32)
            for x in range(nx):
                for u in range(DEEP):
                    carry = finish(
                        x, y0 + u, o[u * chan:(u + 1) * chan, x * nz:(x + 1) * nz], carry)
            return carry
        return lax.fori_loop(0, ny // DEEP, step, init, unroll=2)

    def conv_stats(shifted, w, full):
        def finish(x, y, o, carry):
            full[x, y] = o
            return carry[0] + o, carry[1] + o * o
        return conv_rows(shifted, w, finish, (zero, zero))

    def row_of(values):
        tile = zero
        for k, value in enumerate(values):
            tile = jnp.where(lane == k * chan + chan_of, value, tile)
        return jnp.sum(tile, axis=0, keepdims=True)

    def column(row, k):
        return total(jnp.where(lane == k * chan + chan_of, row, 0.0))

    def all_start(buf, value, send, recv):
        buf[rank] = value
        for offset in others:
            pltpu.make_async_remote_copy(
                src_ref=buf.at[rank], dst_ref=buf.at[rank], send_sem=send,
                recv_sem=recv, device_id=ids(at_offset(offset)), device_id_type=MESH).start()

    def wait_bytes(buf, *sems):
        some = buf.at[pl.ds(0, count - 1)]
        for sem in sems:
            pltpu.make_async_copy(some, some, sem).wait()

    def tree(values):
        while len(values) > 1:
            values = [values[i] + values[i + 1] if i + 1 < len(values) else values[i]
                      for i in range(0, len(values), 2)]
        return values[0]

    def sums_start(j, values):
        all_start(slots.at[j], row_of([total(v) for v in values]), sum_send.at[j],
                  sum_recv.at[j])

    def sums_finish(j):
        wait_bytes(slots.at[j], sum_recv.at[j], sum_send.at[j])
        return tree([slots[j, r] for r in range(count)])

    def norm(row):
        mean = column(row, 0) / voxels
        var = column(row, 1) / voxels - mean * mean
        return spread(mean), spread(lax.rsqrt(var + EPSILON))

    def rounded(value):
        return spread(value / local).astype(bf16).astype(f32)

    def centre_of(sums):
        return rounded(total(sums[0]))

    def set_offsets(k, j, mean, part):
        def off(offset):
            return rounded(column(slots[j, rank_of(at_offset(offset))], 0)) - mean
        for dx in (0,) if part is sides else (-1, 1):
            rows = [-mean if dx == 0 and dy == 0 else off((dx, dy, 0)) for dy in (-1, 0, 1)]
            edges = by_row(*[jnp.where(odd, off((dx, dy, 1)), off((dx, dy, -1)))
                             for dy in (-1, 0, 1)])
            for x in range(1, nx + 1) if dx == 0 else (0,) if dx < 0 else (nx + 1,):
                for kind, value in enumerate(rows + [edges]):
                    offs[k, x, kind] = value

    def pieces(value):
        for u in range(tiles * (chan // 8)):
            r, t = u // tiles, u % tiles
            yield u // units, (u % units) * 8, r, t

    def spread_units(unit, slot, send, recv):
        for place, at, r, t in pieces(wsum):
            unit[place, pl.ds(at, 8)] = wsum[
                r * 8:r * 8 + 8, t * nz:(t + 1) * nz].astype(unit.dtype)
        slot[rank] = unit[rank]
        for offset in others:
            to = at_offset(offset)
            pltpu.make_async_remote_copy(
                src_ref=unit.at[rank_of(to)], dst_ref=slot.at[rank], send_sem=send,
                recv_sem=recv, device_id=ids(to), device_id_type=MESH).start()

    def gather_units(slot, send, recv):
        wait_bytes(slot, recv, send)
        return tree([slot[r].astype(f32) for r in range(count)])

    def share(j, value):
        all_start(wfull.at[j], value.astype(bf16), w_send.at[j], w_recv.at[j])

    def spell(j, out):
        wait_bytes(wfull.at[j], w_recv.at[j], w_send.at[j])
        for place, at, r, t in pieces(wsum):
            piece = wfull[j, place, pl.ds(at, 8)].astype(f32)
            for k in range(nz // chan):
                tap = t * (nz // chan) + k
                if tap < 27:
                    out[tap, pl.ds(r * 8, 8)] = piece[:, k * chan:(k + 1) * chan]

    def wgrad(delta_of, shifted, ones=False):
        cuts = []
        for g in range(ny // DEEP):
            for x in range(nx):
                parts = [delta_of(x, g * DEEP + u) for u in range(DEEP)]
                if ones:
                    parts.append(jnp.ones((16, nz), bf16))
                cuts.append(jnp.concatenate(parts, axis=0))
        delta = jnp.concatenate(cuts, axis=1)
        span = 3 * chan
        for a in range(3):
            groups = [jnp.concatenate(stack_rows(shifted, a, g * DEEP, DEEP), axis=0)
                      for g in range(ny // DEEP)]
            o = lax.dot_general(
                delta, jnp.concatenate(groups, axis=1), (((1,), (1,)), ((), ())),
                preferred_element_type=f32)
            for ty in range(3):
                at = (a * 3 + ty) * span
                wsum[:, at:at + span] = tree(
                    [o[u * chan:(u + 1) * chan, (u + ty) * span:(u + ty + 1) * span]
                     for u in range(DEEP)])
                if ones:
                    xsum[:, at:at + span] = tree(
                        [o[DEEP * chan:DEEP * chan + 1, (u + ty) * span:(u + ty + 1) * span]
                         for u in range(DEEP)])

    def take(k):
        def step(c, carry):
            at_row = pl.multiple_of(c * pitch, 8)
            for x in range(nx):
                tall[pl.ds(at_row + x * ny, ny)] = raw[k, c, x].astype(f32)
            return carry
        lax.fori_loop(0, chan, step, 0, unroll=4)

        def tile_of(x, y):
            return tall[pl.ds(x * ny + y, chan, stride=pitch)]
        return tile_of

    def give(out):
        def step(c, carry):
            at_row = pl.multiple_of(c * pitch, 8)
            for x in range(nx):
                out[c, x] = tall[pl.ds(at_row + x * ny, ny)].astype(bf16)
            return carry
        lax.fori_loop(0, chan, step, 0, unroll=4)

    def put_row(x, y, tile):
        tall[pl.ds(x * ny + y, chan, stride=pitch)] = tile

    def prepare(k):
        taps = [wraw[k, t].astype(f32) for t in range(27)]
        span = 3 * chan
        for turn in range(2):
            flat = jnp.concatenate(taps, axis=0).T if turn else jnp.concatenate(taps, axis=1)
            none = jnp.zeros((chan, span), f32)
            for u in range(DEEP):
                parts = []
                for a in range(3):
                    for yi in range(DEEP + 2):
                        tx, ty = (2 - a, 2 - yi + u) if turn else (a, yi - u)
                        at = (tx * 3 + ty) * span
                        parts.append(flat[:, at:at + span] if 0 <= ty < 3 else none)
                mats[2 * k + turn, u * chan:(u + 1) * chan] = jnp.concatenate(
                    parts, axis=1).astype(bf16)

    loads[0].wait()
    emit(XB, take(0))
    pl.semaphore_wait(barrier, count - 1)
    halo_start(XB)
    loads[2].wait()
    emit(XA, take(1))
    halo_start(XA)
    loads[3].wait()
    emit(GO, take(2))
    loads[1].wait()
    prepare(0)
    loads[4].wait()
    prepare(1)
    for k in range(5, 9):
        loads[k].wait()

    def gain(k):
        value = spread(jnp.concatenate([gains[k]] * (nz // chan), axis=1))
        return spread(column(value, 0))
    gain_one, bias_one, gain_two, bias_two = [gain(k) for k in range(4)]

    for part in (sides, faces):
        halo_wait(XB, part)
        collect(XB, part)
        build(raw_tiles(XB), shift_xb, False, part)
    sums = conv_stats(shift_xb, 0, c1b)
    sums_start(0, sums)
    emit(C1B, lambda x, y: c1b[x, y], centre_of(sums))
    halo_start(C1B)

    for part in (sides, faces):
        halo_wait(XA, part)
        collect(XA, part)
        build(raw_tiles(XA), shift_a, False, part)
    sums = conv_stats(shift_a, 0, c1a)
    sums_start(1, sums)
    emit(C1A, lambda x, y: c1a[x, y], centre_of(sums))
    halo_start(C1A)

    def silu(z):
        return z * jax.nn.sigmoid(z)

    mean_one, scale_one = norm(sums_finish(0))
    steep_one = gain_one * scale_one
    tile_1b = centred(C1B, 0, c1b)

    def z_one(x, y, inner):
        return tile_1b(x, y, inner) * steep_one + bias_one
    for part in (sides, faces):
        set_offsets(0, 0, mean_one, part)
        halo_wait(C1B, part)
        collect(C1B, part)
        build(lambda *at: silu(z_one(*at)), shift_hb, False, part)
    sums = conv_stats(shift_hb, 2, c2b)
    sums_start(2, sums)
    emit(C2B, lambda x, y: c2b[x, y], centre_of(sums))
    halo_start(C2B)
    halo_start(GO)

    mean_a, scale_a = norm(sums_finish(1))
    steep_a = gain_one * scale_a
    tile_1a = centred(C1A, 1, c1a)
    for part in (sides, faces):
        set_offsets(1, 1, mean_a, part)
        halo_wait(C1A, part)
        collect(C1A, part)
        build(lambda *at: silu(tile_1a(*at) * steep_a + bias_one), shift_a, False, part)
    sums = conv_stats(shift_a, 2, c2a)
    sums_start(3, sums)

    mean_two, scale_two = norm(sums_finish(2))
    steep_two = gain_two * scale_two

    def own_two(x, carry):
        sd, sx = carry
        for y in range(ny):
            c = c2b[x, y] - mean_two
            d = pads[GO, x + 1, y + 1].astype(f32) * slope_of(c * steep_two + bias_two)
            fd2[x + 1, y + 1] = d
            sd, sx = sd + d, sx + d * c
        return sd, sx
    sd, sx = lax.fori_loop(0, nx, own_two, (zero, zero))
    sums_start(4, (sx * scale_two, sd))

    wgrad(lambda x, y: ((c1b[x, y] - mean_one) * scale_one).astype(bf16), shift_xb, True)
    spread_units(unit_f.at[0], slot_f.at[0], w_send.at[2], w_recv.at[2])
    all_start(xfull, jnp.concatenate(
        [xsum[:, t * nz:(t + 1) * nz] for t in range(tiles)]
        + [jnp.zeros((8 - tiles % 8, nz), f32)], axis=0), w_send.at[3], w_recv.at[3])

    tile_2b = centred(C2B, 2, c2b)
    tile_go = raw_tiles(GO)

    def d_two(*at):
        return tile_go(*at).astype(f32) * slope_of(tile_2b(*at) * steep_two + bias_two)

    def halo_two(x, y, inner):
        fd2[x, y] = d_two(x, y, inner)

    for part in (sides, faces):
        set_offsets(2, 2, mean_two, part)
        halo_wait(C2B, part)
        halo_wait(GO, part)
        collect(C2B, part)
        collect(GO, part)
        halo_rows(halo_two, part)
        for x in xs_of(part):
            dcols[D2, x] = d_two(x, wide, part is sides)

    mean_a2, scale_a2 = norm(sums_finish(3))
    steep_a2 = gain_two * scale_a2

    def finish_a(x, carry):
        for y in range(ny):
            put_row(x, y, silu((c2a[x, y] - mean_a2) * steep_a2 + bias_two))
        return carry
    lax.fori_loop(0, nx, finish_a, 0)
    give(ya)

    row_two = sums_finish(4)
    sx2 = spread(column(row_two, 0) / voxels) * scale_two
    sd2 = spread(column(row_two, 1) / voxels)

    def dc_two(x, y, inner):
        d = dcols[D2, x] if y == wide else fd2[x, y]
        return steep_two * (d - sd2 - tile_2b(x, y, inner) * sx2)
    build(dc_two, shift_d, True, sides)
    build(dc_two, shift_d, True, faces)

    def back(x, y, o, carry):
        sd, sx = carry
        e1[x, y] = o
        c = c1b[x, y] - mean_one
        d = o * slope_of(c * steep_one + bias_one)
        fd1[x + 1, y + 1] = d
        d1h[x, y] = d.astype(bf16)
        return sd + d, sx + d * c
    sd, sx = conv_rows(shift_d, 3, back, (zero, zero))
    sums_start(5, (sx * scale_one, sd))
    wgrad(lambda x, y: d1h[x, y], shift_xb)
    spread_units(unit_f.at[1], slot_f.at[1], w_send.at[4], w_recv.at[4])
    emit(E1, lambda x, y: e1[x, y])
    halo_start(E1)
    wgrad(lambda x, y: shift_d[(x + 1) * wide + y + 1, chan:2 * chan], shift_hb)
    spread_units(unit_h, slot_h, w_send.at[5], w_recv.at[5])
    along = gather_units(slot_f.at[0], w_send.at[2], w_recv.at[2])
    wait_bytes(xfull, w_recv.at[3], w_send.at[3])
    plain = tree([xfull[r] for r in range(count)])
    xfull[rank] = plain

    row_one = sums_finish(5)
    sx1_wide = spread(column(row_one, 0) / voxels)
    sx1 = sx1_wide * scale_one
    sd1 = spread(column(row_one, 1) / voxels)
    for k, value in enumerate((steep_one * factor, sd1, sx1_wide)):
        kcol[k] = value

    def halo_one(x, y, inner):
        fd1[x, y] = pads[E1, x, y].astype(f32) * slope_of(z_one(x, y, inner))

    def dc_one(x, y, inner):
        d = dcols[D1, x] if y == wide else fd1[x, y]
        return steep_one * (d - sd1 - tile_1b(x, y, inner) * sx1)

    halo_wait(E1, sides)
    collect(E1, sides)
    halo_rows(halo_one, sides)
    for x in xs_of(sides):
        dcols[D1, x] = cols[E1, x].astype(f32) * slope_of(z_one(x, wide, True))
    build(dc_one, shift_d, True, sides)

    straight = gather_units(slot_f.at[1], w_send.at[4], w_recv.at[4])
    mixed = []
    for q in range(units):
        u = rank * units + q
        r = pl.multiple_of(jnp.minimum(lax.div(u, tiles), chan // 8 - 1) * 8, 8)
        k, d, x = [kcol[i, pl.ds(r, 8)] for i in range(3)]
        part = slice(q * 8, q * 8 + 8)
        mixed.append(k * (straight[part] - d * xfull[rank, pl.ds(lax.rem(u, tiles), 1)]
                          - x * along[part]))
    share(0, jnp.concatenate(mixed, axis=0))
    share(1, gather_units(slot_h, w_send.at[5], w_recv.at[5]) * factor)

    halo_wait(E1, faces)
    collect(E1, faces)
    halo_rows(halo_one, faces)
    for x in xs_of(faces):
        dcols[D1, x] = cols[E1, x].astype(f32) * slope_of(z_one(x, wide, False))
    build(dc_one, shift_d, True, faces)

    def last(x, y, o, carry):
        put_row(x, y, o)
        return carry
    conv_rows(shift_d, 1, last, 0)
    give(dxb)
    for k, row in enumerate((row_one, row_two)):
        for j in range(2):
            gnorm[2 * k + j:2 * k + j + 1, :] = row[:, j * chan:(j + 1) * chan] * factor
    spell(0, gw1)
    spell(1, gw2)


def deliver(*refs):
    sem = refs[-1]
    half = (len(refs) - 1) // 2
    copies = [pltpu.make_async_copy(src, dst, sem.at[k])
              for k, (src, dst) in enumerate(zip(refs[:half], refs[half:-1]))]
    for copy in copies:
        copy.start()
    for copy in copies:
        copy.wait()


def body(sizes, x_a, x_b, w_first, w_second, gain_first, bias_first, gain_second, bias_second,
         grad_out):
    chan, nx, ny, nz = x_a.shape
    count = math.prod(sizes)
    voxels = float(nx * ny * nz * count)
    taps = 27 * chan
    bf16, f32 = jnp.bfloat16, jnp.float32
    tiles = -(-taps // nz)
    units = -(-tiles * (chan // 8) // count)
    full = (nx + 2, ny + 2, chan, nz)
    span = (nx + 2) * (ny + 2)
    grid = (nx, ny, chan, nz)
    vmem = pl.BlockSpec(memory_space=pltpu.VMEM)
    hbm = pl.BlockSpec(memory_space=pl.ANY)
    dma = pltpu.SemaphoreType.DMA
    shapes = (
        jax.ShapeDtypeStruct(x_a.shape, bf16),
        jax.ShapeDtypeStruct(x_a.shape, bf16),
        jax.ShapeDtypeStruct((27, chan, chan), f32),
        jax.ShapeDtypeStruct((27, chan, chan), f32),
        jax.ShapeDtypeStruct((4, chan), f32),
    )
    results = pl.pallas_call(
        functools.partial(kernel, sizes, voxels, units),
        out_shape=shapes,
        in_specs=[hbm] * 9,
        out_specs=[vmem] * 5,
        scratch_shapes=[
            pltpu.VMEM((3, chan, nx, ny, nz), bf16),
            pltpu.VMEM((2, 27, chan, chan), bf16),
            pltpu.VMEM((4, 1, chan), f32),
            pltpu.VMEM((chan * (nx * ny + 8), nz), f32),
            pltpu.VMEM((4, DEEP * chan, 9 * (DEEP + 2) * chan), bf16),
            pltpu.VMEM((7,) + full, bf16),
            pltpu.VMEM((7, chan, nz), bf16),
            pltpu.VMEM((7, 27, chan, nz), bf16),
            pltpu.VMEM((7, nx + 2, chan, nz), bf16),
            pltpu.VMEM((2, nx + 2, chan, nz), f32),
            pltpu.VMEM((3, nx + 2, 4, chan, nz), f32),
        ] + [pltpu.VMEM((span, 3 * chan, nz), bf16)] * 4
        + [pltpu.VMEM(full, f32)] * 2
        + [pltpu.VMEM(grid, f32)] * 5
        + [
            pltpu.VMEM(grid, bf16),
            pltpu.VMEM((6, count, 1, nz), f32),
            pltpu.VMEM((1, tiles * nz), f32),
            pltpu.VMEM((count, -(-tiles // 8) * 8, nz), f32),
            pltpu.VMEM((3, chan, nz), f32),
            pltpu.VMEM((chan, tiles * nz), f32),
            pltpu.VMEM((count, 8 * units, nz), bf16),
            pltpu.VMEM((count, 8 * units, nz), bf16),
            pltpu.VMEM((2, count, 8 * units, nz), f32),
            pltpu.VMEM((2, count, 8 * units, nz), f32),
            pltpu.VMEM((2, count, 8 * units, nz), bf16),
            dma((9,)),
            dma((7, 27)), dma((7, 27)),
            dma((6,)), dma((6,)),
            dma((6,)), dma((6,)),
        ],
        compiler_params=pltpu.CompilerParams(
            collective_id=0, has_side_effects=True, vmem_limit_bytes=56 * 1024 * 1024),
    )(
        x_a, x_b, grad_out,
        w_first.reshape(27, chan, chan), w_second.reshape(27, chan, chan),
        gain_first.reshape(1, chan), bias_first.reshape(1, chan),
        gain_second.reshape(1, chan), bias_second.reshape(1, chan),
    )
    y_a, dx_b, gw1, gw2, gnorm = pl.pallas_call(
        deliver,
        out_shape=shapes,
        in_specs=[vmem] * 5,
        out_specs=[hbm] * 5,
        scratch_shapes=[dma((5,))],
    )(*results)
    cube = (3, 3, 3, chan, chan)
    return y_a, dx_b, gw1.reshape(cube), gw2.reshape(cube), gnorm


def solution(mesh):
    sizes = tuple(mesh.shape[a] for a in AXES)
    split = P(None, *AXES)
    return jax.shard_map(
        functools.partial(body, sizes),
        mesh=mesh,
        in_specs=(split, split, P(), P(), P(), P(), P(), P(), split),
        out_specs=(split, split, P(), P(), P()),
        check_vma=False,
    )
```

```python
import functools
import math

import jax
import jax.numpy as jnp
from jax import lax
from jax.experimental import pallas as pl
from jax.experimental.pallas import tpu as pltpu
from jax.sharding import PartitionSpec as P

EPSILON = 1e-05
AXES = ("gx", "gy", "gz")
MESH = pl.DeviceIdType.MESH
XB, XA, GO, C1B, C1A, C2B, E1 = range(7)
D2, D1 = range(2)
OFFSETS = [(a, b, c) for a in (-1, 0, 1) for b in (-1, 0, 1) for c in (-1, 0, 1)
           if (a, b, c) != (0, 0, 0)]
DEEP = 4


def slope_of(z):
    s = jax.nn.sigmoid(z)
    return s * (1.0 + z * (1.0 - s))


def code(offset):
    a, b, c = offset
    return (a + 1) * 9 + (b + 1) * 3 + c + 1


def minus(offset):
    return tuple(-o for o in offset)


def kernel(
    sizes, voxels, units,
    xa, xb, go, w1, w2, g1, b1, g2, b2,
    ya, dxb, gw1, gw2, gnorm,
    raw, wraw, gains, tall, mats, pads, edge_out, edge_in, cols, dcols, offs,
    shift_xb, shift_a, shift_hb, shift_d,
    fd2, fd1, c1b, c1a, c2b, c2a, e1, d1h, slots, xsum, plain, kcol, wsum,
    unit_x, slot_x, line_x, unit_f, slot_f, line_f, unit_h, slot_h, line_h, wfull,
    load_sem, halo_send, halo_recv, sum_send, sum_recv, w_send, w_recv,
):
    chan, nx, ny, nz = raw.shape[1:]
    wide = ny + 2
    own = nx * ny
    pitch = tall.shape[0] // chan
    count = math.prod(sizes)
    local = float(own * nz)
    factor = 1.0 / math.sqrt(voxels)
    tiles = wsum.shape[1] // nz
    me = [lax.axis_index(a) for a in AXES]

    def rank_of(place):
        return (place[0] * sizes[1] + place[1]) * sizes[2] + place[2]
    rank = rank_of(me)
    lane = lax.broadcasted_iota(jnp.int32, (chan, nz), 1)
    chan_of = lax.broadcasted_iota(jnp.int32, (chan, nz), 0)
    odd = lax.rem(lane, 2) == 1
    zero = jnp.zeros((chan, nz), jnp.float32)
    bf16, f32 = jnp.bfloat16, jnp.float32

    others = [(a, b, c) for a in range(sizes[0]) for b in range(sizes[1])
              for c in range(sizes[2])][1:]

    def at_offset(offset):
        return [lax.rem(m + o + s, s) for m, o, s in zip(me, offset, sizes)]

    def ids(place):
        return dict(zip(AXES, place))

    barrier = pltpu.get_barrier_semaphore()
    for offset in others:
        pl.semaphore_signal(
            barrier, inc=1, device_id=ids(at_offset(offset)), device_id_type=MESH)

    loads = []
    for at, (src, dst) in enumerate((
            (xb, raw.at[0]), (w1, wraw.at[0]), (xa, raw.at[1]), (go, raw.at[2]),
            (w2, wraw.at[1]), (g1, gains.at[0]), (b1, gains.at[1]), (g2, gains.at[2]),
            (b2, gains.at[3]))):
        copy = pltpu.make_async_copy(src, dst, load_sem.at[at])
        copy.start()
        loads.append(copy)

    inside = []
    for k in range(3):
        inside.append({-1: me[k] > 0, 0: None, 1: me[k] < sizes[k] - 1})

    def reaches(offset):
        known = [inside[k][o] for k, o in enumerate(offset) if o]
        flag = known[0]
        for more in known[1:]:
            flag = jnp.logical_and(flag, more)
        return flag

    def halo_copy(v, offset):
        to = ids([me[k] + o for k, o in enumerate(offset)])
        if offset[2]:
            src, dst = edge_out.at[v], edge_in.at[v, code(offset)]
        else:
            def cut(o, n):
                if o == 0:
                    return pl.ds(1, n), pl.ds(1, n)
                return (n, 0) if o > 0 else (1, n + 1)
            (sx, dx), (sy, dy) = cut(offset[0], nx), cut(offset[1], ny)
            src, dst = pads.at[v, sx, sy], pads.at[v, dx, dy]
        m = code(offset)
        return pltpu.make_async_remote_copy(
            src_ref=src, dst_ref=dst, send_sem=halo_send.at[v, m],
            recv_sem=halo_recv.at[v, m], device_id=to, device_id_type=MESH)

    order = sorted(OFFSETS, key=lambda o: (o[1] == 0 and o[2] == 0, o[0] != 0))
    sides = [o for o in order if o[0] == 0]
    faces = [o for o in order if o[0] != 0]

    def halo_start(v):
        for offset in order:
            @pl.when(reaches(offset))
            def _(offset=offset):
                halo_copy(v, offset).start()

    def halo_wait(v, part):
        for offset in part:
            @pl.when(reaches(offset))
            def _(offset=offset):
                halo_copy(v, offset).wait_send()
                halo_copy(v, minus(offset)).wait_recv()

    def total(value):
        return jnp.sum(value, axis=1, keepdims=True)

    def spread(value):
        return jnp.broadcast_to(value, zero.shape)

    def turned(tile, by):
        by = by % nz
        return pltpu.roll(tile, by, 1) if by else tile

    def emit(v, tile_of, centre=None):
        def step(x, edge):
            for y in range(ny):
                tile = tile_of(x, y)
                if centre is not None:
                    tile = tile - centre
                pads[v, x + 1, y + 1] = tile.astype(bf16)
                r = 2 * (x * ny + y)
                edge = jnp.where(lane == r, tile[:, nz - 1:nz], edge)
                edge = jnp.where(lane == r + 1, tile[:, 0:1], edge)
            return edge
        edge_out[v] = lax.fori_loop(0, nx, step, zero).astype(bf16)

    first_lanes = jnp.logical_or(lane == 0, lane == nz - 1)
    last_lanes = jnp.logical_or(lane == 2 * ny + 1, lane == 2 * ny + 2)

    def by_row(first, middle, last):
        return jnp.where(first_lanes, first, jnp.where(last_lanes, last, middle))

    def collect(v, part):
        for dx in (0,) if part is sides else (-1, 1):
            low, high = [[edge_in[v, code((-dx, -dy, -dz))] for dy in (-1, 0, 1)]
                         for dz in (-1, 1)]
            for x in range(1, nx + 1) if dx == 0 else (0,) if dx < 0 else (nx + 1,):
                base = (nx - 1, x - 1, 0)[dx + 1] * ny
                moves = (-2 * (base + ny), -2 * base, 2 * ny - 2 * base)
                got = [jnp.where(odd, turned(h, by), turned(l, by + 2))
                       for l, h, by in zip(low, high, moves)]
                cols[v, x] = by_row(*got)

    row_of_lane = jnp.where(lane == nz - 1, 0, lax.div(lane + 1, 2))
    low_y = jnp.where(me[1] > 0, 0, 1)
    high_y = jnp.where(me[1] < sizes[1] - 1, wide, wide - 1)
    low_z = jnp.where(me[2] > 0, 1, 0)
    high_z = jnp.where(me[2] < sizes[2] - 1, 1, 0)
    keep_edge = jnp.where(jnp.logical_and(row_of_lane >= low_y, row_of_lane < high_y),
                          jnp.where(odd, high_z, low_z), 0)

    def build(tile_of, shifted, turn, part):
        inner = part is sides

        def step(i, carry):
            if inner:
                x, x_ok = i + 1, None
            else:
                x = i * (nx + 1)
                x_ok = jnp.where(i == 0, me[0], sizes[0] - 1 - me[0]) > 0

            def both(flag):
                return flag if x_ok is None else jnp.logical_and(x_ok, flag)
            limits = {0: jnp.where(both(me[1] > 0), nz, 0),
                      wide - 1: jnp.where(both(me[1] < sizes[1] - 1), nz, 0)}
            middle = None if inner else jnp.where(x_ok, nz, 0)
            least = 1 if inner else jnp.where(x_ok, 1, 2)
            edge = tile_of(x, wide, inner)
            edge = jnp.where(keep_edge >= least, edge, jnp.zeros_like(edge)).astype(bf16)
            for y in range(wide):
                tile = tile_of(x, y, inner)
                limit = limits.get(y, middle)
                if limit is not None:
                    tile = jnp.where(lane < limit, tile, jnp.zeros_like(tile))
                tile = tile.astype(bf16)
                ends = turned(edge, -2 * y)
                low = jnp.where(lane == 0, ends, turned(tile, 1))
                high = jnp.where(lane == nz - 1, ends, turned(tile, -1))
                row = x * wide + y
                shifted[row, 0:chan] = high if turn else low
                shifted[row, chan:2 * chan] = tile
                shifted[row, 2 * chan:] = low if turn else high
            return carry
        lax.fori_loop(0, nx if inner else 2, step, 0)

    def raw_tiles(v):
        def tile_of(x, y, inner):
            return cols[v, x] if isinstance(y, int) and y == wide else pads[v, x, y]
        return tile_of

    def centred(v, k, full):
        def tile_of(x, y, inner):
            if not isinstance(y, int):
                return pads[v, x, y].astype(f32) + offs[k, x, 1]
            if y == wide:
                return cols[v, x].astype(f32) + offs[k, x, 3]
            if inner and 0 < y < wide - 1:
                return full[x - 1, y - 1] + offs[k, x, 1]
            kind = 0 if y == 0 else 2 if y == wide - 1 else 1
            return pads[v, x, y].astype(f32) + offs[k, x, kind]
        return tile_of

    def halo_rows(fn, part):
        if part is faces:
            def step(i, carry):
                for y in range(wide):
                    fn(i * (nx + 1), y, False)
                return carry
            lax.fori_loop(0, 2, step, 0)
        else:
            for x in range(1, nx + 1):
                for y in (0, wide - 1):
                    fn(x, y, True)

    def xs_of(part):
        return range(1, nx + 1) if part is sides else (0, nx + 1)

    def stack_rows(shifted, a, y, deep):
        parts = []
        for yi in range(deep + 2):
            parts.append(jnp.concatenate(
                [shifted[(x + a) * wide + y + yi] for x in range(nx)], axis=1))
        return parts

    def conv_rows(shifted, w, finish, init):
        def step(i, carry):
            y0 = i * DEEP
            data = jnp.concatenate(
                [p for a in range(3) for p in stack_rows(shifted, a, y0, DEEP)], axis=0)
            o = jnp.dot(mats[w], data, preferred_element_type=f32)
            for x in range(nx):
                for u in range(DEEP):
                    carry = finish(
                        x, y0 + u, o[u * chan:(u + 1) * chan, x * nz:(x + 1) * nz], carry)
            return carry
        return lax.fori_loop(0, ny // DEEP, step, init, unroll=2)

    def conv_stats(shifted, w, full):
        def finish(x, y, o, carry):
            full[x, y] = o
            return carry[0] + o, carry[1] + o * o
        return conv_rows(shifted, w, finish, (zero, zero))

    def row_of(values):
        tile = zero
        for k, value in enumerate(values):
            tile = jnp.where(lane == k * chan + chan_of, value, tile)
        return jnp.sum(tile, axis=0, keepdims=True)

    def column(row, k):
        return total(jnp.where(lane == k * chan + chan_of, row, 0.0))

    def all_start(buf, value, send, recv):
        buf[rank] = value
        for offset in others:
            pltpu.make_async_remote_copy(
                src_ref=buf.at[rank], dst_ref=buf.at[rank], send_sem=send,
                recv_sem=recv, device_id=ids(at_offset(offset)), device_id_type=MESH).start()

    def wait_bytes(buf, n, *sems):
        some = buf.at[pl.ds(0, n - 1)]
        for sem in sems:
            pltpu.make_async_copy(some, some, sem).wait()

    def tree(values):
        while len(values) > 1:
            values = [values[i] + values[i + 1] if i + 1 < len(values) else values[i]
                      for i in range(0, len(values), 2)]
        return values[0]

    def sums_start(j, values):
        all_start(slots.at[j], row_of([total(v) for v in values]), sum_send.at[j],
                  sum_recv.at[j])

    def sums_finish(j):
        wait_bytes(slots.at[j], count, sum_recv.at[j], sum_send.at[j])
        return tree([slots[j, r] for r in range(count)])

    def norm(row):
        mean = column(row, 0) / voxels
        var = column(row, 1) / voxels - mean * mean
        return spread(mean), spread(lax.rsqrt(var + EPSILON))

    def rounded(value):
        return spread(value / local).astype(bf16).astype(f32)

    def centre_of(sums):
        return rounded(total(sums[0]))

    def set_offsets(k, j, mean, part):
        def off(offset):
            return rounded(column(slots[j, rank_of(at_offset(offset))], 0)) - mean
        for dx in (0,) if part is sides else (-1, 1):
            rows = [-mean if dx == 0 and dy == 0 else off((dx, dy, 0)) for dy in (-1, 0, 1)]
            edges = by_row(*[jnp.where(odd, off((dx, dy, 1)), off((dx, dy, -1)))
                             for dy in (-1, 0, 1)])
            for x in range(1, nx + 1) if dx == 0 else (0,) if dx < 0 else (nx + 1,):
                for kind, value in enumerate(rows + [edges]):
                    offs[k, x, kind] = value

    plane = sizes[1] * sizes[2]
    in_plane = lax.rem(rank, plane)
    plane_others = [o for o in others if o[0] == 0]
    line_others = [o for o in others if o[1] == 0 and o[2] == 0]

    def pieces():
        for u in range(tiles * (chan // 8)):
            r, t = u // tiles, u % tiles
            yield u // units, (u % units) * 8, r, t

    def send_some(group, src_of, buf, at, send, recv):
        for offset in group:
            to = at_offset(offset)
            pltpu.make_async_remote_copy(
                src_ref=src_of(to), dst_ref=buf.at[at], send_sem=send,
                recv_sem=recv, device_id=ids(to), device_id_type=MESH).start()

    def plane_start(j, unit, slot, with_x=False):
        for place, at, r, t in pieces():
            unit[place, pl.ds(at, 8)] = wsum[
                r * 8:r * 8 + 8, t * nz:(t + 1) * nz].astype(unit.dtype)
        if with_x:
            for place in range(plane):
                for t in range(tiles):
                    unit[place, pl.ds(8 * units + t, 1)] = xsum[:, t * nz:(t + 1) * nz]
        slot[in_plane] = unit[in_plane]
        send_some(plane_others, lambda to: unit.at[to[1] * sizes[2] + to[2]], slot, in_plane,
                  w_send.at[j], w_recv.at[j])

    def added(j, buf, n):
        wait_bytes(buf, n, w_recv.at[j], w_send.at[j])
        return tree([buf[r].astype(f32) for r in range(n)])

    def line_start(j, slot, line):
        line[me[0]] = added(j, slot, plane).astype(line.dtype)
        send_some(line_others, lambda to: line.at[me[0]], line, me[0],
                  w_send.at[j + 1], w_recv.at[j + 1])

    def line_finish(j, line):
        return added(j + 1, line, sizes[0])

    def share(j, value):
        wfull[j, in_plane] = value.astype(bf16)
        send_some(plane_others, lambda to: wfull.at[j, in_plane], wfull.at[j], in_plane,
                  w_send.at[j], w_recv.at[j])

    def spell(j, out):
        wait_bytes(wfull.at[j], plane, w_recv.at[j], w_send.at[j])
        for place, at, r, t in pieces():
            piece = wfull[j, place, pl.ds(at, 8)].astype(f32)
            for k in range(nz // chan):
                tap = t * (nz // chan) + k
                if tap < 27:
                    out[tap, pl.ds(r * 8, 8)] = piece[:, k * chan:(k + 1) * chan]

    def wgrad(delta_of, shifted, ones=False):
        cuts = []
        for g in range(ny // DEEP):
            for x in range(nx):
                parts = [delta_of(x, g * DEEP + u) for u in range(DEEP)]
                if ones:
                    parts.append(jnp.ones((16, nz), bf16))
                cuts.append(jnp.concatenate(parts, axis=0))
        delta = jnp.concatenate(cuts, axis=1)
        span = 3 * chan
        for a in range(3):
            groups = [jnp.concatenate(stack_rows(shifted, a, g * DEEP, DEEP), axis=0)
                      for g in range(ny // DEEP)]
            o = lax.dot_general(
                delta, jnp.concatenate(groups, axis=1), (((1,), (1,)), ((), ())),
                preferred_element_type=f32)
            for ty in range(3):
                at = (a * 3 + ty) * span
                wsum[:, at:at + span] = tree(
                    [o[u * chan:(u + 1) * chan, (u + ty) * span:(u + ty + 1) * span]
                     for u in range(DEEP)])
                if ones:
                    xsum[:, at:at + span] = tree(
                        [o[DEEP * chan:DEEP * chan + 1, (u + ty) * span:(u + ty + 1) * span]
                         for u in range(DEEP)])

    def take(k):
        def step(c, carry):
            at_row = pl.multiple_of(c * pitch, 8)
            for x in range(nx):
                tall[pl.ds(at_row + x * ny, ny)] = raw[k, c, x].astype(f32)
            return carry
        lax.fori_loop(0, chan, step, 0, unroll=4)

        def tile_of(x, y):
            return tall[pl.ds(x * ny + y, chan, stride=pitch)]
        return tile_of

    def give(out):
        def step(c, carry):
            at_row = pl.multiple_of(c * pitch, 8)
            for x in range(nx):
                out[c, x] = tall[pl.ds(at_row + x * ny, ny)].astype(bf16)
            return carry
        lax.fori_loop(0, chan, step, 0, unroll=4)

    def put_row(x, y, tile):
        tall[pl.ds(x * ny + y, chan, stride=pitch)] = tile

    def prepare(k):
        taps = [wraw[k, t].astype(f32) for t in range(27)]
        span = 3 * chan
        for turn in range(2):
            flat = jnp.concatenate(taps, axis=0).T if turn else jnp.concatenate(taps, axis=1)
            none = jnp.zeros((chan, span), f32)
            for u in range(DEEP):
                parts = []
                for a in range(3):
                    for yi in range(DEEP + 2):
                        tx, ty = (2 - a, 2 - yi + u) if turn else (a, yi - u)
                        at = (tx * 3 + ty) * span
                        parts.append(flat[:, at:at + span] if 0 <= ty < 3 else none)
                mats[2 * k + turn, u * chan:(u + 1) * chan] = jnp.concatenate(
                    parts, axis=1).astype(bf16)

    loads[0].wait()
    emit(XB, take(0))
    pl.semaphore_wait(barrier, count - 1)
    halo_start(XB)
    loads[2].wait()
    emit(XA, take(1))
    halo_start(XA)
    loads[3].wait()
    emit(GO, take(2))
    loads[1].wait()
    prepare(0)
    loads[4].wait()
    prepare(1)
    for k in range(5, 9):
        loads[k].wait()

    def gain(k):
        value = spread(jnp.concatenate([gains[k]] * (nz // chan), axis=1))
        return spread(column(value, 0))
    gain_one, bias_one, gain_two, bias_two = [gain(k) for k in range(4)]

    for part in (sides, faces):
        halo_wait(XB, part)
        collect(XB, part)
        build(raw_tiles(XB), shift_xb, False, part)
    sums = conv_stats(shift_xb, 0, c1b)
    sums_start(0, sums)
    emit(C1B, lambda x, y: c1b[x, y], centre_of(sums))
    halo_start(C1B)

    for part in (sides, faces):
        halo_wait(XA, part)
        collect(XA, part)
        build(raw_tiles(XA), shift_a, False, part)
    sums = conv_stats(shift_a, 0, c1a)
    sums_start(1, sums)
    emit(C1A, lambda x, y: c1a[x, y], centre_of(sums))
    halo_start(C1A)

    def silu(z):
        return z * jax.nn.sigmoid(z)

    mean_one, scale_one = norm(sums_finish(0))
    steep_one = gain_one * scale_one
    tile_1b = centred(C1B, 0, c1b)

    def z_one(x, y, inner):
        return tile_1b(x, y, inner) * steep_one + bias_one
    for part in (sides, faces):
        set_offsets(0, 0, mean_one, part)
        halo_wait(C1B, part)
        collect(C1B, part)
        build(lambda *at: silu(z_one(*at)), shift_hb, False, part)
    sums = conv_stats(shift_hb, 2, c2b)
    sums_start(2, sums)
    emit(C2B, lambda x, y: c2b[x, y], centre_of(sums))
    halo_start(C2B)

    mean_a, scale_a = norm(sums_finish(1))
    steep_a = gain_one * scale_a
    tile_1a = centred(C1A, 1, c1a)
    for part in (sides, faces):
        set_offsets(1, 1, mean_a, part)
        halo_wait(C1A, part)
        collect(C1A, part)
        build(lambda *at: silu(tile_1a(*at) * steep_a + bias_one), shift_a, False, part)
    sums = conv_stats(shift_a, 2, c2a)
    sums_start(3, sums)

    mean_two, scale_two = norm(sums_finish(2))
    steep_two = gain_two * scale_two

    def own_two(x, carry):
        sd, sx = carry
        for y in range(ny):
            c = c2b[x, y] - mean_two
            d = pads[GO, x + 1, y + 1].astype(f32) * slope_of(c * steep_two + bias_two)
            fd2[x + 1, y + 1] = d
            sd, sx = sd + d, sx + d * c
        return sd, sx
    sd, sx = lax.fori_loop(0, nx, own_two, (zero, zero))
    sums_start(4, (sx * scale_two, sd))
    halo_start(GO)

    wgrad(lambda x, y: ((c1b[x, y] - mean_one) * scale_one).astype(bf16), shift_xb, True)
    plane_start(2, unit_x, slot_x, True)

    tile_2b = centred(C2B, 2, c2b)
    tile_go = raw_tiles(GO)

    def d_two(*at):
        return tile_go(*at).astype(f32) * slope_of(tile_2b(*at) * steep_two + bias_two)

    def halo_two(x, y, inner):
        fd2[x, y] = d_two(x, y, inner)

    for part in (sides, faces):
        set_offsets(2, 2, mean_two, part)
        halo_wait(C2B, part)
        halo_wait(GO, part)
        collect(C2B, part)
        collect(GO, part)
        halo_rows(halo_two, part)
        for x in xs_of(part):
            dcols[D2, x] = d_two(x, wide, part is sides)

    mean_a2, scale_a2 = norm(sums_finish(3))
    steep_a2 = gain_two * scale_a2

    def finish_a(x, carry):
        for y in range(ny):
            put_row(x, y, silu((c2a[x, y] - mean_a2) * steep_a2 + bias_two))
        return carry
    lax.fori_loop(0, nx, finish_a, 0)
    give(ya)

    row_two = sums_finish(4)
    sx2 = spread(column(row_two, 0) / voxels) * scale_two
    sd2 = spread(column(row_two, 1) / voxels)

    def dc_two(x, y, inner):
        d = dcols[D2, x] if y == wide else fd2[x, y]
        return steep_two * (d - sd2 - tile_2b(x, y, inner) * sx2)
    build(dc_two, shift_d, True, sides)
    build(dc_two, shift_d, True, faces)

    def back(x, y, o, carry):
        sd, sx = carry
        e1[x, y] = o
        c = c1b[x, y] - mean_one
        d = o * slope_of(c * steep_one + bias_one)
        fd1[x + 1, y + 1] = d
        d1h[x, y] = d.astype(bf16)
        return sd + d, sx + d * c
    sd, sx = conv_rows(shift_d, 3, back, (zero, zero))
    sums_start(5, (sx * scale_one, sd))
    emit(E1, lambda x, y: e1[x, y])
    halo_start(E1)
    wgrad(lambda x, y: d1h[x, y], shift_xb)
    plane_start(4, unit_f, slot_f)
    line_start(2, slot_x, line_x)
    wgrad(lambda x, y: shift_d[(x + 1) * wide + y + 1, chan:2 * chan], shift_hb)
    plane_start(6, unit_h, slot_h)

    row_one = sums_finish(5)
    sx1_wide = spread(column(row_one, 0) / voxels)
    sx1 = sx1_wide * scale_one
    sd1 = spread(column(row_one, 1) / voxels)
    for k, value in enumerate((steep_one * factor, sd1, sx1_wide)):
        kcol[k] = value

    def halo_one(x, y, inner):
        fd1[x, y] = pads[E1, x, y].astype(f32) * slope_of(z_one(x, y, inner))

    def dc_one(x, y, inner):
        d = dcols[D1, x] if y == wide else fd1[x, y]
        return steep_one * (d - sd1 - tile_1b(x, y, inner) * sx1)

    halo_wait(E1, sides)
    collect(E1, sides)
    halo_rows(halo_one, sides)
    for x in xs_of(sides):
        dcols[D1, x] = cols[E1, x].astype(f32) * slope_of(z_one(x, wide, True))
    build(dc_one, shift_d, True, sides)

    line_start(4, slot_f, line_f)

    halo_wait(E1, faces)
    collect(E1, faces)
    halo_rows(halo_one, faces)
    for x in xs_of(faces):
        dcols[D1, x] = cols[E1, x].astype(f32) * slope_of(z_one(x, wide, False))
    build(dc_one, shift_d, True, faces)
    line_start(6, slot_h, line_h)

    def last(x, y, o, carry):
        put_row(x, y, o)
        return carry
    conv_rows(shift_d, 1, last, 0)
    give(dxb)
    along = line_finish(2, line_x)
    plain[...] = along[8 * units:]
    straight = line_finish(4, line_f)
    mixed = []
    for q in range(units):
        u = in_plane * units + q
        r = pl.multiple_of(jnp.minimum(lax.div(u, tiles), chan // 8 - 1) * 8, 8)
        k, d, x = [kcol[i, pl.ds(r, 8)] for i in range(3)]
        part = slice(q * 8, q * 8 + 8)
        mixed.append(k * (straight[part] - d * plain[pl.ds(lax.rem(u, tiles), 1)]
                          - x * along[part]))
    share(0, jnp.concatenate(mixed, axis=0))
    share(1, line_finish(6, line_h) * factor)
    for k, row in enumerate((row_one, row_two)):
        for j in range(2):
            gnorm[2 * k + j:2 * k + j + 1, :] = row[:, j * chan:(j + 1) * chan] * factor
    spell(0, gw1)
    spell(1, gw2)


def deliver(*refs):
    sem = refs[-1]
    half = (len(refs) - 1) // 2
    copies = [pltpu.make_async_copy(src, dst, sem.at[k])
              for k, (src, dst) in enumerate(zip(refs[:half], refs[half:-1]))]
    for copy in copies:
        copy.start()
    for copy in copies:
        copy.wait()


def body(sizes, x_a, x_b, w_first, w_second, gain_first, bias_first, gain_second, bias_second,
         grad_out):
    chan, nx, ny, nz = x_a.shape
    count = math.prod(sizes)
    voxels = float(nx * ny * nz * count)
    taps = 27 * chan
    bf16, f32 = jnp.bfloat16, jnp.float32
    tiles = -(-taps // nz)
    plane = sizes[1] * sizes[2]
    units = -(-tiles * (chan // 8) // plane)
    full = (nx + 2, ny + 2, chan, nz)
    span = (nx + 2) * (ny + 2)
    grid = (nx, ny, chan, nz)
    vmem = pl.BlockSpec(memory_space=pltpu.VMEM)
    hbm = pl.BlockSpec(memory_space=pl.ANY)
    dma = pltpu.SemaphoreType.DMA
    shapes = (
        jax.ShapeDtypeStruct(x_a.shape, bf16),
        jax.ShapeDtypeStruct(x_a.shape, bf16),
        jax.ShapeDtypeStruct((27, chan, chan), f32),
        jax.ShapeDtypeStruct((27, chan, chan), f32),
        jax.ShapeDtypeStruct((4, chan), f32),
    )
    results = pl.pallas_call(
        functools.partial(kernel, sizes, voxels, units),
        out_shape=shapes,
        in_specs=[hbm] * 9,
        out_specs=[vmem] * 5,
        scratch_shapes=[
            pltpu.VMEM((3, chan, nx, ny, nz), bf16),
            pltpu.VMEM((2, 27, chan, chan), bf16),
            pltpu.VMEM((4, 1, chan), f32),
            pltpu.VMEM((chan * (nx * ny + 8), nz), f32),
            pltpu.VMEM((4, DEEP * chan, 9 * (DEEP + 2) * chan), bf16),
            pltpu.VMEM((7,) + full, bf16),
            pltpu.VMEM((7, chan, nz), bf16),
            pltpu.VMEM((7, 27, chan, nz), bf16),
            pltpu.VMEM((7, nx + 2, chan, nz), bf16),
            pltpu.VMEM((2, nx + 2, chan, nz), f32),
            pltpu.VMEM((3, nx + 2, 4, chan, nz), f32),
        ] + [pltpu.VMEM((span, 3 * chan, nz), bf16)] * 4
        + [pltpu.VMEM(full, f32)] * 2
        + [pltpu.VMEM(grid, f32)] * 5
        + [
            pltpu.VMEM(grid, bf16),
            pltpu.VMEM((6, count, 1, nz), f32),
            pltpu.VMEM((1, tiles * nz), f32),
            pltpu.VMEM((8, nz), f32),
            pltpu.VMEM((3, chan, nz), f32),
            pltpu.VMEM((chan, tiles * nz), f32),
            pltpu.VMEM((plane, 8 * units + 8, nz), f32),
            pltpu.VMEM((plane, 8 * units + 8, nz), f32),
            pltpu.VMEM((sizes[0], 8 * units + 8, nz), f32),
            pltpu.VMEM((plane, 8 * units, nz), f32),
            pltpu.VMEM((plane, 8 * units, nz), f32),
            pltpu.VMEM((sizes[0], 8 * units, nz), f32),
            pltpu.VMEM((plane, 8 * units, nz), bf16),
            pltpu.VMEM((plane, 8 * units, nz), bf16),
            pltpu.VMEM((sizes[0], 8 * units, nz), bf16),
            pltpu.VMEM((2, plane, 8 * units, nz), bf16),
            dma((9,)),
            dma((7, 27)), dma((7, 27)),
            dma((6,)), dma((6,)),
            dma((8,)), dma((8,)),
        ],
        compiler_params=pltpu.CompilerParams(
            collective_id=0, has_side_effects=True, vmem_limit_bytes=56 * 1024 * 1024),
    )(
        x_a, x_b, grad_out,
        w_first.reshape(27, chan, chan), w_second.reshape(27, chan, chan),
        gain_first.reshape(1, chan), bias_first.reshape(1, chan),
        gain_second.reshape(1, chan), bias_second.reshape(1, chan),
    )
    y_a, dx_b, gw1, gw2, gnorm = pl.pallas_call(
        deliver,
        out_shape=shapes,
        in_specs=[vmem] * 5,
        out_specs=[hbm] * 5,
        scratch_shapes=[dma((5,))],
    )(*results)
    cube = (3, 3, 3, chan, chan)
    return y_a, dx_b, gw1.reshape(cube), gw2.reshape(cube), gnorm


def solution(mesh):
    sizes = tuple(mesh.shape[a] for a in AXES)
    split = P(None, *AXES)
    return jax.shard_map(
        functools.partial(body, sizes),
        mesh=mesh,
        in_specs=(split, split, P(), P(), P(), P(), P(), P(), split),
        out_specs=(split, split, P(), P(), P()),
        check_vma=False,
    )
```

```python
import functools
import math

import jax
import jax.numpy as jnp
from jax import lax
from jax.experimental import pallas as pl
from jax.experimental.pallas import tpu as pltpu
from jax.sharding import PartitionSpec as P

EPSILON = 1e-05
AXES = ("gx", "gy", "gz")
MESH = pl.DeviceIdType.MESH
XB, XA, GO, C1B, C1A, C2B, E1 = range(7)
D2, D1 = range(2)
OFFSETS = [(a, b, c) for a in (-1, 0, 1) for b in (-1, 0, 1) for c in (-1, 0, 1)
           if (a, b, c) != (0, 0, 0)]
DEEP = 4


def sigmoid(z):
    return 0.5 * jnp.tanh(0.5 * z) + 0.5


def slope_of(z):
    s = sigmoid(z)
    return s * (1.0 + z * (1.0 - s))


def code(offset):
    a, b, c = offset
    return (a + 1) * 9 + (b + 1) * 3 + c + 1


def minus(offset):
    return tuple(-o for o in offset)


def kernel(
    sizes, voxels, units,
    xa, xb, go, w1, w2, g1, b1, g2, b2,
    ya, dxb, gw1, gw2, gnorm,
    raw, wraw, gains, tall, mats, pads, edge_out, edge_in, cols, dcols, offs,
    shift_xb, shift_a, shift_hb, shift_d,
    fd2, fd1, c1b, c1a, c2b, c2a, e1, d1h, slots, xsum, plain, kcol, wsum,
    unit_x, slot_x, line_x, unit_f, slot_f, line_f, unit_h, slot_h, line_h, wfull,
    bytes_of, load_sem, halo_send, halo_recv, sum_send, sum_recv, w_send, w_recv,
):
    chan, nx, ny, nz = raw.shape[1:]
    wide = ny + 2
    own = nx * ny
    pitch = tall.shape[0] // chan
    count = math.prod(sizes)
    local = float(own * nz)
    factor = 1.0 / math.sqrt(voxels)
    tiles = wsum.shape[1] // nz
    me = [lax.axis_index(a) for a in AXES]

    def rank_of(place):
        return (place[0] * sizes[1] + place[1]) * sizes[2] + place[2]
    rank = rank_of(me)
    lane = lax.broadcasted_iota(jnp.int32, (chan, nz), 1)
    chan_of = lax.broadcasted_iota(jnp.int32, (chan, nz), 0)
    odd = lax.rem(lane, 2) == 1
    zero = jnp.zeros((chan, nz), jnp.float32)
    bf16, f32 = jnp.bfloat16, jnp.float32

    others = [(a, b, c) for a in range(sizes[0]) for b in range(sizes[1])
              for c in range(sizes[2])][:0:-1]

    def at_offset(offset):
        return [lax.rem(m + o + s, s) for m, o, s in zip(me, offset, sizes)]

    def ids(place):
        return dict(zip(AXES, place))

    barrier = pltpu.get_barrier_semaphore()
    for offset in others:
        pl.semaphore_signal(
            barrier, inc=1, device_id=ids(at_offset(offset)), device_id_type=MESH)

    loads = []
    for at, (src, dst) in enumerate((
            (xb, raw.at[0]), (w1, wraw.at[0]), (xa, raw.at[1]), (go, raw.at[2]),
            (w2, wraw.at[1]), (g1, gains.at[0]), (b1, gains.at[1]), (g2, gains.at[2]),
            (b2, gains.at[3]))):
        copy = pltpu.make_async_copy(src, dst, load_sem.at[at])
        copy.start()
        loads.append(copy)

    inside = []
    for k in range(3):
        inside.append({-1: me[k] > 0, 0: None, 1: me[k] < sizes[k] - 1})

    def reaches(offset):
        known = [inside[k][o] for k, o in enumerate(offset) if o]
        flag = known[0]
        for more in known[1:]:
            flag = jnp.logical_and(flag, more)
        return flag

    def halo_copy(v, offset):
        to = ids([me[k] + o for k, o in enumerate(offset)])
        if offset[2]:
            src, dst = edge_out.at[v], edge_in.at[v, code(offset)]
        else:
            def cut(o, n):
                if o == 0:
                    return pl.ds(1, n), pl.ds(1, n)
                return (n, 0) if o > 0 else (1, n + 1)
            (sx, dx), (sy, dy) = cut(offset[0], nx), cut(offset[1], ny)
            src, dst = pads.at[v, sx, sy], pads.at[v, dx, dy]
        m = 0 if offset[0] == 0 else 1
        return pltpu.make_async_remote_copy(
            src_ref=src, dst_ref=dst, send_sem=halo_send.at[v, m],
            recv_sem=halo_recv.at[v, m], device_id=to, device_id_type=MESH)

    order = sorted(OFFSETS, key=lambda o: (o[1] == 0 and o[2] == 0, o[0] != 0))
    sides = [o for o in order if o[0] == 0]
    faces = [o for o in order if o[0] != 0]

    def halo_start(v):
        for offset in order:
            @pl.when(reaches(offset))
            def _(offset=offset):
                halo_copy(v, offset).start()

    near = [jnp.where(inside[k][-1], 1, 0) + jnp.where(inside[k][1], 1, 0) for k in range(3)]
    cases = [(0,) if n == 1 else (1,) if n == 2 else (1, 2) for n in sizes]

    def halo_wait(v, part):
        m = 0 if part is sides else 1
        for a in ((0,) if part is sides else cases[0]):
            for b in cases[1]:
                for c in cases[2]:
                    rows = b * nx + c * (1 + b) if part is sides else a * (
                        ny + b + c * (1 + b))
                    if not rows:
                        continue
                    flag = jnp.logical_and(near[1] == b, near[2] == c)
                    if part is faces:
                        flag = jnp.logical_and(flag, near[0] == a)

                    @pl.when(flag)
                    def _(rows=rows):
                        some = bytes_of.at[pl.ds(0, rows)]
                        for sem in (halo_recv.at[v, m], halo_send.at[v, m]):
                            pltpu.make_async_copy(some, some, sem).wait()

    def total(value):
        return jnp.sum(value, axis=1, keepdims=True)

    def spread(value):
        return jnp.broadcast_to(value, zero.shape)

    def turned(tile, by):
        by = by % nz
        return pltpu.roll(tile, by, 1) if by else tile

    def emit(v, tile_of, centre=None):
        def step(x, edge):
            for y in range(ny):
                tile = tile_of(x, y)
                if centre is not None:
                    tile = tile - centre
                tile = tile.astype(bf16)
                pads[v, x + 1, y + 1] = tile
                r = 2 * (x * ny + y)
                edge = jnp.where(lane == r, tile[:, nz - 1:nz], edge)
                edge = jnp.where(lane == r + 1, tile[:, 0:1], edge)
            return edge
        edge_out[v] = lax.fori_loop(0, nx, step, zero.astype(bf16))

    first_lanes = jnp.logical_or(lane == 0, lane == nz - 1)
    last_lanes = jnp.logical_or(lane == 2 * ny + 1, lane == 2 * ny + 2)

    def by_row(first, middle, last):
        return jnp.where(first_lanes, first, jnp.where(last_lanes, last, middle))

    def collect(v, part):
        for dx in (0,) if part is sides else (-1, 1):
            low, high = [[edge_in[v, code((-dx, -dy, -dz))] for dy in (-1, 0, 1)]
                         for dz in (-1, 1)]
            for x in range(1, nx + 1) if dx == 0 else (0,) if dx < 0 else (nx + 1,):
                base = (nx - 1, x - 1, 0)[dx + 1] * ny
                moves = (-2 * (base + ny), -2 * base, 2 * ny - 2 * base)
                got = [jnp.where(odd, turned(h, by), turned(l, by + 2))
                       for l, h, by in zip(low, high, moves)]
                cols[v, x] = by_row(*got)

    row_of_lane = jnp.where(lane == nz - 1, 0, lax.div(lane + 1, 2))
    low_y = jnp.where(me[1] > 0, 0, 1)
    high_y = jnp.where(me[1] < sizes[1] - 1, wide, wide - 1)
    low_z = jnp.where(me[2] > 0, 1, 0)
    high_z = jnp.where(me[2] < sizes[2] - 1, 1, 0)
    keep_edge = jnp.where(jnp.logical_and(row_of_lane >= low_y, row_of_lane < high_y),
                          jnp.where(odd, high_z, low_z), 0)

    def build(tile_of, shifted, turn, part):
        inner = part is sides

        def step(i, carry):
            if inner:
                x, x_ok = i + 1, None
            else:
                x = i * (nx + 1)
                x_ok = jnp.where(i == 0, me[0], sizes[0] - 1 - me[0]) > 0

            def both(flag):
                return flag if x_ok is None else jnp.logical_and(x_ok, flag)
            limits = {0: jnp.where(both(me[1] > 0), nz, 0),
                      wide - 1: jnp.where(both(me[1] < sizes[1] - 1), nz, 0)}
            middle = None if inner else jnp.where(x_ok, nz, 0)
            least = 1 if inner else jnp.where(x_ok, 1, 2)
            edge = tile_of(x, wide, inner)
            edge = jnp.where(keep_edge >= least, edge, jnp.zeros_like(edge)).astype(bf16)
            for y in range(wide):
                tile = tile_of(x, y, inner)
                limit = limits.get(y, middle)
                if limit is not None:
                    tile = jnp.where(lane < limit, tile, jnp.zeros_like(tile))
                tile = tile.astype(bf16)
                ends = turned(edge, -2 * y)
                low = jnp.where(lane == 0, ends, turned(tile, 1))
                high = jnp.where(lane == nz - 1, ends, turned(tile, -1))
                row = x * wide + y
                shifted[row, 0:chan] = high if turn else low
                shifted[row, chan:2 * chan] = tile
                shifted[row, 2 * chan:] = low if turn else high
            return carry
        lax.fori_loop(0, nx if inner else 2, step, 0)

    def raw_tiles(v):
        def tile_of(x, y, inner):
            return cols[v, x] if isinstance(y, int) and y == wide else pads[v, x, y]
        return tile_of

    def centred(v, k, full):
        def tile_of(x, y, inner):
            if not isinstance(y, int):
                return pads[v, x, y].astype(f32) + offs[k, x, 1]
            if y == wide:
                return cols[v, x].astype(f32) + offs[k, x, 3]
            if inner and 0 < y < wide - 1:
                return full[x - 1, y - 1] + offs[k, x, 1]
            kind = 0 if y == 0 else 2 if y == wide - 1 else 1
            return pads[v, x, y].astype(f32) + offs[k, x, kind]
        return tile_of

    def halo_rows(fn):
        for x in range(1, nx + 1):
            for y in (0, wide - 1):
                fn(x, y, True)

    def stack_rows(shifted, a, y, deep):
        parts = []
        for yi in range(deep + 2):
            parts.append(jnp.concatenate(
                [shifted[(x + a) * wide + y + yi] for x in range(nx)], axis=1))
        return parts

    def conv_rows(shifted, w, finish, init):
        def step(i, carry):
            y0 = i * DEEP
            data = jnp.concatenate(
                [p for a in range(3) for p in stack_rows(shifted, a, y0, DEEP)], axis=0)
            o = jnp.dot(mats[w], data, preferred_element_type=f32)
            for x in range(nx):
                for u in range(DEEP):
                    carry = finish(
                        x, y0 + u, o[u * chan:(u + 1) * chan, x * nz:(x + 1) * nz], carry)
            return carry
        return lax.fori_loop(0, ny // DEEP, step, init, unroll=2)

    def conv_stats(shifted, w, full):
        def finish(x, y, o, carry):
            full[x, y] = o
            return carry[0] + o, carry[1] + o * o
        return conv_rows(shifted, w, finish, (zero, zero))

    def row_of(values):
        tile = zero
        for k, value in enumerate(values):
            tile = jnp.where(lane == k * chan + chan_of, value, tile)
        return jnp.sum(tile, axis=0, keepdims=True)

    def column(row, k):
        return total(jnp.where(lane == k * chan + chan_of, row, 0.0))

    def all_start(buf, value, send, recv):
        buf[rank] = value
        for offset in others:
            pltpu.make_async_remote_copy(
                src_ref=buf.at[rank], dst_ref=buf.at[rank], send_sem=send,
                recv_sem=recv, device_id=ids(at_offset(offset)), device_id_type=MESH).start()

    def wait_bytes(buf, n, *sems):
        some = buf.at[pl.ds(0, n - 1)]
        for sem in sems:
            pltpu.make_async_copy(some, some, sem).wait()

    def tree(values):
        while len(values) > 1:
            values = [values[i] + values[i + 1] if i + 1 < len(values) else values[i]
                      for i in range(0, len(values), 2)]
        return values[0]

    def sums_start(j, values):
        all_start(slots.at[j], row_of([total(v) for v in values]), sum_send.at[j],
                  sum_recv.at[j])

    def sums_finish(j):
        wait_bytes(slots.at[j], count, sum_recv.at[j], sum_send.at[j])
        return tree([slots[j, r] for r in range(count)])

    def norm(row):
        mean = column(row, 0) / voxels
        var = column(row, 1) / voxels - mean * mean
        return spread(mean), spread(lax.rsqrt(var + EPSILON))

    def rounded(value):
        return spread(value / local).astype(bf16).astype(f32)

    def centre_of(sums):
        return rounded(total(sums[0]))

    def set_offsets(k, j, mean, part):
        def off(offset):
            return rounded(column(slots[j, rank_of(at_offset(offset))], 0)) - mean
        for dx in (0,) if part is sides else (-1, 1):
            rows = [-mean if dx == 0 and dy == 0 else off((dx, dy, 0)) for dy in (-1, 0, 1)]
            edges = by_row(*[jnp.where(odd, off((dx, dy, 1)), off((dx, dy, -1)))
                             for dy in (-1, 0, 1)])
            for x in range(1, nx + 1) if dx == 0 else (0,) if dx < 0 else (nx + 1,):
                for kind, value in enumerate(rows + [edges]):
                    offs[k, x, kind] = value

    plane = sizes[1] * sizes[2]
    in_plane = lax.rem(rank, plane)
    plane_others = [o for o in others if o[0] == 0]
    line_others = [o for o in others if o[1] == 0 and o[2] == 0]

    def pieces():
        for u in range(tiles * (chan // 8)):
            r, t = u // tiles, u % tiles
            yield u // units, (u % units) * 8, r, t

    def send_some(group, src_of, buf, at, send, recv):
        for offset in group:
            to = at_offset(offset)
            pltpu.make_async_remote_copy(
                src_ref=src_of(to), dst_ref=buf.at[at], send_sem=send,
                recv_sem=recv, device_id=ids(to), device_id_type=MESH).start()

    def plane_start(j, unit, slot, with_x=False):
        for place, at, r, t in pieces():
            unit[place, pl.ds(at, 8)] = wsum[
                r * 8:r * 8 + 8, t * nz:(t + 1) * nz].astype(unit.dtype)
        if with_x:
            for place in range(plane):
                for t in range(tiles):
                    unit[place, pl.ds(8 * units + t, 1)] = xsum[:, t * nz:(t + 1) * nz]
        slot[in_plane] = unit[in_plane]
        send_some(plane_others, lambda to: unit.at[to[1] * sizes[2] + to[2]], slot, in_plane,
                  w_send.at[j], w_recv.at[j])

    def added(j, buf, n):
        wait_bytes(buf, n, w_recv.at[j], w_send.at[j])
        return tree([buf[r].astype(f32) for r in range(n)])

    def line_start(j, slot, line):
        line[me[0]] = added(j, slot, plane).astype(line.dtype)
        send_some(line_others, lambda to: line.at[me[0]], line, me[0],
                  w_send.at[j + 1], w_recv.at[j + 1])

    def line_finish(j, line):
        return added(j + 1, line, sizes[0])

    def share(j, value):
        wfull[j, in_plane] = value.astype(bf16)
        send_some(plane_others, lambda to: wfull.at[j, in_plane], wfull.at[j], in_plane,
                  w_send.at[j], w_recv.at[j])

    def spell(j, out):
        wait_bytes(wfull.at[j], plane, w_recv.at[j], w_send.at[j])
        for place, at, r, t in pieces():
            piece = wfull[j, place, pl.ds(at, 8)].astype(f32)
            for k in range(nz // chan):
                tap = t * (nz // chan) + k
                if tap < 27:
                    out[tap, pl.ds(r * 8, 8)] = piece[:, k * chan:(k + 1) * chan]

    def wgrad(delta_of, shifted, ones=False):
        cuts = []
        for g in range(ny // DEEP):
            for x in range(nx):
                parts = [delta_of(x, g * DEEP + u) for u in range(DEEP)]
                if ones:
                    parts.append(jnp.ones((16, nz), bf16))
                cuts.append(jnp.concatenate(parts, axis=0))
        delta = jnp.concatenate(cuts, axis=1)
        span = 3 * chan
        for a in range(3):
            groups = [jnp.concatenate(stack_rows(shifted, a, g * DEEP, DEEP), axis=0)
                      for g in range(ny // DEEP)]
            o = lax.dot_general(
                delta, jnp.concatenate(groups, axis=1), (((1,), (1,)), ((), ())),
                preferred_element_type=f32)
            for ty in range(3):
                at = (a * 3 + ty) * span
                wsum[:, at:at + span] = tree(
                    [o[u * chan:(u + 1) * chan, (u + ty) * span:(u + ty + 1) * span]
                     for u in range(DEEP)])
                if ones:
                    xsum[:, at:at + span] = tree(
                        [o[DEEP * chan:DEEP * chan + 1, (u + ty) * span:(u + ty + 1) * span]
                         for u in range(DEEP)])

    def take(k):
        def step(c, carry):
            at_row = pl.multiple_of(c * pitch, 8)
            for x in range(nx):
                tall[pl.ds(at_row + x * ny, ny)] = raw[k, c, x].astype(f32)
            return carry
        lax.fori_loop(0, chan, step, 0, unroll=4)

        def tile_of(x, y):
            return tall[pl.ds(x * ny + y, chan, stride=pitch)]
        return tile_of

    def give(out):
        def step(c, carry):
            at_row = pl.multiple_of(c * pitch, 8)
            for x in range(nx):
                out[c, x] = tall[pl.ds(at_row + x * ny, ny)].astype(bf16)
            return carry
        lax.fori_loop(0, chan, step, 0, unroll=4)

    def put_row(x, y, tile):
        tall[pl.ds(x * ny + y, chan, stride=pitch)] = tile

    def prepare(k):
        taps = [wraw[k, t].astype(f32) for t in range(27)]
        span = 3 * chan
        for turn in range(2):
            flat = jnp.concatenate(taps, axis=0).T if turn else jnp.concatenate(taps, axis=1)
            none = jnp.zeros((chan, span), f32)
            for u in range(DEEP):
                parts = []
                for a in range(3):
                    for yi in range(DEEP + 2):
                        tx, ty = (2 - a, 2 - yi + u) if turn else (a, yi - u)
                        at = (tx * 3 + ty) * span
                        parts.append(flat[:, at:at + span] if 0 <= ty < 3 else none)
                mats[2 * k + turn, u * chan:(u + 1) * chan] = jnp.concatenate(
                    parts, axis=1).astype(bf16)

    loads[0].wait()
    emit(XB, take(0))
    pl.semaphore_wait(barrier, count - 1)
    halo_start(XB)
    loads[2].wait()
    emit(XA, take(1))
    halo_start(XA)
    loads[3].wait()
    emit(GO, take(2))
    loads[1].wait()
    prepare(0)
    loads[4].wait()
    prepare(1)
    for k in range(5, 9):
        loads[k].wait()

    def gain(k):
        value = spread(jnp.concatenate([gains[k]] * (nz // chan), axis=1))
        return spread(column(value, 0))
    gain_one, bias_one, gain_two, bias_two = [gain(k) for k in range(4)]

    for part in (sides, faces):
        halo_wait(XB, part)
        collect(XB, part)
        build(raw_tiles(XB), shift_xb, False, part)
    sums = conv_stats(shift_xb, 0, c1b)
    sums_start(0, sums)
    emit(C1B, lambda x, y: c1b[x, y], centre_of(sums))
    halo_start(C1B)

    for part in (sides, faces):
        halo_wait(XA, part)
        collect(XA, part)
        build(raw_tiles(XA), shift_a, False, part)
    sums = conv_stats(shift_a, 0, c1a)
    sums_start(1, sums)
    emit(C1A, lambda x, y: c1a[x, y], centre_of(sums))
    halo_start(C1A)

    def silu(z):
        return z * sigmoid(z)

    mean_one, scale_one = norm(sums_finish(0))
    steep_one = gain_one * scale_one
    tile_1b = centred(C1B, 0, c1b)

    def z_one(x, y, inner):
        return tile_1b(x, y, inner) * steep_one + bias_one
    for part in (sides, faces):
        set_offsets(0, 0, mean_one, part)
        halo_wait(C1B, part)
        collect(C1B, part)
        build(lambda *at: silu(z_one(*at)), shift_hb, False, part)
    sums = conv_stats(shift_hb, 2, c2b)
    sums_start(2, sums)
    emit(C2B, lambda x, y: c2b[x, y], centre_of(sums))
    halo_start(C2B)

    mean_a, scale_a = norm(sums_finish(1))
    steep_a = gain_one * scale_a
    tile_1a = centred(C1A, 1, c1a)
    for part in (sides, faces):
        set_offsets(1, 1, mean_a, part)
        halo_wait(C1A, part)
        collect(C1A, part)
        build(lambda *at: silu(tile_1a(*at) * steep_a + bias_one), shift_a, False, part)
    sums = conv_stats(shift_a, 2, c2a)
    sums_start(3, sums)

    mean_two, scale_two = norm(sums_finish(2))
    steep_two = gain_two * scale_two

    def own_two(x, carry):
        sd, sx = carry
        for y in range(ny):
            c = c2b[x, y] - mean_two
            d = pads[GO, x + 1, y + 1].astype(f32) * slope_of(c * steep_two + bias_two)
            fd2[x + 1, y + 1] = d
            sd, sx = sd + d, sx + d * c
        return sd, sx
    sd, sx = lax.fori_loop(0, nx, own_two, (zero, zero))
    sums_start(4, (sx * scale_two, sd))
    halo_start(GO)

    wgrad(lambda x, y: ((c1b[x, y] - mean_one) * scale_one).astype(bf16), shift_xb, True)
    plane_start(2, unit_x, slot_x, True)

    tile_2b = centred(C2B, 2, c2b)
    tile_go = raw_tiles(GO)

    def d_two(*at):
        return tile_go(*at).astype(f32) * slope_of(tile_2b(*at) * steep_two + bias_two)

    def halo_two(x, y, inner):
        fd2[x, y] = d_two(x, y, inner)

    set_offsets(2, 2, mean_two, sides)
    halo_wait(C2B, sides)
    collect(C2B, sides)
    halo_wait(GO, sides)
    collect(GO, sides)
    halo_rows(halo_two)
    for x in range(1, nx + 1):
        dcols[D2, x] = d_two(x, wide, True)
    set_offsets(2, 2, mean_two, faces)
    halo_wait(C2B, faces)
    collect(C2B, faces)

    mean_a2, scale_a2 = norm(sums_finish(3))
    steep_a2 = gain_two * scale_a2

    def finish_a(x, carry):
        for y in range(ny):
            put_row(x, y, silu((c2a[x, y] - mean_a2) * steep_a2 + bias_two))
        return carry
    lax.fori_loop(0, nx, finish_a, 0)
    give(ya)

    row_two = sums_finish(4)
    sx2 = spread(column(row_two, 0) / voxels) * scale_two
    sd2 = spread(column(row_two, 1) / voxels)

    def dc_two(x, y, inner):
        c = tile_2b(x, y, inner)
        if not inner:
            d = tile_go(x, y, inner).astype(f32) * slope_of(c * steep_two + bias_two)
        else:
            d = dcols[D2, x] if y == wide else fd2[x, y]
        return steep_two * (d - sd2 - c * sx2)
    build(dc_two, shift_d, True, sides)
    halo_wait(GO, faces)
    collect(GO, faces)
    build(dc_two, shift_d, True, faces)

    def back(x, y, o, carry):
        sd, sx = carry
        e1[x, y] = o
        c = c1b[x, y] - mean_one
        d = o * slope_of(c * steep_one + bias_one)
        fd1[x + 1, y + 1] = d
        d1h[x, y] = d.astype(bf16)
        return sd + d, sx + d * c
    sd, sx = conv_rows(shift_d, 3, back, (zero, zero))
    sums_start(5, (sx * scale_one, sd))
    emit(E1, lambda x, y: e1[x, y])
    halo_start(E1)
    wgrad(lambda x, y: d1h[x, y], shift_xb)
    plane_start(4, unit_f, slot_f)
    line_start(2, slot_x, line_x)
    wgrad(lambda x, y: shift_d[(x + 1) * wide + y + 1, chan:2 * chan], shift_hb)
    plane_start(6, unit_h, slot_h)

    row_one = sums_finish(5)
    sx1_wide = spread(column(row_one, 0) / voxels)
    sx1 = sx1_wide * scale_one
    sd1 = spread(column(row_one, 1) / voxels)
    for k, value in enumerate((steep_one * factor, sd1, sx1_wide)):
        kcol[k] = value

    def halo_one(x, y, inner):
        fd1[x, y] = pads[E1, x, y].astype(f32) * slope_of(z_one(x, y, inner))

    def dc_one(x, y, inner):
        c = tile_1b(x, y, inner)
        if inner:
            d = dcols[D1, x] if y == wide else fd1[x, y]
        else:
            e = cols[E1, x] if y == wide else pads[E1, x, y]
            d = e.astype(f32) * slope_of(c * steep_one + bias_one)
        return steep_one * (d - sd1 - c * sx1)

    halo_wait(E1, sides)
    collect(E1, sides)
    halo_rows(halo_one)
    for x in range(1, nx + 1):
        dcols[D1, x] = cols[E1, x].astype(f32) * slope_of(z_one(x, wide, True))
    build(dc_one, shift_d, True, sides)

    line_start(4, slot_f, line_f)

    halo_wait(E1, faces)
    collect(E1, faces)
    build(dc_one, shift_d, True, faces)
    line_start(6, slot_h, line_h)

    def last(x, y, o, carry):
        put_row(x, y, o)
        return carry
    conv_rows(shift_d, 1, last, 0)
    give(dxb)
    along = line_finish(2, line_x)
    plain[...] = along[8 * units:]
    straight = line_finish(4, line_f)
    mixed = []
    for q in range(units):
        u = in_plane * units + q
        r = pl.multiple_of(jnp.minimum(lax.div(u, tiles), chan // 8 - 1) * 8, 8)
        k, d, x = [kcol[i, pl.ds(r, 8)] for i in range(3)]
        part = slice(q * 8, q * 8 + 8)
        mixed.append(k * (straight[part] - d * plain[pl.ds(lax.rem(u, tiles), 1)]
                          - x * along[part]))
    share(0, jnp.concatenate(mixed, axis=0))
    share(1, line_finish(6, line_h) * factor)
    for k, row in enumerate((row_one, row_two)):
        for j in range(2):
            gnorm[2 * k + j:2 * k + j + 1, :] = row[:, j * chan:(j + 1) * chan] * factor
    spell(0, gw1)
    spell(1, gw2)


def deliver(*refs):
    sem = refs[-1]
    half = (len(refs) - 1) // 2
    copies = [pltpu.make_async_copy(src, dst, sem.at[k])
              for k, (src, dst) in enumerate(zip(refs[:half], refs[half:-1]))]
    for copy in copies:
        copy.start()
    for copy in copies:
        copy.wait()


def body(sizes, x_a, x_b, w_first, w_second, gain_first, bias_first, gain_second, bias_second,
         grad_out):
    chan, nx, ny, nz = x_a.shape
    count = math.prod(sizes)
    voxels = float(nx * ny * nz * count)
    taps = 27 * chan
    bf16, f32 = jnp.bfloat16, jnp.float32
    tiles = -(-taps // nz)
    plane = sizes[1] * sizes[2]
    units = -(-tiles * (chan // 8) // plane)
    full = (nx + 2, ny + 2, chan, nz)
    span = (nx + 2) * (ny + 2)
    grid = (nx, ny, chan, nz)
    vmem = pl.BlockSpec(memory_space=pltpu.VMEM)
    hbm = pl.BlockSpec(memory_space=pltpu.HBM)
    dma = pltpu.SemaphoreType.DMA
    shapes = (
        jax.ShapeDtypeStruct(x_a.shape, bf16),
        jax.ShapeDtypeStruct(x_a.shape, bf16),
        jax.ShapeDtypeStruct((27, chan, chan), f32),
        jax.ShapeDtypeStruct((27, chan, chan), f32),
        jax.ShapeDtypeStruct((4, chan), f32),
    )
    results = pl.pallas_call(
        functools.partial(kernel, sizes, voxels, units),
        out_shape=shapes,
        in_specs=[hbm] * 9,
        out_specs=[vmem] * 5,
        scratch_shapes=[
            pltpu.VMEM((3, chan, nx, ny, nz), bf16),
            pltpu.VMEM((2, 27, chan, chan), bf16),
            pltpu.VMEM((4, 1, chan), f32),
            pltpu.VMEM((chan * (nx * ny + 8), nz), f32),
            pltpu.VMEM((4, DEEP * chan, 9 * (DEEP + 2) * chan), bf16),
            pltpu.VMEM((7,) + full, bf16),
            pltpu.VMEM((7, chan, nz), bf16),
            pltpu.VMEM((7, 27, chan, nz), bf16),
            pltpu.VMEM((7, nx + 2, chan, nz), bf16),
            pltpu.VMEM((2, nx + 2, chan, nz), f32),
            pltpu.VMEM((3, nx + 2, 4, chan, nz), f32),
        ] + [pltpu.VMEM((span, 3 * chan, nz), bf16)] * 4
        + [pltpu.VMEM(full, f32)] * 2
        + [pltpu.VMEM(grid, f32)] * 5
        + [
            pltpu.VMEM(grid, bf16),
            pltpu.VMEM((6, count, 1, nz), f32),
            pltpu.VMEM((1, tiles * nz), f32),
            pltpu.VMEM((8, nz), f32),
            pltpu.VMEM((3, chan, nz), f32),
            pltpu.VMEM((chan, tiles * nz), f32),
            pltpu.VMEM((plane, 8 * units + 8, nz), f32),
            pltpu.VMEM((plane, 8 * units + 8, nz), f32),
            pltpu.VMEM((sizes[0], 8 * units + 8, nz), f32),
            pltpu.VMEM((plane, 8 * units, nz), f32),
            pltpu.VMEM((plane, 8 * units, nz), f32),
            pltpu.VMEM((sizes[0], 8 * units, nz), f32),
            pltpu.VMEM((plane, 8 * units, nz), bf16),
            pltpu.VMEM((plane, 8 * units, nz), bf16),
            pltpu.VMEM((sizes[0], 8 * units, nz), bf16),
            pltpu.VMEM((2, plane, 8 * units, nz), bf16),
            pltpu.VMEM((2 * (ny + 8), chan, nz), bf16),
            dma((9,)),
            dma((7, 2)), dma((7, 2)),
            dma((6,)), dma((6,)),
            dma((8,)), dma((8,)),
        ],
        compiler_params=pltpu.CompilerParams(
            collective_id=0, has_side_effects=True, vmem_limit_bytes=40 * 1024 * 1024),
    )(*[pltpu.with_memory_space_constraint(v, pltpu.HBM) for v in (
        x_a, x_b, grad_out,
        w_first.reshape(27, chan, chan), w_second.reshape(27, chan, chan),
        gain_first.reshape(1, chan), bias_first.reshape(1, chan),
        gain_second.reshape(1, chan), bias_second.reshape(1, chan),
    )])
    y_a, dx_b, gw1, gw2, gnorm = pl.pallas_call(
        deliver,
        out_shape=shapes,
        in_specs=[vmem] * 5,
        out_specs=[hbm] * 5,
        scratch_shapes=[dma((5,))],
        compiler_params=pltpu.CompilerParams(vmem_limit_bytes=8 * 1024 * 1024),
    )(*results)
    cube = (3, 3, 3, chan, chan)
    return y_a, dx_b, gw1.reshape(cube), gw2.reshape(cube), gnorm


def solution(mesh):
    sizes = tuple(mesh.shape[a] for a in AXES)
    split = P(None, *AXES)
    return jax.shard_map(
        functools.partial(body, sizes),
        mesh=mesh,
        in_specs=(split, split, P(), P(), P(), P(), P(), P(), split),
        out_specs=(split, split, P(), P(), P()),
        check_vma=False,
    )
```

```python
import functools
import math

import jax
import jax.numpy as jnp
from jax import lax
from jax.experimental import pallas as pl
from jax.experimental.pallas import tpu as pltpu
from jax.sharding import PartitionSpec as P

EPSILON = 1e-05
AXES = ("gx", "gy", "gz")
MESH = pl.DeviceIdType.MESH
XB, XA, GO, C1B, C1A, C2B, E1 = range(7)
D2, D1 = range(2)
OFFSETS = [(a, b, c) for a in (-1, 0, 1) for b in (-1, 0, 1) for c in (-1, 0, 1)
           if (a, b, c) != (0, 0, 0)]
DEEP = 4


def sigmoid(z):
    return 0.5 * jnp.tanh(0.5 * z) + 0.5


def slope_of(z):
    s = sigmoid(z)
    return s * (1.0 + z * (1.0 - s))


def code(offset):
    a, b, c = offset
    return (a + 1) * 9 + (b + 1) * 3 + c + 1


def minus(offset):
    return tuple(-o for o in offset)


def kernel(
    sizes, voxels,
    xa, xb, go, w1, w2, g1, b1, g2, b2,
    ya, dxb, gw1, gw2, gnorm,
    raw, wraw, gains, tall, mats, pads, edge_out, edge_in, cols, dcols, offs,
    shift_xb, shift_a, shift_hb, shift_d,
    fd2, fd1, c1b, c1a, c2b, c2a, e1, d1h, slots, xsum, wsum,
    unit_x, slot_x, line_x, unit_f, slot_f, line_f, unit_h, slot_h, line_h, wfull,
    bytes_of, load_sem, halo_send, halo_recv, sum_send, sum_recv, w_send, w_recv,
):
    chan, nx, ny, nz = raw.shape[1:]
    wide = ny + 2
    own = nx * ny
    pitch = tall.shape[0] // chan
    count = math.prod(sizes)
    local = float(own * nz)
    factor = 1.0 / math.sqrt(voxels)
    tiles = wsum.shape[1] // nz
    me = [lax.axis_index(a) for a in AXES]

    def rank_of(place):
        return (place[0] * sizes[1] + place[1]) * sizes[2] + place[2]
    rank = rank_of(me)
    lane = lax.broadcasted_iota(jnp.int32, (chan, nz), 1)
    chan_of = lax.broadcasted_iota(jnp.int32, (chan, nz), 0)
    odd = lax.rem(lane, 2) == 1
    zero = jnp.zeros((chan, nz), jnp.float32)
    bf16, f32 = jnp.bfloat16, jnp.float32

    others = [(a, b, c) for a in range(sizes[0]) for b in range(sizes[1])
              for c in range(sizes[2])][:0:-1]

    def at_offset(offset):
        return [lax.rem(m + o + s, s) for m, o, s in zip(me, offset, sizes)]

    def ids(place):
        return dict(zip(AXES, place))

    barrier = pltpu.get_barrier_semaphore()
    for offset in others:
        pl.semaphore_signal(
            barrier, inc=1, device_id=ids(at_offset(offset)), device_id_type=MESH)

    loads = []
    for at, (src, dst) in enumerate((
            (xb, raw.at[0]), (w1, wraw.at[0]), (xa, raw.at[1]), (go, raw.at[2]),
            (w2, wraw.at[1]), (g1, gains.at[0]), (b1, gains.at[1]), (g2, gains.at[2]),
            (b2, gains.at[3]))):
        copy = pltpu.make_async_copy(src, dst, load_sem.at[at])
        copy.start()
        loads.append(copy)

    inside = []
    for k in range(3):
        inside.append({-1: me[k] > 0, 0: None, 1: me[k] < sizes[k] - 1})

    def reaches(offset):
        known = [inside[k][o] for k, o in enumerate(offset) if o]
        flag = known[0]
        for more in known[1:]:
            flag = jnp.logical_and(flag, more)
        return flag

    SIDES, FIRST, LAST = range(3)
    split = ny // 2 + 1

    def halo_pieces(v, offset):
        if offset[2]:
            part = FIRST if offset[0] else SIDES
            return [(part, edge_out.at[v], edge_in.at[v, code(offset)])]

        def cut(o, n):
            if o == 0:
                return pl.ds(1, n), pl.ds(1, n)
            return (n, 0) if o > 0 else (1, n + 1)
        (sx, dx), (sy, dy) = cut(offset[0], nx), cut(offset[1], ny)
        if offset[0] and not offset[1]:
            return [(part, pads.at[v, sx, rows], pads.at[v, dx, rows])
                    for part, rows in ((FIRST, pl.ds(1, split)),
                                       (LAST, pl.ds(1 + split, ny - split)))]
        part = FIRST if offset[0] else SIDES
        return [(part, pads.at[v, sx, sy], pads.at[v, dx, dy])]

    order = sorted(OFFSETS, key=lambda o: (o[1] == 0 and o[2] == 0, o[0] != 0))

    def halo_start(v):
        for offset in order:
            to = ids([me[k] + o for k, o in enumerate(offset)])

            @pl.when(reaches(offset))
            def _(offset=offset, to=to):
                for part, src, dst in halo_pieces(v, offset):
                    pltpu.make_async_remote_copy(
                        src_ref=src, dst_ref=dst, send_sem=halo_send.at[v, part],
                        recv_sem=halo_recv.at[v, part], device_id=to,
                        device_id_type=MESH).start()

    near = [jnp.where(inside[k][-1], 1, 0) + jnp.where(inside[k][1], 1, 0) for k in range(3)]
    cases = [(0,) if n == 1 else (1,) if n == 2 else (1, 2) for n in sizes]

    def halo_wait(v, part):
        for a in ((0,) if part == SIDES else cases[0]):
            for b in (0,) if part == LAST else cases[1]:
                for c in (0,) if part == LAST else cases[2]:
                    edges = b + c * (1 + b)
                    rows = (b * nx + c * (1 + b), a * (split + edges), a * (ny - split))[part]
                    if not rows:
                        continue
                    known = []
                    if part != SIDES:
                        known.append(near[0] == a)
                    if part != LAST:
                        known += [near[1] == b, near[2] == c]
                    flag = known[0]
                    for more in known[1:]:
                        flag = jnp.logical_and(flag, more)

                    @pl.when(flag)
                    def _(rows=rows):
                        some = bytes_of.at[pl.ds(0, rows)]
                        for sem in (halo_recv.at[v, part], halo_send.at[v, part]):
                            pltpu.make_async_copy(some, some, sem).wait()

    def total(value):
        return jnp.sum(value, axis=1, keepdims=True)

    def spread(value):
        return jnp.broadcast_to(value, zero.shape)

    def turned(tile, by):
        by = by % nz
        return pltpu.roll(tile, by, 1) if by else tile

    def emit(v, tile_of, centre=None):
        def step(x, edge):
            for y in range(ny):
                tile = tile_of(x, y)
                if centre is not None:
                    tile = tile - centre
                tile = tile.astype(bf16)
                pads[v, x + 1, y + 1] = tile
                r = 2 * (x * ny + y)
                edge = jnp.where(lane == r, tile[:, nz - 1:nz], edge)
                edge = jnp.where(lane == r + 1, tile[:, 0:1], edge)
            return edge
        edge_out[v] = lax.fori_loop(0, nx, step, zero.astype(bf16))

    first_lanes = jnp.logical_or(lane == 0, lane == nz - 1)
    last_lanes = jnp.logical_or(lane == 2 * ny + 1, lane == 2 * ny + 2)

    def by_row(first, middle, last):
        return jnp.where(first_lanes, first, jnp.where(last_lanes, last, middle))

    def collect(v, part):
        for dx in (0,) if part == SIDES else (-1, 1):
            low, high = [[edge_in[v, code((-dx, -dy, -dz))] for dy in (-1, 0, 1)]
                         for dz in (-1, 1)]
            for x in range(1, nx + 1) if dx == 0 else (0,) if dx < 0 else (nx + 1,):
                base = (nx - 1, x - 1, 0)[dx + 1] * ny
                moves = (-2 * (base + ny), -2 * base, 2 * ny - 2 * base)
                got = [jnp.where(odd, turned(h, by), turned(l, by + 2))
                       for l, h, by in zip(low, high, moves)]
                cols[v, x] = by_row(*got)

    row_of_lane = jnp.where(lane == nz - 1, 0, lax.div(lane + 1, 2))
    low_y = jnp.where(me[1] > 0, 0, 1)
    high_y = jnp.where(me[1] < sizes[1] - 1, wide, wide - 1)
    low_z = jnp.where(me[2] > 0, 1, 0)
    high_z = jnp.where(me[2] < sizes[2] - 1, 1, 0)
    keep_edge = jnp.where(jnp.logical_and(row_of_lane >= low_y, row_of_lane < high_y),
                          jnp.where(odd, high_z, low_z), 0)

    def build(tile_of, shifted, turn, part):
        inner = part == SIDES
        rows = (range(wide), range(split + 1), range(split + 1, wide))[part]

        def step(i, carry):
            if inner:
                x, x_ok = i + 1, None
            else:
                x = i * (nx + 1)
                x_ok = jnp.where(i == 0, me[0], sizes[0] - 1 - me[0]) > 0

            def both(flag):
                return flag if x_ok is None else jnp.logical_and(x_ok, flag)
            limits = {0: jnp.where(both(me[1] > 0), nz, 0),
                      wide - 1: jnp.where(both(me[1] < sizes[1] - 1), nz, 0)}
            middle = None if inner else jnp.where(x_ok, nz, 0)
            least = 1 if inner else jnp.where(x_ok, 1, 2)
            edge = tile_of(x, wide, inner)
            edge = jnp.where(keep_edge >= least, edge, jnp.zeros_like(edge)).astype(bf16)
            for y in rows:
                tile = tile_of(x, y, inner)
                limit = limits.get(y, middle)
                if limit is not None:
                    tile = jnp.where(lane < limit, tile, jnp.zeros_like(tile))
                tile = tile.astype(bf16)
                ends = turned(edge, -2 * y)
                low = jnp.where(lane == 0, ends, turned(tile, 1))
                high = jnp.where(lane == nz - 1, ends, turned(tile, -1))
                row = x * wide + y
                shifted[row, 0:chan] = high if turn else low
                shifted[row, chan:2 * chan] = tile
                shifted[row, 2 * chan:] = low if turn else high
            return carry
        lax.fori_loop(0, nx if inner else 2, step, 0)

    def raw_tiles(v):
        def tile_of(x, y, inner):
            return cols[v, x] if isinstance(y, int) and y == wide else pads[v, x, y]
        return tile_of

    def centred(v, k, full):
        def tile_of(x, y, inner):
            if not isinstance(y, int):
                return pads[v, x, y].astype(f32) + offs[k, x, 1]
            if y == wide:
                return cols[v, x].astype(f32) + offs[k, x, 3]
            if inner and 0 < y < wide - 1:
                return full[x - 1, y - 1] + offs[k, x, 1]
            kind = 0 if y == 0 else 2 if y == wide - 1 else 1
            return pads[v, x, y].astype(f32) + offs[k, x, kind]
        return tile_of

    def halo_rows(fn):
        for x in range(1, nx + 1):
            for y in (0, wide - 1):
                fn(x, y, True)

    def stack_rows(shifted, a, y, deep):
        parts = []
        for yi in range(deep + 2):
            parts.append(jnp.concatenate(
                [shifted[(x + a) * wide + y + yi] for x in range(nx)], axis=1))
        return parts

    def conv_rows(shifted, w, finish, carry, between):
        groups = ny // DEEP
        for half in range(2):
            def step(i, carry):
                y0 = i * DEEP
                data = jnp.concatenate(
                    [p for a in range(3) for p in stack_rows(shifted, a, y0, DEEP)], axis=0)
                o = jnp.dot(mats[w], data, preferred_element_type=f32)
                for x in range(nx):
                    for u in range(DEEP):
                        carry = finish(
                            x, y0 + u, o[u * chan:(u + 1) * chan, x * nz:(x + 1) * nz], carry)
                return carry
            if half:
                between()
            carry = lax.fori_loop(
                half * (groups // 2), groups // 2 if half == 0 else groups, step, carry,
                unroll=2)
        return carry

    def conv_stats(shifted, w, full, between):
        def finish(x, y, o, carry):
            full[x, y] = o
            return carry[0] + o, carry[1] + o * o
        return conv_rows(shifted, w, finish, (zero, zero), between)

    def row_of(values):
        tile = zero
        for k, value in enumerate(values):
            tile = jnp.where(lane == k * chan + chan_of, value, tile)
        return jnp.sum(tile, axis=0, keepdims=True)

    def column(row, k):
        return total(jnp.where(lane == k * chan + chan_of, row, 0.0))

    def all_start(buf, value, send, recv):
        buf[rank] = value
        for offset in others:
            pltpu.make_async_remote_copy(
                src_ref=buf.at[rank], dst_ref=buf.at[rank], send_sem=send,
                recv_sem=recv, device_id=ids(at_offset(offset)), device_id_type=MESH).start()

    def wait_bytes(buf, n, *sems):
        some = buf.at[pl.ds(0, n - 1)]
        for sem in sems:
            pltpu.make_async_copy(some, some, sem).wait()

    def tree(values):
        while len(values) > 1:
            values = [values[i] + values[i + 1] if i + 1 < len(values) else values[i]
                      for i in range(0, len(values), 2)]
        return values[0]

    def sums_start(j, values):
        all_start(slots.at[j], row_of([total(v) for v in values]), sum_send.at[j],
                  sum_recv.at[j])

    def sums_finish(j):
        wait_bytes(slots.at[j], count, sum_recv.at[j], sum_send.at[j])
        return tree([slots[j, r] for r in range(count)])

    def norm(row):
        mean = column(row, 0) / voxels
        var = column(row, 1) / voxels - mean * mean
        return spread(mean), spread(lax.rsqrt(var + EPSILON))

    def rounded(value):
        return spread(value / local).astype(bf16).astype(f32)

    def centre_of(sums):
        return rounded(total(sums[0]))

    def set_offsets(k, j, mean, part):
        def off(offset):
            return rounded(column(slots[j, rank_of(at_offset(offset))], 0)) - mean
        for dx in (0,) if part == SIDES else (-1, 1):
            rows = [-mean if dx == 0 and dy == 0 else off((dx, dy, 0)) for dy in (-1, 0, 1)]
            edges = by_row(*[jnp.where(odd, off((dx, dy, 1)), off((dx, dy, -1)))
                             for dy in (-1, 0, 1)])
            for x in range(1, nx + 1) if dx == 0 else (0,) if dx < 0 else (nx + 1,):
                for kind, value in enumerate(rows + [edges]):
                    offs[k, x, kind] = value

    plane = sizes[1] * sizes[2]
    assert plane >= tiles
    in_plane = lax.rem(rank, plane)
    owner = in_plane < tiles
    plane_others = [o for o in others if o[0] == 0]
    line_others = [o for o in others if o[1] == 0 and o[2] == 0]

    def send_some(group, src, dst, send, recv):
        for offset in group:
            pltpu.make_async_remote_copy(
                src_ref=src, dst_ref=dst, send_sem=send, recv_sem=recv,
                device_id=ids(at_offset(offset)), device_id_type=MESH).start()

    def plane_start(j, unit, slot):
        for t in range(tiles):
            unit[t, 0:chan] = wsum[:, t * nz:(t + 1) * nz].astype(unit.dtype)
            if unit.shape[1] > chan:
                unit[t, chan:chan + 1] = xsum[:, t * nz:(t + 1) * nz]
        for t in range(tiles):
            @pl.when(in_plane != t)
            def _(t=t):
                pltpu.make_async_remote_copy(
                    src_ref=unit.at[t], dst_ref=slot.at[in_plane], send_sem=w_send.at[j],
                    recv_sem=w_recv.at[j], device_id_type=MESH,
                    device_id={AXES[1]: t // sizes[2], AXES[2]: t % sizes[2]}).start()

        @pl.when(owner)
        def _():
            slot[in_plane] = unit[in_plane]

    def added(buf, n):
        return tree([buf[r].astype(f32) for r in range(n)])

    def line_start(j, unit, slot, line):
        @pl.when(owner)
        def _():
            wait_bytes(slot, plane, w_recv.at[j])
            wait_bytes(unit, tiles, w_send.at[j])
            line[me[0]] = added(slot, plane).astype(line.dtype)
            here = line.at[me[0]]
            send_some(line_others, here, here, w_send.at[j + 1], w_recv.at[j + 1])

        @pl.when(jnp.logical_not(owner))
        def _():
            wait_bytes(unit, tiles + 1, w_send.at[j])

    def line_sum(j, line):
        wait_bytes(line, sizes[0], w_recv.at[j + 1], w_send.at[j + 1])
        return added(line, sizes[0])

    def share(j, value):
        wfull[j, in_plane] = value.astype(bf16)
        here = wfull.at[j, in_plane]
        send_some(plane_others, here, here, w_send.at[j], w_recv.at[j])

    def spell(j, out):
        @pl.when(owner)
        def _():
            wait_bytes(wfull.at[j], tiles, w_recv.at[j])
            wait_bytes(wfull.at[j], plane, w_send.at[j])

        @pl.when(jnp.logical_not(owner))
        def _():
            wait_bytes(wfull.at[j], tiles + 1, w_recv.at[j])
        for t in range(tiles):
            piece = wfull[j, t].astype(f32)
            for k in range(nz // chan):
                tap = t * (nz // chan) + k
                if tap < 27:
                    out[tap] = piece[:, k * chan:(k + 1) * chan]

    def wgrad(delta_of, shifted, ones=False):
        cuts = []
        for g in range(ny // DEEP):
            for x in range(nx):
                parts = [delta_of(x, g * DEEP + u) for u in range(DEEP)]
                if ones:
                    parts.append(jnp.ones((16, nz), bf16))
                cuts.append(jnp.concatenate(parts, axis=0))
        delta = jnp.concatenate(cuts, axis=1)
        span = 3 * chan
        for a in range(3):
            groups = [jnp.concatenate(stack_rows(shifted, a, g * DEEP, DEEP), axis=0)
                      for g in range(ny // DEEP)]
            o = lax.dot_general(
                delta, jnp.concatenate(groups, axis=1), (((1,), (1,)), ((), ())),
                preferred_element_type=f32)
            for ty in range(3):
                at = (a * 3 + ty) * span
                wsum[:, at:at + span] = tree(
                    [o[u * chan:(u + 1) * chan, (u + ty) * span:(u + ty + 1) * span]
                     for u in range(DEEP)])
                if ones:
                    xsum[:, at:at + span] = tree(
                        [o[DEEP * chan:DEEP * chan + 1, (u + ty) * span:(u + ty + 1) * span]
                         for u in range(DEEP)])

    def take(k):
        def step(c, carry):
            at_row = pl.multiple_of(c * pitch, 8)
            for x in range(nx):
                tall[pl.ds(at_row + x * ny, ny)] = raw[k, c, x].astype(f32)
            return carry
        lax.fori_loop(0, chan, step, 0, unroll=4)

        def tile_of(x, y):
            return tall[pl.ds(x * ny + y, chan, stride=pitch)]
        return tile_of

    def give(out):
        def step(c, carry):
            at_row = pl.multiple_of(c * pitch, 8)
            for x in range(nx):
                out[c, x] = tall[pl.ds(at_row + x * ny, ny)].astype(bf16)
            return carry
        lax.fori_loop(0, chan, step, 0, unroll=4)

    def put_row(x, y, tile):
        tall[pl.ds(x * ny + y, chan, stride=pitch)] = tile

    def prepare(k):
        taps = [wraw[k, t].astype(f32) for t in range(27)]
        span = 3 * chan
        for turn in range(2):
            flat = jnp.concatenate(taps, axis=0).T if turn else jnp.concatenate(taps, axis=1)
            none = jnp.zeros((chan, span), f32)
            for u in range(DEEP):
                parts = []
                for a in range(3):
                    for yi in range(DEEP + 2):
                        tx, ty = (2 - a, 2 - yi + u) if turn else (a, yi - u)
                        at = (tx * 3 + ty) * span
                        parts.append(flat[:, at:at + span] if 0 <= ty < 3 else none)
                mats[2 * k + turn, u * chan:(u + 1) * chan] = jnp.concatenate(
                    parts, axis=1).astype(bf16)

    loads[0].wait()
    emit(XB, take(0))
    pl.semaphore_wait(barrier, count - 1)
    halo_start(XB)
    loads[2].wait()
    emit(XA, take(1))
    halo_start(XA)
    loads[3].wait()
    emit(GO, take(2))
    loads[1].wait()
    prepare(0)
    loads[4].wait()
    prepare(1)
    for k in range(5, 9):
        loads[k].wait()

    def gain(k):
        value = spread(jnp.concatenate([gains[k]] * (nz // chan), axis=1))
        return spread(column(value, 0))
    gain_one, bias_one, gain_two, bias_two = [gain(k) for k in range(4)]

    def bring(v, shifted, tile_of, part, ready=None):
        if part != LAST and ready is not None:
            ready(part)
        halo_wait(v, part)
        if part != LAST:
            collect(v, part)
        build(tile_of, shifted, False, part)

    def bring_conv(v, shifted, tile_of, w, full, ready=None):
        bring(v, shifted, tile_of, SIDES, ready)
        bring(v, shifted, tile_of, FIRST, ready)
        return conv_stats(shifted, w, full, lambda: bring(v, shifted, tile_of, LAST))

    sums = bring_conv(XB, shift_xb, raw_tiles(XB), 0, c1b)
    sums_start(0, sums)
    emit(C1B, lambda x, y: c1b[x, y], centre_of(sums))
    halo_start(C1B)

    sums = bring_conv(XA, shift_a, raw_tiles(XA), 0, c1a)
    sums_start(1, sums)
    emit(C1A, lambda x, y: c1a[x, y], centre_of(sums))
    halo_start(C1A)

    def silu(z):
        return z * sigmoid(z)

    mean_one, scale_one = norm(sums_finish(0))
    steep_one = gain_one * scale_one
    tile_1b = centred(C1B, 0, c1b)

    def z_one(x, y, inner):
        return tile_1b(x, y, inner) * steep_one + bias_one
    sums = bring_conv(C1B, shift_hb, lambda *at: silu(z_one(*at)), 2, c2b,
                      lambda part: set_offsets(0, 0, mean_one, part))
    sums_start(2, sums)
    emit(C2B, lambda x, y: c2b[x, y], centre_of(sums))
    halo_start(C2B)

    mean_a, scale_a = norm(sums_finish(1))
    steep_a = gain_one * scale_a
    tile_1a = centred(C1A, 1, c1a)
    sums = bring_conv(C1A, shift_a, lambda *at: silu(tile_1a(*at) * steep_a + bias_one), 2,
                      c2a, lambda part: set_offsets(1, 1, mean_a, part))
    sums_start(3, sums)

    mean_two, scale_two = norm(sums_finish(2))
    steep_two = gain_two * scale_two

    def own_two(x, carry):
        sd, sx = carry
        for y in range(ny):
            c = c2b[x, y] - mean_two
            d = pads[GO, x + 1, y + 1].astype(f32) * slope_of(c * steep_two + bias_two)
            fd2[x + 1, y + 1] = d
            sd, sx = sd + d, sx + d * c
        return sd, sx
    sd, sx = lax.fori_loop(0, nx, own_two, (zero, zero))
    sums_start(4, (sx * scale_two, sd))
    halo_start(GO)

    wgrad(lambda x, y: ((c1b[x, y] - mean_one) * scale_one).astype(bf16), shift_xb,
          True)
    plane_start(2, unit_x, slot_x)

    tile_2b = centred(C2B, 2, c2b)
    tile_go = raw_tiles(GO)

    def d_two(*at):
        return tile_go(*at).astype(f32) * slope_of(tile_2b(*at) * steep_two + bias_two)

    def halo_two(x, y, inner):
        fd2[x, y] = d_two(x, y, inner)

    set_offsets(2, 2, mean_two, SIDES)
    halo_wait(C2B, SIDES)
    collect(C2B, SIDES)
    halo_wait(GO, SIDES)
    collect(GO, SIDES)
    halo_rows(halo_two)
    for x in range(1, nx + 1):
        dcols[D2, x] = d_two(x, wide, True)
    set_offsets(2, 2, mean_two, FIRST)
    halo_wait(C2B, FIRST)
    collect(C2B, FIRST)
    halo_wait(C2B, LAST)

    mean_a2, scale_a2 = norm(sums_finish(3))
    steep_a2 = gain_two * scale_a2

    def finish_a(x, carry):
        for y in range(ny):
            put_row(x, y, silu((c2a[x, y] - mean_a2) * steep_a2 + bias_two))
        return carry
    lax.fori_loop(0, nx, finish_a, 0)
    give(ya)

    row_two = sums_finish(4)
    sx2 = spread(column(row_two, 0) / voxels) * scale_two
    sd2 = spread(column(row_two, 1) / voxels)

    def dc_two(x, y, inner):
        c = tile_2b(x, y, inner)
        if not inner:
            d = tile_go(x, y, inner).astype(f32) * slope_of(c * steep_two + bias_two)
        else:
            d = dcols[D2, x] if y == wide else fd2[x, y]
        return steep_two * (d - sd2 - c * sx2)
    build(dc_two, shift_d, True, SIDES)
    halo_wait(GO, FIRST)
    collect(GO, FIRST)
    build(dc_two, shift_d, True, FIRST)

    def rest_two():
        line_start(2, unit_x, slot_x, line_x)
        halo_wait(GO, LAST)
        build(dc_two, shift_d, True, LAST)

    def back(x, y, o, carry):
        sd, sx = carry
        e1[x, y] = o
        c = c1b[x, y] - mean_one
        d = o * slope_of(c * steep_one + bias_one)
        fd1[x + 1, y + 1] = d
        d1h[x, y] = d.astype(bf16)
        return sd + d, sx + d * c
    sd, sx = conv_rows(shift_d, 3, back, (zero, zero), rest_two)
    sums_start(5, (sx * scale_one, sd))
    emit(E1, lambda x, y: e1[x, y])
    halo_start(E1)
    wgrad(lambda x, y: d1h[x, y], shift_xb)
    plane_start(4, unit_f, slot_f)
    wgrad(lambda x, y: shift_d[(x + 1) * wide + y + 1, chan:2 * chan], shift_hb)
    plane_start(6, unit_h, slot_h)

    row_one = sums_finish(5)
    sx1_wide = spread(column(row_one, 0) / voxels)
    sx1 = sx1_wide * scale_one
    sd1 = spread(column(row_one, 1) / voxels)
    line_start(4, unit_f, slot_f, line_f)
    def halo_one(x, y, inner):
        fd1[x, y] = pads[E1, x, y].astype(f32) * slope_of(z_one(x, y, inner))

    def dc_one(x, y, inner):
        c = tile_1b(x, y, inner)
        if inner:
            d = dcols[D1, x] if y == wide else fd1[x, y]
        else:
            e = cols[E1, x] if y == wide else pads[E1, x, y]
            d = e.astype(f32) * slope_of(c * steep_one + bias_one)
        return steep_one * (d - sd1 - c * sx1)

    halo_wait(E1, SIDES)
    collect(E1, SIDES)
    halo_rows(halo_one)
    for x in range(1, nx + 1):
        dcols[D1, x] = cols[E1, x].astype(f32) * slope_of(z_one(x, wide, True))
    build(dc_one, shift_d, True, SIDES)

    halo_wait(E1, FIRST)
    collect(E1, FIRST)
    build(dc_one, shift_d, True, FIRST)
    line_start(6, unit_h, slot_h, line_h)

    def rest_one():
        halo_wait(E1, LAST)
        build(dc_one, shift_d, True, LAST)

    def last(x, y, o, carry):
        put_row(x, y, o)
        return carry
    conv_rows(shift_d, 1, last, 0, rest_one)
    give(dxb)

    @pl.when(owner)
    def _():
        along = line_sum(2, line_x)
        share(0, steep_one * factor * (
            line_sum(4, line_f) - sd1 * along[chan:chan + 1] - sx1_wide * along[0:chan]))
        share(1, line_sum(6, line_h) * factor)
    for k, row in enumerate((row_one, row_two)):
        for j in range(2):
            gnorm[2 * k + j:2 * k + j + 1, :] = row[:, j * chan:(j + 1) * chan] * factor
    spell(0, gw1)
    spell(1, gw2)


def deliver(*refs):
    sem = refs[-1]
    half = (len(refs) - 1) // 2
    copies = [pltpu.make_async_copy(src, dst, sem.at[k])
              for k, (src, dst) in enumerate(zip(refs[:half], refs[half:-1]))]
    for copy in copies:
        copy.start()
    for copy in copies:
        copy.wait()


def body(sizes, x_a, x_b, w_first, w_second, gain_first, bias_first, gain_second, bias_second,
         grad_out):
    chan, nx, ny, nz = x_a.shape
    count = math.prod(sizes)
    voxels = float(nx * ny * nz * count)
    taps = 27 * chan
    bf16, f32 = jnp.bfloat16, jnp.float32
    tiles = -(-taps // nz)
    plane = sizes[1] * sizes[2]
    full = (nx + 2, ny + 2, chan, nz)
    span = (nx + 2) * (ny + 2)
    grid = (nx, ny, chan, nz)
    vmem = pl.BlockSpec(memory_space=pltpu.VMEM)
    hbm = pl.BlockSpec(memory_space=pltpu.HBM)
    dma = pltpu.SemaphoreType.DMA
    shapes = (
        jax.ShapeDtypeStruct(x_a.shape, bf16),
        jax.ShapeDtypeStruct(x_a.shape, bf16),
        jax.ShapeDtypeStruct((27, chan, chan), f32),
        jax.ShapeDtypeStruct((27, chan, chan), f32),
        jax.ShapeDtypeStruct((4, chan), f32),
    )
    results = pl.pallas_call(
        functools.partial(kernel, sizes, voxels),
        out_shape=shapes,
        in_specs=[hbm] * 9,
        out_specs=[vmem] * 5,
        scratch_shapes=[
            pltpu.VMEM((3, chan, nx, ny, nz), bf16),
            pltpu.VMEM((2, 27, chan, chan), bf16),
            pltpu.VMEM((4, 1, chan), f32),
            pltpu.VMEM((chan * (nx * ny + 8), nz), f32),
            pltpu.VMEM((4, DEEP * chan, 9 * (DEEP + 2) * chan), bf16),
            pltpu.VMEM((7,) + full, bf16),
            pltpu.VMEM((7, chan, nz), bf16),
            pltpu.VMEM((7, 27, chan, nz), bf16),
            pltpu.VMEM((7, nx + 2, chan, nz), bf16),
            pltpu.VMEM((2, nx + 2, chan, nz), f32),
            pltpu.VMEM((3, nx + 2, 4, chan, nz), f32),
        ] + [pltpu.VMEM((span, 3 * chan, nz), bf16)] * 4
        + [pltpu.VMEM(full, f32)] * 2
        + [pltpu.VMEM(grid, f32)] * 5
        + [
            pltpu.VMEM(grid, bf16),
            pltpu.VMEM((6, count, 1, nz), f32),
            pltpu.VMEM((1, tiles * nz), f32),
            pltpu.VMEM((chan, tiles * nz), f32),
            pltpu.VMEM((tiles + 1, chan + 8, nz), f32),
            pltpu.VMEM((plane, chan + 8, nz), f32),
            pltpu.VMEM((sizes[0], chan + 8, nz), f32),
            pltpu.VMEM((tiles + 1, chan, nz), f32),
            pltpu.VMEM((plane, chan, nz), f32),
            pltpu.VMEM((sizes[0], chan, nz), f32),
            pltpu.VMEM((tiles + 1, chan, nz), bf16),
            pltpu.VMEM((plane, chan, nz), bf16),
            pltpu.VMEM((sizes[0], chan, nz), bf16),
            pltpu.VMEM((2, plane + 1, chan, nz), bf16),
            pltpu.VMEM((2 * (ny + 8), chan, nz), bf16),
            dma((9,)),
            dma((7, 3)), dma((7, 3)),
            dma((6,)), dma((6,)),
            dma((8,)), dma((8,)),
        ],
        compiler_params=pltpu.CompilerParams(
            collective_id=0, has_side_effects=True, vmem_limit_bytes=40 * 1024 * 1024),
    )(*[pltpu.with_memory_space_constraint(v, pltpu.HBM) for v in (
        x_a, x_b, grad_out,
        w_first.reshape(27, chan, chan), w_second.reshape(27, chan, chan),
        gain_first.reshape(1, chan), bias_first.reshape(1, chan),
        gain_second.reshape(1, chan), bias_second.reshape(1, chan),
    )])
    y_a, dx_b, gw1, gw2, gnorm = pl.pallas_call(
        deliver,
        out_shape=shapes,
        in_specs=[vmem] * 5,
        out_specs=[hbm] * 5,
        scratch_shapes=[dma((5,))],
        compiler_params=pltpu.CompilerParams(vmem_limit_bytes=8 * 1024 * 1024),
    )(*results)
    cube = (3, 3, 3, chan, chan)
    return y_a, dx_b, gw1.reshape(cube), gw2.reshape(cube), gnorm


def solution(mesh):
    sizes = tuple(mesh.shape[a] for a in AXES)
    split = P(None, *AXES)
    return jax.shard_map(
        functools.partial(body, sizes),
        mesh=mesh,
        in_specs=(split, split, P(), P(), P(), P(), P(), P(), split),
        out_specs=(split, split, P(), P(), P()),
        check_vma=False,
    )
```

```python
import functools
import math

import jax
import jax.numpy as jnp
from jax import lax
from jax.experimental import pallas as pl
from jax.experimental.pallas import tpu as pltpu
from jax.sharding import PartitionSpec as P

EPSILON = 1e-05
AXES = ("gx", "gy", "gz")
MESH = pl.DeviceIdType.MESH
XB, XA, GO, C1B, C1A, C2B, E1 = range(7)
D2, D1 = range(2)
OFFSETS = [(a, b, c) for a in (-1, 0, 1) for b in (-1, 0, 1) for c in (-1, 0, 1)
           if (a, b, c) != (0, 0, 0)]
DEEP = 4


def sigmoid(z):
    return 0.5 * jnp.tanh(0.5 * z) + 0.5


def slope_of(z):
    s = sigmoid(z)
    return s * (1.0 + z * (1.0 - s))


def code(offset):
    a, b, c = offset
    return (a + 1) * 9 + (b + 1) * 3 + c + 1


def minus(offset):
    return tuple(-o for o in offset)


def kernel(
    sizes, voxels,
    xa, xb, go, w1, w2, g1, b1, g2, b2,
    ya, dxb, gw1, gw2, gnorm,
    raw, wraw, gains, tall, mats, pads, edge_out, edge_in, cols, dcols, offs,
    shift_xb, shift_a, shift_hb, shift_d,
    fd2, fd1, c1b, c1a, c2b, c2a, d1h, slots, xsum, wsum,
    unit_x, slot_x, line_x, unit_f, slot_f, line_f, unit_h, slot_h, line_h, wfull,
    bytes_of, load_sem, halo_send, halo_recv, sum_send, sum_recv, w_send, w_recv,
):
    chan, nx, ny, nz = raw.shape[1:]
    wide = ny + 2
    own = nx * ny
    pitch = tall.shape[0] // chan
    count = math.prod(sizes)
    local = float(own * nz)
    factor = 1.0 / math.sqrt(voxels)
    tiles = wsum.shape[1] // nz
    me = [lax.axis_index(a) for a in AXES]

    def rank_of(place):
        return (place[0] * sizes[1] + place[1]) * sizes[2] + place[2]
    rank = rank_of(me)
    lane = lax.broadcasted_iota(jnp.int32, (chan, nz), 1)
    chan_of = lax.broadcasted_iota(jnp.int32, (chan, nz), 0)
    odd = lax.rem(lane, 2) == 1
    zero = jnp.zeros((chan, nz), jnp.float32)
    bf16, f32 = jnp.bfloat16, jnp.float32

    others = [(a, b, c) for a in range(sizes[0]) for b in range(sizes[1])
              for c in range(sizes[2])][:0:-1]

    places = [{o: lax.rem(m + o + s, s) for o in range(-1, s)} for m, s in zip(me, sizes)]

    def at_offset(offset):
        return [places[k][o] for k, o in enumerate(offset)]

    def ids(place):
        return dict(zip(AXES, place))

    loads = []
    for at, (src, dst) in enumerate((
            (xb, raw.at[0]), (w1, wraw.at[0]), (xa, raw.at[1]), (go, raw.at[2]),
            (w2, wraw.at[1]), (g1, gains.at[0]), (b1, gains.at[1]), (g2, gains.at[2]),
            (b2, gains.at[3]))):
        copy = pltpu.make_async_copy(src, dst, load_sem.at[at])
        copy.start()
        loads.append(copy)

    barrier = pltpu.get_barrier_semaphore()
    for offset in others:
        pl.semaphore_signal(
            barrier, inc=1, device_id=ids(at_offset(offset)), device_id_type=MESH)

    inside = []
    for k in range(3):
        inside.append({-1: me[k] > 0, 0: None, 1: me[k] < sizes[k] - 1})

    def reaches(offset):
        known = [inside[k][o] for k, o in enumerate(offset) if o]
        flag = known[0]
        for more in known[1:]:
            flag = jnp.logical_and(flag, more)
        return flag

    SIDES, FIRST, LAST = range(3)
    split = ny // 2 + 1

    def halo_pieces(v, offset):
        if offset[2]:
            part = FIRST if offset[0] else SIDES
            return [(part, edge_out.at[v], edge_in.at[v, code(offset)])]

        def cut(o, n):
            if o == 0:
                return pl.ds(1, n), pl.ds(1, n)
            return (n, 0) if o > 0 else (1, n + 1)
        (sx, dx), (sy, dy) = cut(offset[0], nx), cut(offset[1], ny)
        if offset[0] and not offset[1]:
            return [(part, pads.at[v, sx, rows], pads.at[v, dx, rows])
                    for part, rows in ((FIRST, pl.ds(1, split)),
                                       (LAST, pl.ds(1 + split, ny - split)))]
        part = FIRST if offset[0] else SIDES
        return [(part, pads.at[v, sx, sy], pads.at[v, dx, dy])]

    order = sorted(OFFSETS, key=lambda o: (o[1] == 0 and o[2] == 0, o[0] != 0))

    def halo_start(v):
        for offset in order:
            to = ids([me[k] + o for k, o in enumerate(offset)])

            @pl.when(reaches(offset))
            def _(offset=offset, to=to):
                for part, src, dst in halo_pieces(v, offset):
                    pltpu.make_async_remote_copy(
                        src_ref=src, dst_ref=dst, send_sem=halo_send.at[v, part],
                        recv_sem=halo_recv.at[v, part], device_id=to,
                        device_id_type=MESH).start()

    near = [jnp.where(inside[k][-1], 1, 0) + jnp.where(inside[k][1], 1, 0) for k in range(3)]
    cases = [(0,) if n == 1 else (1,) if n == 2 else (1, 2) for n in sizes]

    def halo_wait(v, part):
        for a in ((0,) if part == SIDES else cases[0]):
            for b in (0,) if part == LAST else cases[1]:
                for c in (0,) if part == LAST else cases[2]:
                    edges = b + c * (1 + b)
                    rows = (b * nx + c * (1 + b), a * (split + edges), a * (ny - split))[part]
                    if not rows:
                        continue
                    known = []
                    if part != SIDES:
                        known.append(near[0] == a)
                    if part != LAST:
                        known += [near[1] == b, near[2] == c]
                    flag = known[0]
                    for more in known[1:]:
                        flag = jnp.logical_and(flag, more)

                    @pl.when(flag)
                    def _(rows=rows):
                        some = bytes_of.at[pl.ds(0, rows)]
                        for sem in (halo_recv.at[v, part], halo_send.at[v, part]):
                            pltpu.make_async_copy(some, some, sem).wait()

    def total(value):
        return jnp.sum(value, axis=1, keepdims=True)

    def spread(value):
        return jnp.broadcast_to(value, zero.shape)

    def turned(tile, by):
        by = by % nz
        return pltpu.roll(tile, by, 1) if by else tile

    def put(v, x, y, tile, edge):
        tile = tile.astype(bf16)
        pads[v, x + 1, y + 1] = tile
        r = 2 * (x * ny + y)
        edge = jnp.where(lane == r, tile[:, nz - 1:nz], edge)
        return jnp.where(lane == r + 1, tile[:, 0:1], edge)

    blank = jnp.zeros((chan, nz), bf16)

    def emit(v, tile_of):
        def step(x, edge):
            for y in range(ny):
                edge = put(v, x, y, tile_of(x, y), edge)
            return edge
        edge_out[v] = lax.fori_loop(0, nx, step, blank)

    first_lanes = jnp.logical_or(lane == 0, lane == nz - 1)
    last_lanes = jnp.logical_or(lane == 2 * ny + 1, lane == 2 * ny + 2)

    def by_row(first, middle, last):
        return jnp.where(first_lanes, first, jnp.where(last_lanes, last, middle))

    def collect(v, part):
        for dx in (0,) if part == SIDES else (-1, 1):
            low, high = [[edge_in[v, code((-dx, -dy, -dz))] for dy in (-1, 0, 1)]
                         for dz in (-1, 1)]
            for x in range(1, nx + 1) if dx == 0 else (0,) if dx < 0 else (nx + 1,):
                base = (nx - 1, x - 1, 0)[dx + 1] * ny
                moves = (-2 * (base + ny), -2 * base, 2 * ny - 2 * base)
                got = [jnp.where(odd, turned(h, by), turned(l, by + 2))
                       for l, h, by in zip(low, high, moves)]
                cols[v, x] = by_row(*got)

    row_of_lane = jnp.where(lane == nz - 1, 0, lax.div(lane + 1, 2))
    low_y = jnp.where(me[1] > 0, 0, 1)
    high_y = jnp.where(me[1] < sizes[1] - 1, wide, wide - 1)
    low_z = jnp.where(me[2] > 0, 1, 0)
    high_z = jnp.where(me[2] < sizes[2] - 1, 1, 0)
    keep_edge = jnp.where(jnp.logical_and(row_of_lane >= low_y, row_of_lane < high_y),
                          jnp.where(odd, high_z, low_z), 0)

    def build(tile_of, shifted, turn, part):
        inner = part == SIDES
        rows = (range(wide), range(split + 1), range(split + 1, wide))[part]

        def step(i, carry):
            if inner:
                x, x_ok = i + 1, None
            else:
                x = i * (nx + 1)
                x_ok = jnp.where(i == 0, me[0], sizes[0] - 1 - me[0]) > 0

            def both(flag):
                return flag if x_ok is None else jnp.logical_and(x_ok, flag)
            limits = {0: jnp.where(both(me[1] > 0), nz, 0),
                      wide - 1: jnp.where(both(me[1] < sizes[1] - 1), nz, 0)}
            middle = None if inner else jnp.where(x_ok, nz, 0)
            least = 1 if inner else jnp.where(x_ok, 1, 2)
            edge = tile_of(x, wide, inner)
            edge = jnp.where(keep_edge >= least, edge, jnp.zeros_like(edge)).astype(bf16)
            for y in rows:
                tile = tile_of(x, y, inner)
                limit = limits.get(y, middle)
                if limit is not None:
                    tile = jnp.where(lane < limit, tile, jnp.zeros_like(tile))
                tile = tile.astype(bf16)
                ends = turned(edge, -2 * y)
                low = jnp.where(lane == 0, ends, turned(tile, 1))
                high = jnp.where(lane == nz - 1, ends, turned(tile, -1))
                row = x * wide + y
                shifted[row, 0:chan] = high if turn else low
                shifted[row, chan:2 * chan] = tile
                shifted[row, 2 * chan:] = low if turn else high
            return carry
        lax.fori_loop(0, nx if inner else 2, step, 0)

    def raw_tiles(v):
        def tile_of(x, y, inner):
            return cols[v, x] if isinstance(y, int) and y == wide else pads[v, x, y]
        return tile_of

    def centred(v, k, full):
        def tile_of(x, y, inner):
            if not isinstance(y, int):
                return pads[v, x, y].astype(f32) + offs[k, x, 1]
            if y == wide:
                return cols[v, x].astype(f32) + offs[k, x, 3]
            if inner and 0 < y < wide - 1:
                return full[x - 1, y - 1] + offs[k, x, 1]
            kind = 0 if y == 0 else 2 if y == wide - 1 else 1
            return pads[v, x, y].astype(f32) + offs[k, x, kind]
        return tile_of

    def halo_rows(fn):
        for x in range(1, nx + 1):
            for y in (0, wide - 1):
                fn(x, y, True)

    def stack_rows(shifted, a, y, deep):
        parts = []
        for yi in range(deep + 2):
            parts.append(jnp.concatenate(
                [shifted[(x + a) * wide + y + yi] for x in range(nx)], axis=1))
        return parts

    def conv_rows(shifted, w, finish, carry, between):
        groups = ny // DEEP
        for half in range(2):
            def step(i, carry):
                y0 = i * DEEP
                data = jnp.concatenate(
                    [p for a in range(3) for p in stack_rows(shifted, a, y0, DEEP)], axis=0)
                o = jnp.dot(mats[w], data, preferred_element_type=f32)
                for x in range(nx):
                    for u in range(DEEP):
                        carry = finish(
                            x, y0 + u, o[u * chan:(u + 1) * chan, x * nz:(x + 1) * nz],
                            carry, half)
                return carry
            if half:
                carry = between(carry)
            carry = lax.fori_loop(
                half * (groups // 2), groups // 2 if half == 0 else groups, step, carry,
                unroll=2)
        return carry

    def conv_stats(v, shifted, w, full, between):
        centre = []

        def finish(x, y, o, carry, half):
            full[x, y] = o
            first, second, edge = carry
            if half and v is not None:
                edge = put(v, x, y, o - centre[0], edge)
            return first + o, second + o * o, edge

        def middle(carry):
            first, second, edge = carry
            if v is not None:
                mean = spread(total(first) / (0.5 * local))
                centre.append(mean.astype(bf16).astype(f32))
                for x in range(nx):
                    for y in range(ny // 2):
                        edge = put(v, x, y, full[x, y] - centre[0], edge)
            between()
            return first, second, edge
        first, second, edge = conv_rows(shifted, w, finish, (zero, zero, blank), middle)
        if v is None:
            return total(first), total(second)
        edge_out[v] = edge
        return total(first), total(second), centre[0]

    def row_of(values):
        tile = zero
        for k, value in enumerate(values):
            tile = jnp.where(lane == k * chan + chan_of, value, tile)
        return jnp.sum(tile, axis=0, keepdims=True)

    def column(row, k):
        return total(jnp.where(lane == k * chan + chan_of, row, 0.0))

    def all_start(buf, value, send, recv):
        buf[rank] = value
        for offset in others:
            pltpu.make_async_remote_copy(
                src_ref=buf.at[rank], dst_ref=buf.at[rank], send_sem=send,
                recv_sem=recv, device_id=ids(at_offset(offset)), device_id_type=MESH).start()

    def wait_bytes(buf, n, *sems):
        some = buf.at[pl.ds(0, n - 1)]
        for sem in sems:
            pltpu.make_async_copy(some, some, sem).wait()

    def tree(values):
        while len(values) > 1:
            values = [values[i] + values[i + 1] if i + 1 < len(values) else values[i]
                      for i in range(0, len(values), 2)]
        return values[0]

    def sums_start(j, values):
        all_start(slots.at[j], row_of(values), sum_send.at[j],
                  sum_recv.at[j])

    def sums_finish(j):
        wait_bytes(slots.at[j], count, sum_recv.at[j], sum_send.at[j])
        return tree([slots[j, r] for r in range(count)])

    def norm(row):
        mean = column(row, 0) / voxels
        var = column(row, 1) / voxels - mean * mean
        return spread(mean), spread(lax.rsqrt(var + EPSILON))

    def set_offsets(k, j, mean, part):
        def off(offset):
            return spread(column(slots[j, rank_of(at_offset(offset))], 2)) - mean
        for dx in (0,) if part == SIDES else (-1, 1):
            rows = [-mean if dx == 0 and dy == 0 else off((dx, dy, 0)) for dy in (-1, 0, 1)]
            edges = by_row(*[jnp.where(odd, off((dx, dy, 1)), off((dx, dy, -1)))
                             for dy in (-1, 0, 1)])
            for x in range(1, nx + 1) if dx == 0 else (0,) if dx < 0 else (nx + 1,):
                for kind, value in enumerate(rows + [edges]):
                    offs[k, x, kind] = value

    plane = sizes[1] * sizes[2]
    assert plane >= tiles
    in_plane = lax.rem(rank, plane)
    owner = in_plane < tiles
    plane_others = [o for o in others if o[0] == 0]
    line_others = [o for o in others if o[1] == 0 and o[2] == 0]

    def send_some(group, src, dst, send, recv):
        for offset in group:
            pltpu.make_async_remote_copy(
                src_ref=src, dst_ref=dst, send_sem=send, recv_sem=recv,
                device_id=ids(at_offset(offset)), device_id_type=MESH).start()

    def plane_start(j, unit, slot):
        for t in range(tiles):
            unit[t, 0:chan] = wsum[:, t * nz:(t + 1) * nz].astype(unit.dtype)
            if unit.shape[1] > chan:
                unit[t, chan:chan + 1] = xsum[:, t * nz:(t + 1) * nz]
        for t in range(tiles):
            @pl.when(in_plane != t)
            def _(t=t):
                pltpu.make_async_remote_copy(
                    src_ref=unit.at[t], dst_ref=slot.at[in_plane], send_sem=w_send.at[j],
                    recv_sem=w_recv.at[j], device_id_type=MESH,
                    device_id={AXES[1]: t // sizes[2], AXES[2]: t % sizes[2]}).start()

        @pl.when(owner)
        def _():
            slot[in_plane] = unit[in_plane]

    def added(buf, n):
        return tree([buf[r].astype(f32) for r in range(n)])

    def line_start(j, unit, slot, line):
        @pl.when(owner)
        def _():
            wait_bytes(slot, plane, w_recv.at[j])
            wait_bytes(unit, tiles, w_send.at[j])
            line[me[0]] = added(slot, plane).astype(line.dtype)
            here = line.at[me[0]]
            send_some(line_others, here, here, w_send.at[j + 1], w_recv.at[j + 1])

        @pl.when(jnp.logical_not(owner))
        def _():
            wait_bytes(unit, tiles + 1, w_send.at[j])

    def line_sum(j, line):
        wait_bytes(line, sizes[0], w_recv.at[j + 1], w_send.at[j + 1])
        return added(line, sizes[0])

    def share(j, value):
        wfull[j, in_plane] = value.astype(bf16)
        here = wfull.at[j, in_plane]
        send_some(plane_others, here, here, w_send.at[j], w_recv.at[j])

    def spell(j, out):
        @pl.when(owner)
        def _():
            wait_bytes(wfull.at[j], tiles, w_recv.at[j])
            wait_bytes(wfull.at[j], plane, w_send.at[j])

        @pl.when(jnp.logical_not(owner))
        def _():
            wait_bytes(wfull.at[j], tiles + 1, w_recv.at[j])
        for t in range(tiles):
            piece = wfull[j, t].astype(f32)
            for k in range(nz // chan):
                tap = t * (nz // chan) + k
                if tap < 27:
                    out[tap] = piece[:, k * chan:(k + 1) * chan]

    def wgrad(delta_of, shifted, ones=False):
        cuts = []
        for g in range(ny // DEEP):
            for x in range(nx):
                parts = [delta_of(x, g * DEEP + u) for u in range(DEEP)]
                if ones:
                    parts.append(jnp.ones((16, nz), bf16))
                cuts.append(jnp.concatenate(parts, axis=0))
        delta = jnp.concatenate(cuts, axis=1)
        span = 3 * chan
        band = (DEEP + 2) * span
        groups = [jnp.concatenate(
            [p for a in range(3) for p in stack_rows(shifted, a, g * DEEP, DEEP)], axis=0)
            for g in range(ny // DEEP)]
        o = lax.dot_general(
            delta, jnp.concatenate(groups, axis=1), (((1,), (1,)), ((), ())),
            preferred_element_type=f32)
        for a in range(3):
            for ty in range(3):
                at = (a * 3 + ty) * span
                spots = [a * band + (u + ty) * span for u in range(DEEP)]
                wsum[:, at:at + span] = tree(
                    [o[u * chan:(u + 1) * chan, spot:spot + span]
                     for u, spot in enumerate(spots)])
                if ones:
                    xsum[:, at:at + span] = tree(
                        [o[DEEP * chan:DEEP * chan + 1, spot:spot + span] for spot in spots])

    def take(k):
        def step(c, carry):
            at_row = pl.multiple_of(c * pitch, 8)
            for x in range(nx):
                tall[pl.ds(at_row + x * ny, ny)] = raw[k, c, x].astype(f32)
            return carry
        lax.fori_loop(0, chan, step, 0, unroll=4)

        def tile_of(x, y):
            return tall[pl.ds(x * ny + y, chan, stride=pitch)]
        return tile_of

    def give(out):
        def step(c, carry):
            at_row = pl.multiple_of(c * pitch, 8)
            for x in range(nx):
                out[c, x] = tall[pl.ds(at_row + x * ny, ny)].astype(bf16)
            return carry
        lax.fori_loop(0, chan, step, 0, unroll=4)

    def put_row(x, y, tile):
        tall[pl.ds(x * ny + y, chan, stride=pitch)] = tile

    def prepare(k):
        taps = [wraw[k, t].astype(f32) for t in range(27)]
        span = 3 * chan
        for turn in range(2):
            flat = jnp.concatenate(taps, axis=0).T if turn else jnp.concatenate(taps, axis=1)
            none = jnp.zeros((chan, span), f32)
            for u in range(DEEP):
                parts = []
                for a in range(3):
                    for yi in range(DEEP + 2):
                        tx, ty = (2 - a, 2 - yi + u) if turn else (a, yi - u)
                        at = (tx * 3 + ty) * span
                        parts.append(flat[:, at:at + span] if 0 <= ty < 3 else none)
                mats[2 * k + turn, u * chan:(u + 1) * chan] = jnp.concatenate(
                    parts, axis=1).astype(bf16)

    loads[0].wait()
    emit(XB, take(0))
    pl.semaphore_wait(barrier, count - 1)
    halo_start(XB)
    loads[2].wait()
    emit(XA, take(1))
    halo_start(XA)
    loads[3].wait()
    emit(GO, take(2))
    loads[1].wait()
    prepare(0)
    loads[4].wait()
    prepare(1)
    for k in range(5, 9):
        loads[k].wait()

    def gain(k):
        value = spread(jnp.concatenate([gains[k]] * (nz // chan), axis=1))
        return spread(column(value, 0))
    gain_one, bias_one, gain_two, bias_two = [gain(k) for k in range(4)]

    def bring(v, shifted, tile_of, part, ready=None):
        if part != LAST and ready is not None:
            ready(part)
        halo_wait(v, part)
        if part != LAST:
            collect(v, part)
        build(tile_of, shifted, False, part)

    def bring_conv(v, shifted, tile_of, w, full, out, ready=None):
        bring(v, shifted, tile_of, SIDES, ready)
        bring(v, shifted, tile_of, FIRST, ready)
        return conv_stats(out, shifted, w, full, lambda: bring(v, shifted, tile_of, LAST))

    sums = bring_conv(XB, shift_xb, raw_tiles(XB), 0, c1b, C1B)
    sums_start(0, sums)
    halo_start(C1B)

    sums = bring_conv(XA, shift_a, raw_tiles(XA), 0, c1a, C1A)
    sums_start(1, sums)
    halo_start(C1A)

    def silu(z):
        return z * sigmoid(z)

    mean_one, scale_one = norm(sums_finish(0))
    steep_one = gain_one * scale_one
    tile_1b = centred(C1B, 0, c1b)

    def z_one(x, y, inner):
        return tile_1b(x, y, inner) * steep_one + bias_one
    sums = bring_conv(C1B, shift_hb, lambda *at: silu(z_one(*at)), 2, c2b, C2B,
                      lambda part: set_offsets(0, 0, mean_one, part))
    sums_start(2, sums)
    halo_start(C2B)

    mean_a, scale_a = norm(sums_finish(1))
    steep_a = gain_one * scale_a
    tile_1a = centred(C1A, 1, c1a)
    sums = bring_conv(C1A, shift_a, lambda *at: silu(tile_1a(*at) * steep_a + bias_one), 2,
                      c2a, None, lambda part: set_offsets(1, 1, mean_a, part))
    sums_start(3, sums)

    mean_two, scale_two = norm(sums_finish(2))
    steep_two = gain_two * scale_two

    def own_two(x, carry):
        sd, sx = carry
        for y in range(ny):
            c = c2b[x, y] - mean_two
            d = pads[GO, x + 1, y + 1].astype(f32) * slope_of(c * steep_two + bias_two)
            fd2[x + 1, y + 1] = d
            sd, sx = sd + d, sx + d * c
        return sd, sx
    sd, sx = lax.fori_loop(0, nx, own_two, (zero, zero))
    sums_start(4, (total(sx * scale_two), total(sd)))
    halo_start(GO)

    wgrad(lambda x, y: ((c1b[x, y] - mean_one) * scale_one).astype(bf16), shift_xb,
          True)
    plane_start(2, unit_x, slot_x)

    tile_2b = centred(C2B, 2, c2b)
    tile_go = raw_tiles(GO)

    def d_two(*at):
        return tile_go(*at).astype(f32) * slope_of(tile_2b(*at) * steep_two + bias_two)

    def halo_two(x, y, inner):
        fd2[x, y] = d_two(x, y, inner)

    set_offsets(2, 2, mean_two, SIDES)
    halo_wait(C2B, SIDES)
    collect(C2B, SIDES)
    halo_wait(GO, SIDES)
    collect(GO, SIDES)
    halo_rows(halo_two)
    for x in range(1, nx + 1):
        dcols[D2, x] = d_two(x, wide, True)
    set_offsets(2, 2, mean_two, FIRST)
    halo_wait(C2B, FIRST)
    collect(C2B, FIRST)
    halo_wait(C2B, LAST)

    mean_a2, scale_a2 = norm(sums_finish(3))
    steep_a2 = gain_two * scale_a2

    def finish_a(x, carry):
        for y in range(ny):
            put_row(x, y, silu((c2a[x, y] - mean_a2) * steep_a2 + bias_two))
        return carry
    lax.fori_loop(0, nx, finish_a, 0)
    give(ya)

    row_two = sums_finish(4)
    sx2 = spread(column(row_two, 0) / voxels) * scale_two
    sd2 = spread(column(row_two, 1) / voxels)

    def dc_two(x, y, inner):
        c = tile_2b(x, y, inner)
        if not inner:
            d = tile_go(x, y, inner).astype(f32) * slope_of(c * steep_two + bias_two)
        else:
            d = dcols[D2, x] if y == wide else fd2[x, y]
        return steep_two * (d - sd2 - c * sx2)
    build(dc_two, shift_d, True, SIDES)
    halo_wait(GO, FIRST)
    collect(GO, FIRST)
    build(dc_two, shift_d, True, FIRST)

    def rest_two():
        halo_wait(GO, LAST)
        build(dc_two, shift_d, True, LAST)

    def back(x, y, o, carry, half):
        sd, sx, edge = carry
        c = c1b[x, y] - mean_one
        d = o * slope_of(c * steep_one + bias_one)
        fd1[x + 1, y + 1] = d
        d1h[x, y] = d.astype(bf16)
        return sd + d, sx + d * c, put(E1, x, y, o, edge)

    def rest_of_two(carry):
        rest_two()
        return carry
    sd, sx, edge = conv_rows(shift_d, 3, back, (zero, zero, blank), rest_of_two)
    edge_out[E1] = edge
    sums_start(5, (total(sx * scale_one), total(sd)))
    halo_start(E1)
    wgrad(lambda x, y: d1h[x, y], shift_xb)
    plane_start(4, unit_f, slot_f)
    line_start(2, unit_x, slot_x, line_x)
    wgrad(lambda x, y: shift_d[(x + 1) * wide + y + 1, chan:2 * chan], shift_hb)
    plane_start(6, unit_h, slot_h)

    row_one = sums_finish(5)
    sx1_wide = spread(column(row_one, 0) / voxels)
    sx1 = sx1_wide * scale_one
    sd1 = spread(column(row_one, 1) / voxels)
    line_start(4, unit_f, slot_f, line_f)
    def halo_one(x, y, inner):
        fd1[x, y] = pads[E1, x, y].astype(f32) * slope_of(z_one(x, y, inner))

    def dc_one(x, y, inner):
        c = tile_1b(x, y, inner)
        if inner:
            d = dcols[D1, x] if y == wide else fd1[x, y]
        else:
            e = cols[E1, x] if y == wide else pads[E1, x, y]
            d = e.astype(f32) * slope_of(c * steep_one + bias_one)
        return steep_one * (d - sd1 - c * sx1)

    halo_wait(E1, SIDES)
    collect(E1, SIDES)
    halo_rows(halo_one)
    for x in range(1, nx + 1):
        dcols[D1, x] = cols[E1, x].astype(f32) * slope_of(z_one(x, wide, True))
    build(dc_one, shift_d, True, SIDES)

    halo_wait(E1, FIRST)
    collect(E1, FIRST)
    build(dc_one, shift_d, True, FIRST)
    line_start(6, unit_h, slot_h, line_h)

    def rest_one():
        halo_wait(E1, LAST)
        build(dc_one, shift_d, True, LAST)

    def last(x, y, o, carry, half):
        put_row(x, y, o)
        return carry

    def rest_of_one(carry):
        rest_one()
        return carry
    conv_rows(shift_d, 1, last, 0, rest_of_one)
    give(dxb)

    @pl.when(owner)
    def _():
        along = line_sum(2, line_x)
        share(0, steep_one * factor * (
            line_sum(4, line_f) - sd1 * along[chan:chan + 1] - sx1_wide * along[0:chan]))
        share(1, line_sum(6, line_h) * factor)
    for k, row in enumerate((row_one, row_two)):
        for j in range(2):
            gnorm[2 * k + j:2 * k + j + 1, :] = row[:, j * chan:(j + 1) * chan] * factor
    spell(0, gw1)
    spell(1, gw2)


def deliver(*refs):
    sem = refs[-1]
    half = (len(refs) - 1) // 2
    copies = [pltpu.make_async_copy(src, dst, sem.at[k])
              for k, (src, dst) in enumerate(zip(refs[:half], refs[half:-1]))]
    for copy in copies:
        copy.start()
    for copy in copies:
        copy.wait()


def body(sizes, x_a, x_b, w_first, w_second, gain_first, bias_first, gain_second, bias_second,
         grad_out):
    chan, nx, ny, nz = x_a.shape
    count = math.prod(sizes)
    voxels = float(nx * ny * nz * count)
    taps = 27 * chan
    bf16, f32 = jnp.bfloat16, jnp.float32
    tiles = -(-taps // nz)
    plane = sizes[1] * sizes[2]
    full = (nx + 2, ny + 2, chan, nz)
    span = (nx + 2) * (ny + 2)
    grid = (nx, ny, chan, nz)
    vmem = pl.BlockSpec(memory_space=pltpu.VMEM)
    hbm = pl.BlockSpec(memory_space=pltpu.HBM)
    dma = pltpu.SemaphoreType.DMA
    shapes = (
        jax.ShapeDtypeStruct(x_a.shape, bf16),
        jax.ShapeDtypeStruct(x_a.shape, bf16),
        jax.ShapeDtypeStruct((27, chan, chan), f32),
        jax.ShapeDtypeStruct((27, chan, chan), f32),
        jax.ShapeDtypeStruct((4, chan), f32),
    )
    results = pl.pallas_call(
        functools.partial(kernel, sizes, voxels),
        out_shape=shapes,
        in_specs=[hbm] * 9,
        out_specs=[vmem] * 5,
        scratch_shapes=[
            pltpu.VMEM((3, chan, nx, ny, nz), bf16),
            pltpu.VMEM((2, 27, chan, chan), bf16),
            pltpu.VMEM((4, 1, chan), f32),
            pltpu.VMEM((chan * (nx * ny + 8), nz), f32),
            pltpu.VMEM((4, DEEP * chan, 9 * (DEEP + 2) * chan), bf16),
            pltpu.VMEM((7,) + full, bf16),
            pltpu.VMEM((7, chan, nz), bf16),
            pltpu.VMEM((7, 27, chan, nz), bf16),
            pltpu.VMEM((7, nx + 2, chan, nz), bf16),
            pltpu.VMEM((2, nx + 2, chan, nz), f32),
            pltpu.VMEM((3, nx + 2, 4, chan, nz), f32),
        ] + [pltpu.VMEM((span, 3 * chan, nz), bf16)] * 4
        + [pltpu.VMEM(full, f32)] * 2
        + [pltpu.VMEM(grid, f32)] * 4
        + [
            pltpu.VMEM(grid, bf16),
            pltpu.VMEM((6, count, 1, nz), f32),
            pltpu.VMEM((1, tiles * nz), f32),
            pltpu.VMEM((chan, tiles * nz), f32),
            pltpu.VMEM((tiles + 1, chan + 8, nz), f32),
            pltpu.VMEM((plane, chan + 8, nz), f32),
            pltpu.VMEM((sizes[0], chan + 8, nz), f32),
            pltpu.VMEM((tiles + 1, chan, nz), f32),
            pltpu.VMEM((plane, chan, nz), f32),
            pltpu.VMEM((sizes[0], chan, nz), f32),
            pltpu.VMEM((tiles + 1, chan, nz), bf16),
            pltpu.VMEM((plane, chan, nz), bf16),
            pltpu.VMEM((sizes[0], chan, nz), bf16),
            pltpu.VMEM((2, plane + 1, chan, nz), bf16),
            pltpu.VMEM((2 * (ny + 8), chan, nz), bf16),
            dma((9,)),
            dma((7, 3)), dma((7, 3)),
            dma((6,)), dma((6,)),
            dma((8,)), dma((8,)),
        ],
        compiler_params=pltpu.CompilerParams(
            collective_id=0, has_side_effects=True, vmem_limit_bytes=40 * 1024 * 1024),
    )(*[pltpu.with_memory_space_constraint(v, pltpu.HBM) for v in (
        x_a, x_b, grad_out,
        w_first.reshape(27, chan, chan), w_second.reshape(27, chan, chan),
        gain_first.reshape(1, chan), bias_first.reshape(1, chan),
        gain_second.reshape(1, chan), bias_second.reshape(1, chan),
    )])
    y_a, dx_b, gw1, gw2, gnorm = pl.pallas_call(
        deliver,
        out_shape=shapes,
        in_specs=[vmem] * 5,
        out_specs=[hbm] * 5,
        scratch_shapes=[dma((5,))],
        compiler_params=pltpu.CompilerParams(vmem_limit_bytes=8 * 1024 * 1024),
    )(*results)
    cube = (3, 3, 3, chan, chan)
    return y_a, dx_b, gw1.reshape(cube), gw2.reshape(cube), gnorm


def solution(mesh):
    sizes = tuple(mesh.shape[a] for a in AXES)
    split = P(None, *AXES)
    return jax.shard_map(
        functools.partial(body, sizes),
        mesh=mesh,
        in_specs=(split, split, P(), P(), P(), P(), P(), P(), split),
        out_specs=(split, split, P(), P(), P()),
        check_vma=False,
    )
```

```python
import functools
import math

import jax
import jax.numpy as jnp
from jax import lax
from jax.experimental import pallas as pl
from jax.experimental.pallas import tpu as pltpu
from jax.sharding import PartitionSpec as P

EPSILON = 1e-05
AXES = ("gx", "gy", "gz")
MESH = pl.DeviceIdType.MESH
XB, XA, GO, C1B, C1A, C2B, E1 = range(7)
D2, D1 = range(2)
OFFSETS = [(a, b, c) for a in (-1, 0, 1) for b in (-1, 0, 1) for c in (-1, 0, 1)
           if (a, b, c) != (0, 0, 0)]
DEEP = 4


def sigmoid(z):
    return 0.5 * jnp.tanh(0.5 * z) + 0.5


def slope_of(z):
    s = sigmoid(z)
    return s * (1.0 + z * (1.0 - s))


def code(offset):
    a, b, c = offset
    return (a + 1) * 9 + (b + 1) * 3 + c + 1


def minus(offset):
    return tuple(-o for o in offset)


def kernel(
    sizes, voxels,
    xa, xb, go, w1, w2, g1, b1, g2, b2,
    ya, dxb, gw1, gw2, gnorm,
    raw, wraw, gains, tall, mats, pads, edge_out, edge_in, cols, dcols, offs,
    shift_xb, shift_a, shift_hb, shift_d,
    fd2, fd1, c1b, c1a, c2b, c2a, d1h, slots, xsum, wsum,
    unit_x, slot_x, line_x, unit_f, slot_f, line_f, unit_h, slot_h, line_h, wfull,
    bytes_of, load_sem, halo_send, halo_recv, sum_send, sum_recv, w_send, w_recv,
):
    chan, nx, ny, nz = raw.shape[1:]
    wide = ny + 2
    own = nx * ny
    pitch = tall.shape[0] // chan
    count = math.prod(sizes)
    local = float(own * nz)
    factor = 1.0 / math.sqrt(voxels)
    tiles = wsum.shape[1] // nz
    me = [lax.axis_index(a) for a in AXES]

    def rank_of(place):
        return (place[0] * sizes[1] + place[1]) * sizes[2] + place[2]
    rank = rank_of(me)
    lane = lax.broadcasted_iota(jnp.int32, (chan, nz), 1)
    chan_of = lax.broadcasted_iota(jnp.int32, (chan, nz), 0)
    odd = lax.rem(lane, 2) == 1
    zero = jnp.zeros((chan, nz), jnp.float32)
    bf16, f32 = jnp.bfloat16, jnp.float32

    others = [(a, b, c) for a in range(sizes[0]) for b in range(sizes[1])
              for c in range(sizes[2])][:0:-1]

    places = [{o: lax.rem(m + o + s, s) for o in range(-1, s)} for m, s in zip(me, sizes)]

    def at_offset(offset):
        return [places[k][o] for k, o in enumerate(offset)]

    def ids(place):
        return dict(zip(AXES, place))

    loads = []
    for at, (src, dst) in enumerate((
            (xb, raw.at[0]), (w1, wraw.at[0]), (xa, raw.at[1]), (go, raw.at[2]),
            (w2, wraw.at[1]), (g1, gains.at[0]), (b1, gains.at[1]), (g2, gains.at[2]),
            (b2, gains.at[3]))):
        copy = pltpu.make_async_copy(src, dst, load_sem.at[at])
        copy.start()
        loads.append(copy)

    barrier = pltpu.get_barrier_semaphore()
    for offset in others:
        pl.semaphore_signal(
            barrier, inc=1, device_id=ids(at_offset(offset)), device_id_type=MESH)

    inside = []
    for k in range(3):
        inside.append({-1: me[k] > 0, 0: None, 1: me[k] < sizes[k] - 1})

    def reaches(offset):
        known = [inside[k][o] for k, o in enumerate(offset) if o]
        flag = known[0]
        for more in known[1:]:
            flag = jnp.logical_and(flag, more)
        return flag

    SIDES, FIRST, LAST = range(3)
    split = ny // 2 + 1

    def halo_pieces(v, offset):
        if offset[2]:
            part = FIRST if offset[0] else SIDES
            return [(part, edge_out.at[v], edge_in.at[v, code(offset)])]

        def cut(o, n):
            if o == 0:
                return pl.ds(1, n), pl.ds(1, n)
            return (n, 0) if o > 0 else (1, n + 1)
        (sx, dx), (sy, dy) = cut(offset[0], nx), cut(offset[1], ny)
        if offset[0] and not offset[1]:
            return [(part, pads.at[v, sx, rows], pads.at[v, dx, rows])
                    for part, rows in ((FIRST, pl.ds(1, split)),
                                       (LAST, pl.ds(1 + split, ny - split)))]
        part = FIRST if offset[0] else SIDES
        return [(part, pads.at[v, sx, sy], pads.at[v, dx, dy])]

    order = sorted(OFFSETS, key=lambda o: (o[1] == 0 and o[2] == 0, o[0] != 0))

    def halo_start(v):
        for offset in order:
            to = ids([me[k] + o for k, o in enumerate(offset)])

            @pl.when(reaches(offset))
            def _(offset=offset, to=to):
                for part, src, dst in halo_pieces(v, offset):
                    pltpu.make_async_remote_copy(
                        src_ref=src, dst_ref=dst, send_sem=halo_send.at[v, part],
                        recv_sem=halo_recv.at[v, part], device_id=to,
                        device_id_type=MESH).start()

    near = [jnp.where(inside[k][-1], 1, 0) + jnp.where(inside[k][1], 1, 0) for k in range(3)]
    cases = [(0,) if n == 1 else (1,) if n == 2 else (1, 2) for n in sizes]

    def halo_wait(v, part):
        for a in ((0,) if part == SIDES else cases[0]):
            for b in (0,) if part == LAST else cases[1]:
                for c in (0,) if part == LAST else cases[2]:
                    edges = b + c * (1 + b)
                    rows = (b * nx + c * (1 + b), a * (split + edges), a * (ny - split))[part]
                    if not rows:
                        continue
                    known = []
                    if part != SIDES:
                        known.append(near[0] == a)
                    if part != LAST:
                        known += [near[1] == b, near[2] == c]
                    flag = known[0]
                    for more in known[1:]:
                        flag = jnp.logical_and(flag, more)

                    @pl.when(flag)
                    def _(rows=rows):
                        some = bytes_of.at[pl.ds(0, rows)]
                        for sem in (halo_recv.at[v, part], halo_send.at[v, part]):
                            pltpu.make_async_copy(some, some, sem).wait()

    def total(value):
        return jnp.sum(value, axis=1, keepdims=True)

    def spread(value):
        return jnp.broadcast_to(value, zero.shape)

    def turned(tile, by):
        by = by % nz
        return pltpu.roll(tile, by, 1) if by else tile

    def put(v, x, y, tile, edge):
        tile = tile.astype(bf16)
        pads[v, x + 1, y + 1] = tile
        r = 2 * (x * ny + y)
        edge = jnp.where(lane == r, tile[:, nz - 1:nz], edge)
        return jnp.where(lane == r + 1, tile[:, 0:1], edge)

    blank = jnp.zeros((chan, nz), bf16)

    def emit(v, tile_of):
        def step(x, edge):
            for y in range(ny):
                edge = put(v, x, y, tile_of(x, y), edge)
            return edge
        edge_out[v] = lax.fori_loop(0, nx, step, blank)

    first_lanes = jnp.logical_or(lane == 0, lane == nz - 1)
    last_lanes = jnp.logical_or(lane == 2 * ny + 1, lane == 2 * ny + 2)

    def by_row(first, middle, last):
        return jnp.where(first_lanes, first, jnp.where(last_lanes, last, middle))

    def collect(v, part):
        for dx in (0,) if part == SIDES else (-1, 1):
            low, high = [[edge_in[v, code((-dx, -dy, -dz))] for dy in (-1, 0, 1)]
                         for dz in (-1, 1)]
            for x in range(1, nx + 1) if dx == 0 else (0,) if dx < 0 else (nx + 1,):
                base = (nx - 1, x - 1, 0)[dx + 1] * ny
                moves = (-2 * (base + ny), -2 * base, 2 * ny - 2 * base)
                got = [jnp.where(odd, turned(h, by), turned(l, by + 2))
                       for l, h, by in zip(low, high, moves)]
                cols[v, x] = by_row(*got)

    row_of_lane = jnp.where(lane == nz - 1, 0, lax.div(lane + 1, 2))
    low_y = jnp.where(me[1] > 0, 0, 1)
    high_y = jnp.where(me[1] < sizes[1] - 1, wide, wide - 1)
    low_z = jnp.where(me[2] > 0, 1, 0)
    high_z = jnp.where(me[2] < sizes[2] - 1, 1, 0)
    keep_edge = jnp.where(jnp.logical_and(row_of_lane >= low_y, row_of_lane < high_y),
                          jnp.where(odd, high_z, low_z), 0)

    def build(tile_of, shifted, turn, part):
        inner = part == SIDES
        rows = (range(wide), range(split + 1), range(split + 1, wide))[part]

        def step(i, carry):
            if inner:
                x, x_ok = i + 1, None
            else:
                x = i * (nx + 1)
                x_ok = jnp.where(i == 0, me[0], sizes[0] - 1 - me[0]) > 0

            def both(flag):
                return flag if x_ok is None else jnp.logical_and(x_ok, flag)
            limits = {0: jnp.where(both(me[1] > 0), nz, 0),
                      wide - 1: jnp.where(both(me[1] < sizes[1] - 1), nz, 0)}
            middle = None if inner else jnp.where(x_ok, nz, 0)
            least = 1 if inner else jnp.where(x_ok, 1, 2)
            edge = tile_of(x, wide, inner)
            edge = jnp.where(keep_edge >= least, edge, jnp.zeros_like(edge)).astype(bf16)
            for y in rows:
                tile = tile_of(x, y, inner)
                limit = limits.get(y, middle)
                if limit is not None:
                    tile = jnp.where(lane < limit, tile, jnp.zeros_like(tile))
                tile = tile.astype(bf16)
                ends = turned(edge, -2 * y)
                low = jnp.where(lane == 0, ends, turned(tile, 1))
                high = jnp.where(lane == nz - 1, ends, turned(tile, -1))
                row = x * wide + y
                shifted[row, 0:chan] = high if turn else low
                shifted[row, chan:2 * chan] = tile
                shifted[row, 2 * chan:] = low if turn else high
            return carry
        lax.fori_loop(0, nx if inner else 2, step, 0, unroll=2)

    def raw_tiles(v):
        def tile_of(x, y, inner):
            return cols[v, x] if isinstance(y, int) and y == wide else pads[v, x, y]
        return tile_of

    def centred(v, k, full):
        def tile_of(x, y, inner):
            if not isinstance(y, int):
                return pads[v, x, y].astype(f32) + offs[k, x, 1]
            if y == wide:
                return cols[v, x].astype(f32) + offs[k, x, 3]
            if inner and 0 < y < wide - 1:
                return full[x - 1, y - 1] + offs[k, x, 1]
            kind = 0 if y == 0 else 2 if y == wide - 1 else 1
            return pads[v, x, y].astype(f32) + offs[k, x, kind]
        return tile_of

    def halo_rows(fn):
        for x in range(1, nx + 1):
            for y in (0, wide - 1):
                fn(x, y, True)

    def stack_rows(shifted, a, y, deep):
        parts = []
        for yi in range(deep + 2):
            parts.append(jnp.concatenate(
                [shifted[(x + a) * wide + y + yi] for x in range(nx)], axis=1))
        return parts

    def conv_rows(shifted, w, finish, carry, between):
        groups = ny // DEEP
        for half in range(2):
            def step(i, carry):
                y0 = i * DEEP
                data = jnp.concatenate(
                    [p for a in range(3) for p in stack_rows(shifted, a, y0, DEEP)], axis=0)
                o = jnp.dot(mats[w], data, preferred_element_type=f32)
                for x in range(nx):
                    for u in range(DEEP):
                        carry = finish(
                            x, y0 + u, o[u * chan:(u + 1) * chan, x * nz:(x + 1) * nz],
                            carry, half)
                return carry
            if half:
                carry = between(carry)
            carry = lax.fori_loop(
                half * (groups // 2), groups // 2 if half == 0 else groups, step, carry,
                unroll=2)
        return carry

    def conv_stats(v, shifted, w, full, between):
        centre = []

        def finish(x, y, o, carry, half):
            full[x, y] = o
            first, second, edge = carry
            if half and v is not None:
                edge = put(v, x, y, o - centre[0], edge)
            return first + o, second + o * o, edge

        def middle(carry):
            first, second, edge = carry
            if v is not None:
                mean = spread(total(first) / (0.5 * local))
                centre.append(mean.astype(bf16).astype(f32))
                for x in range(nx):
                    for y in range(ny // 2):
                        edge = put(v, x, y, full[x, y] - centre[0], edge)
            between()
            return first, second, edge
        first, second, edge = conv_rows(shifted, w, finish, (zero, zero, blank), middle)
        if v is None:
            return total(first), total(second)
        edge_out[v] = edge
        return total(first), total(second), centre[0]

    def row_of(values):
        tile = zero
        for k, value in enumerate(values):
            tile = jnp.where(lane == k * chan + chan_of, value, tile)
        return jnp.sum(tile, axis=0, keepdims=True)

    def column(row, k):
        return total(jnp.where(lane == k * chan + chan_of, row, 0.0))

    def all_start(buf, value, send, recv):
        buf[rank] = value
        for offset in others:
            pltpu.make_async_remote_copy(
                src_ref=buf.at[rank], dst_ref=buf.at[rank], send_sem=send,
                recv_sem=recv, device_id=ids(at_offset(offset)), device_id_type=MESH).start()

    def wait_bytes(buf, n, *sems):
        some = buf.at[pl.ds(0, n - 1)]
        for sem in sems:
            pltpu.make_async_copy(some, some, sem).wait()

    def tree(values):
        while len(values) > 1:
            values = [values[i] + values[i + 1] if i + 1 < len(values) else values[i]
                      for i in range(0, len(values), 2)]
        return values[0]

    def sums_start(j, values):
        all_start(slots.at[j], row_of(values), sum_send.at[j],
                  sum_recv.at[j])

    def sums_finish(j):
        wait_bytes(slots.at[j], count, sum_recv.at[j], sum_send.at[j])
        return tree([slots[j, r] for r in range(count)])

    def norm(row):
        mean = column(row, 0) / voxels
        var = column(row, 1) / voxels - mean * mean
        return spread(mean), spread(lax.rsqrt(var + EPSILON))

    def set_offsets(k, j, mean, part):
        def off(offset):
            return spread(column(slots[j, rank_of(at_offset(offset))], 2)) - mean
        for dx in (0,) if part == SIDES else (-1, 1):
            rows = [-mean if dx == 0 and dy == 0 else off((dx, dy, 0)) for dy in (-1, 0, 1)]
            edges = by_row(*[jnp.where(odd, off((dx, dy, 1)), off((dx, dy, -1)))
                             for dy in (-1, 0, 1)])
            for x in range(1, nx + 1) if dx == 0 else (0,) if dx < 0 else (nx + 1,):
                for kind, value in enumerate(rows + [edges]):
                    offs[k, x, kind] = value

    plane = sizes[1] * sizes[2]
    assert plane >= tiles
    in_plane = lax.rem(rank, plane)
    owner = in_plane < tiles
    plane_others = [o for o in others if o[0] == 0]
    line_others = [o for o in others if o[1] == 0 and o[2] == 0]

    def send_some(group, src, dst, send, recv):
        for offset in group:
            pltpu.make_async_remote_copy(
                src_ref=src, dst_ref=dst, send_sem=send, recv_sem=recv,
                device_id=ids(at_offset(offset)), device_id_type=MESH).start()

    def plane_start(j, unit, slot):
        for t in range(tiles):
            unit[t, 0:chan] = wsum[:, t * nz:(t + 1) * nz].astype(unit.dtype)
            if unit.shape[1] > chan:
                unit[t, chan:chan + 1] = xsum[:, t * nz:(t + 1) * nz]
        for t in range(tiles):
            @pl.when(in_plane != t)
            def _(t=t):
                pltpu.make_async_remote_copy(
                    src_ref=unit.at[t], dst_ref=slot.at[in_plane], send_sem=w_send.at[j],
                    recv_sem=w_recv.at[j], device_id_type=MESH,
                    device_id={AXES[1]: t // sizes[2], AXES[2]: t % sizes[2]}).start()

        @pl.when(owner)
        def _():
            slot[in_plane] = unit[in_plane]

    def added(buf, n):
        return tree([buf[r].astype(f32) for r in range(n)])

    def line_start(j, unit, slot, line):
        @pl.when(owner)
        def _():
            wait_bytes(slot, plane, w_recv.at[j])
            wait_bytes(unit, tiles, w_send.at[j])
            line[me[0]] = added(slot, plane).astype(line.dtype)
            here = line.at[me[0]]
            send_some(line_others, here, here, w_send.at[j + 1], w_recv.at[j + 1])

        @pl.when(jnp.logical_not(owner))
        def _():
            wait_bytes(unit, tiles + 1, w_send.at[j])

    def line_sum(j, line):
        wait_bytes(line, sizes[0], w_recv.at[j + 1], w_send.at[j + 1])
        return added(line, sizes[0])

    def share(j, value):
        wfull[j, in_plane] = value.astype(bf16)
        here = wfull.at[j, in_plane]
        send_some(plane_others, here, here, w_send.at[j], w_recv.at[j])

    def spell(j, out):
        @pl.when(owner)
        def _():
            wait_bytes(wfull.at[j], tiles, w_recv.at[j])
            wait_bytes(wfull.at[j], plane, w_send.at[j])

        @pl.when(jnp.logical_not(owner))
        def _():
            wait_bytes(wfull.at[j], tiles + 1, w_recv.at[j])
        for t in range(tiles):
            piece = wfull[j, t].astype(f32)
            for k in range(nz // chan):
                tap = t * (nz // chan) + k
                if tap < 27:
                    out[tap] = piece[:, k * chan:(k + 1) * chan]

    def wgrad(delta_of, shifted, ones=False):
        cuts = []
        for g in range(ny // DEEP):
            for x in range(nx):
                parts = [delta_of(x, g * DEEP + u) for u in range(DEEP)]
                if ones:
                    parts.append(jnp.ones((16, nz), bf16))
                cuts.append(jnp.concatenate(parts, axis=0))
        delta = jnp.concatenate(cuts, axis=1)
        span = 3 * chan
        band = (DEEP + 2) * span
        groups = [jnp.concatenate(
            [p for a in range(3) for p in stack_rows(shifted, a, g * DEEP, DEEP)], axis=0)
            for g in range(ny // DEEP)]
        o = lax.dot_general(
            delta, jnp.concatenate(groups, axis=1), (((1,), (1,)), ((), ())),
            preferred_element_type=f32)
        for a in range(3):
            for ty in range(3):
                at = (a * 3 + ty) * span
                spots = [a * band + (u + ty) * span for u in range(DEEP)]
                wsum[:, at:at + span] = tree(
                    [o[u * chan:(u + 1) * chan, spot:spot + span]
                     for u, spot in enumerate(spots)])
                if ones:
                    xsum[:, at:at + span] = tree(
                        [o[DEEP * chan:DEEP * chan + 1, spot:spot + span] for spot in spots])

    def take(k):
        def step(c, carry):
            at_row = pl.multiple_of(c * pitch, 8)
            for x in range(nx):
                tall[pl.ds(at_row + x * ny, ny)] = raw[k, c, x].astype(f32)
            return carry
        lax.fori_loop(0, chan, step, 0, unroll=4)

        def tile_of(x, y):
            return tall[pl.ds(x * ny + y, chan, stride=pitch)]
        return tile_of

    def give(out):
        def step(c, carry):
            at_row = pl.multiple_of(c * pitch, 8)
            for x in range(nx):
                out[c, x] = tall[pl.ds(at_row + x * ny, ny)].astype(bf16)
            return carry
        lax.fori_loop(0, chan, step, 0, unroll=4)

    def put_row(x, y, tile):
        tall[pl.ds(x * ny + y, chan, stride=pitch)] = tile

    def prepare(k):
        taps = [wraw[k, t].astype(f32) for t in range(27)]
        span = 3 * chan
        for turn in range(2):
            flat = jnp.concatenate(taps, axis=0).T if turn else jnp.concatenate(taps, axis=1)
            none = jnp.zeros((chan, span), f32)
            for u in range(DEEP):
                parts = []
                for a in range(3):
                    for yi in range(DEEP + 2):
                        tx, ty = (2 - a, 2 - yi + u) if turn else (a, yi - u)
                        at = (tx * 3 + ty) * span
                        parts.append(flat[:, at:at + span] if 0 <= ty < 3 else none)
                mats[2 * k + turn, u * chan:(u + 1) * chan] = jnp.concatenate(
                    parts, axis=1).astype(bf16)

    loads[0].wait()
    emit(XB, take(0))
    pl.semaphore_wait(barrier, count - 1)
    halo_start(XB)
    loads[2].wait()
    emit(XA, take(1))
    halo_start(XA)
    loads[3].wait()
    emit(GO, take(2))
    loads[1].wait()
    prepare(0)
    loads[4].wait()
    prepare(1)
    for k in range(5, 9):
        loads[k].wait()

    def gain(k):
        value = spread(jnp.concatenate([gains[k]] * (nz // chan), axis=1))
        return spread(column(value, 0))
    gain_one, bias_one, gain_two, bias_two = [gain(k) for k in range(4)]

    def bring(v, shifted, tile_of, part, ready=None):
        if part != LAST and ready is not None:
            ready(part)
        halo_wait(v, part)
        if part != LAST:
            collect(v, part)
        build(tile_of, shifted, False, part)

    def bring_conv(v, shifted, tile_of, w, full, out, ready=None):
        bring(v, shifted, tile_of, SIDES, ready)
        bring(v, shifted, tile_of, FIRST, ready)
        return conv_stats(out, shifted, w, full, lambda: bring(v, shifted, tile_of, LAST))

    sums = bring_conv(XB, shift_xb, raw_tiles(XB), 0, c1b, C1B)
    sums_start(0, sums)
    halo_start(C1B)

    sums = bring_conv(XA, shift_a, raw_tiles(XA), 0, c1a, C1A)
    sums_start(1, sums)
    halo_start(C1A)

    def silu(z):
        return z * sigmoid(z)

    mean_one, scale_one = norm(sums_finish(0))
    steep_one = gain_one * scale_one
    tile_1b = centred(C1B, 0, c1b)

    def z_one(x, y, inner):
        return tile_1b(x, y, inner) * steep_one + bias_one
    sums = bring_conv(C1B, shift_hb, lambda *at: silu(z_one(*at)), 2, c2b, C2B,
                      lambda part: set_offsets(0, 0, mean_one, part))
    sums_start(2, sums)
    halo_start(C2B)

    mean_a, scale_a = norm(sums_finish(1))
    steep_a = gain_one * scale_a
    tile_1a = centred(C1A, 1, c1a)
    sums = bring_conv(C1A, shift_a, lambda *at: silu(tile_1a(*at) * steep_a + bias_one), 2,
                      c2a, None, lambda part: set_offsets(1, 1, mean_a, part))
    sums_start(3, sums)

    mean_two, scale_two = norm(sums_finish(2))
    steep_two = gain_two * scale_two

    def own_two(x, carry):
        sd, sx = carry
        for y in range(ny):
            c = c2b[x, y] - mean_two
            d = pads[GO, x + 1, y + 1].astype(f32) * slope_of(c * steep_two + bias_two)
            fd2[x + 1, y + 1] = d
            sd, sx = sd + d, sx + d * c
        return sd, sx
    sd, sx = lax.fori_loop(0, nx, own_two, (zero, zero))
    sums_start(4, (total(sx * scale_two), total(sd)))
    halo_start(GO)

    wgrad(lambda x, y: ((c1b[x, y] - mean_one) * scale_one).astype(bf16), shift_xb,
          True)
    plane_start(2, unit_x, slot_x)

    tile_2b = centred(C2B, 2, c2b)
    tile_go = raw_tiles(GO)

    def d_two(*at):
        return tile_go(*at).astype(f32) * slope_of(tile_2b(*at) * steep_two + bias_two)

    def halo_two(x, y, inner):
        fd2[x, y] = d_two(x, y, inner)

    set_offsets(2, 2, mean_two, SIDES)
    halo_wait(C2B, SIDES)
    collect(C2B, SIDES)
    halo_wait(GO, SIDES)
    collect(GO, SIDES)
    halo_rows(halo_two)
    for x in range(1, nx + 1):
        dcols[D2, x] = d_two(x, wide, True)
    set_offsets(2, 2, mean_two, FIRST)
    halo_wait(C2B, FIRST)
    collect(C2B, FIRST)
    halo_wait(C2B, LAST)

    mean_a2, scale_a2 = norm(sums_finish(3))
    steep_a2 = gain_two * scale_a2

    def finish_a(x, carry):
        for y in range(ny):
            put_row(x, y, silu((c2a[x, y] - mean_a2) * steep_a2 + bias_two))
        return carry
    lax.fori_loop(0, nx, finish_a, 0)
    give(ya)

    row_two = sums_finish(4)
    sx2 = spread(column(row_two, 0) / voxels) * scale_two
    sd2 = spread(column(row_two, 1) / voxels)

    def dc_two(x, y, inner):
        c = tile_2b(x, y, inner)
        if not inner:
            d = tile_go(x, y, inner).astype(f32) * slope_of(c * steep_two + bias_two)
        else:
            d = dcols[D2, x] if y == wide else fd2[x, y]
        return steep_two * (d - sd2 - c * sx2)
    build(dc_two, shift_d, True, SIDES)
    halo_wait(GO, FIRST)
    collect(GO, FIRST)
    build(dc_two, shift_d, True, FIRST)

    def rest_two():
        halo_wait(GO, LAST)
        build(dc_two, shift_d, True, LAST)

    def back(x, y, o, carry, half):
        sd, sx, edge = carry
        c = c1b[x, y] - mean_one
        d = o * slope_of(c * steep_one + bias_one)
        fd1[x + 1, y + 1] = d
        d1h[x, y] = d.astype(bf16)
        return sd + d, sx + d * c, put(E1, x, y, o, edge)

    def rest_of_two(carry):
        rest_two()
        return carry
    sd, sx, edge = conv_rows(shift_d, 3, back, (zero, zero, blank), rest_of_two)
    edge_out[E1] = edge
    sums_start(5, (total(sx * scale_one), total(sd)))
    halo_start(E1)
    wgrad(lambda x, y: d1h[x, y], shift_xb)
    plane_start(4, unit_f, slot_f)
    line_start(2, unit_x, slot_x, line_x)
    wgrad(lambda x, y: shift_d[(x + 1) * wide + y + 1, chan:2 * chan], shift_hb)
    plane_start(6, unit_h, slot_h)

    row_one = sums_finish(5)
    sx1_wide = spread(column(row_one, 0) / voxels)
    sx1 = sx1_wide * scale_one
    sd1 = spread(column(row_one, 1) / voxels)
    line_start(4, unit_f, slot_f, line_f)
    def halo_one(x, y, inner):
        fd1[x, y] = pads[E1, x, y].astype(f32) * slope_of(z_one(x, y, inner))

    def dc_one(x, y, inner):
        c = tile_1b(x, y, inner)
        if inner:
            d = dcols[D1, x] if y == wide else fd1[x, y]
        else:
            e = cols[E1, x] if y == wide else pads[E1, x, y]
            d = e.astype(f32) * slope_of(c * steep_one + bias_one)
        return steep_one * (d - sd1 - c * sx1)

    halo_wait(E1, SIDES)
    collect(E1, SIDES)
    halo_rows(halo_one)
    for x in range(1, nx + 1):
        dcols[D1, x] = cols[E1, x].astype(f32) * slope_of(z_one(x, wide, True))
    build(dc_one, shift_d, True, SIDES)

    halo_wait(E1, FIRST)
    collect(E1, FIRST)
    build(dc_one, shift_d, True, FIRST)
    line_start(6, unit_h, slot_h, line_h)

    def rest_one():
        halo_wait(E1, LAST)
        build(dc_one, shift_d, True, LAST)

    def last(x, y, o, carry, half):
        put_row(x, y, o)
        return carry

    def rest_of_one(carry):
        rest_one()
        return carry
    conv_rows(shift_d, 1, last, 0, rest_of_one)
    give(dxb)

    @pl.when(owner)
    def _():
        along = line_sum(2, line_x)
        share(0, steep_one * factor * (
            line_sum(4, line_f) - sd1 * along[chan:chan + 1] - sx1_wide * along[0:chan]))
        share(1, line_sum(6, line_h) * factor)
    for k, row in enumerate((row_one, row_two)):
        for j in range(2):
            gnorm[2 * k + j:2 * k + j + 1, :] = row[:, j * chan:(j + 1) * chan] * factor
    spell(0, gw1)
    spell(1, gw2)


def deliver(*refs):
    sem = refs[-1]
    half = (len(refs) - 1) // 2
    copies = [pltpu.make_async_copy(src, dst, sem.at[k])
              for k, (src, dst) in enumerate(zip(refs[:half], refs[half:-1]))]
    for copy in copies:
        copy.start()
    for copy in copies:
        copy.wait()


def body(sizes, x_a, x_b, w_first, w_second, gain_first, bias_first, gain_second, bias_second,
         grad_out):
    chan, nx, ny, nz = x_a.shape
    count = math.prod(sizes)
    voxels = float(nx * ny * nz * count)
    taps = 27 * chan
    bf16, f32 = jnp.bfloat16, jnp.float32
    tiles = -(-taps // nz)
    plane = sizes[1] * sizes[2]
    full = (nx + 2, ny + 2, chan, nz)
    span = (nx + 2) * (ny + 2)
    grid = (nx, ny, chan, nz)
    vmem = pl.BlockSpec(memory_space=pltpu.VMEM)
    hbm = pl.BlockSpec(memory_space=pltpu.HBM)
    dma = pltpu.SemaphoreType.DMA
    shapes = (
        jax.ShapeDtypeStruct(x_a.shape, bf16),
        jax.ShapeDtypeStruct(x_a.shape, bf16),
        jax.ShapeDtypeStruct((27, chan, chan), f32),
        jax.ShapeDtypeStruct((27, chan, chan), f32),
        jax.ShapeDtypeStruct((4, chan), f32),
    )
    results = pl.pallas_call(
        functools.partial(kernel, sizes, voxels),
        out_shape=shapes,
        in_specs=[hbm] * 9,
        out_specs=[vmem] * 5,
        scratch_shapes=[
            pltpu.VMEM((3, chan, nx, ny, nz), bf16),
            pltpu.VMEM((2, 27, chan, chan), bf16),
            pltpu.VMEM((4, 1, chan), f32),
            pltpu.VMEM((chan * (nx * ny + 8), nz), f32),
            pltpu.VMEM((4, DEEP * chan, 9 * (DEEP + 2) * chan), bf16),
            pltpu.VMEM((7,) + full, bf16),
            pltpu.VMEM((7, chan, nz), bf16),
            pltpu.VMEM((7, 27, chan, nz), bf16),
            pltpu.VMEM((7, nx + 2, chan, nz), bf16),
            pltpu.VMEM((2, nx + 2, chan, nz), f32),
            pltpu.VMEM((3, nx + 2, 4, chan, nz), f32),
        ] + [pltpu.VMEM((span, 3 * chan, nz), bf16)] * 4
        + [pltpu.VMEM(full, f32)] * 2
        + [pltpu.VMEM(grid, f32)] * 4
        + [
            pltpu.VMEM(grid, bf16),
            pltpu.VMEM((6, count, 1, nz), f32),
            pltpu.VMEM((1, tiles * nz), f32),
            pltpu.VMEM((chan, tiles * nz), f32),
            pltpu.VMEM((tiles + 1, chan + 8, nz), f32),
            pltpu.VMEM((plane, chan + 8, nz), f32),
            pltpu.VMEM((sizes[0], chan + 8, nz), f32),
            pltpu.VMEM((tiles + 1, chan, nz), f32),
            pltpu.VMEM((plane, chan, nz), f32),
            pltpu.VMEM((sizes[0], chan, nz), f32),
            pltpu.VMEM((tiles + 1, chan, nz), bf16),
            pltpu.VMEM((plane, chan, nz), bf16),
            pltpu.VMEM((sizes[0], chan, nz), bf16),
            pltpu.VMEM((2, plane + 1, chan, nz), bf16),
            pltpu.VMEM((2 * (ny + 8), chan, nz), bf16),
            dma((9,)),
            dma((7, 3)), dma((7, 3)),
            dma((6,)), dma((6,)),
            dma((8,)), dma((8,)),
        ],
        compiler_params=pltpu.CompilerParams(
            collective_id=0, has_side_effects=True, vmem_limit_bytes=40 * 1024 * 1024),
    )(*[pltpu.with_memory_space_constraint(v, pltpu.HBM) for v in (
        x_a, x_b, grad_out,
        w_first.reshape(27, chan, chan), w_second.reshape(27, chan, chan),
        gain_first.reshape(1, chan), bias_first.reshape(1, chan),
        gain_second.reshape(1, chan), bias_second.reshape(1, chan),
    )])
    y_a, dx_b, gw1, gw2, gnorm = pl.pallas_call(
        deliver,
        out_shape=shapes,
        in_specs=[vmem] * 5,
        out_specs=[hbm] * 5,
        scratch_shapes=[dma((5,))],
        compiler_params=pltpu.CompilerParams(vmem_limit_bytes=8 * 1024 * 1024),
    )(*results)
    cube = (3, 3, 3, chan, chan)
    return y_a, dx_b, gw1.reshape(cube), gw2.reshape(cube), gnorm


def solution(mesh):
    sizes = tuple(mesh.shape[a] for a in AXES)
    split = P(None, *AXES)
    return jax.shard_map(
        functools.partial(body, sizes),
        mesh=mesh,
        in_specs=(split, split, P(), P(), P(), P(), P(), P(), split),
        out_specs=(split, split, P(), P(), P()),
        check_vma=False,
    )
```
